32 devices in a mesh: seq: 8 (over z, core), head: 4 (over y, x).
Axes of the slice: x: 2, y: 2, z: 4, core: 2. Of those that a mesh axis runs over, the one named last changes fastest.
Arguments:
- queries: bfloat16 [4096, 1024], P('seq', 'head'), may hold values from -6 to 6
- keys: bfloat16 [4096, 256], P(('seq', 'head')), may hold values from -6 to 6
- values: bfloat16 [4096, 256], P(('seq', 'head')), may hold values from -3 to 3
- attn_out: bfloat16 [4096, 1024], P('seq', 'head'), may hold values from -1.796875 to 1.796875
- out_grad: bfloat16 [4096, 1024], P('seq', 'head'), may hold values from -6 to 6
- log_norm: float32 [8, 4096], P('head', 'seq'), may hold values from 3.5 to 5.5
- block_layout: int32 [8, 32, 32], P('head'), may hold values 0 or 1
- document_ids: int32 [4096], replicated, may hold values from 0 to 7, never falling along the last dimension, each value on 1 to 2048 neighbouring positions
- block_order: int32 [32], replicated, may hold values from 0 to 31, each once
Outputs:
- query_grad: float32 [4096, 1024], P('seq', 'head')
- key_grad: float32 [4096, 256], P(('seq', 'head'))
- value_grad: float32 [4096, 256], P(('seq', 'head'))
The draws below stay inside these ranges and needn't reach their ends.
Inputs may be any that keep to these rules, and one draw needn't show every extreme that they name: `document_ids`: never falls along the sequence position; each document covers 1 to 2048 positions, one exactly 2048. `block_order`: each sequence block once.
All inputs are finite; a program needn't handle non-finite values.
Results may differ from the reference program's by a relative error of at most 0.0029.
Values may be sent and summed in bfloat16 or wider, within the bound.
A program may use at most 128 MiB of HBM per device.

```python
import math
import jax
import jax.numpy as jnp
import numpy as np
from jax import lax

D_HEAD = 128
GROUP = 4
BLOCK = 128
DOCS = 8
HEADS = 8
KV_HEADS = 2
SEQ = 4096
NBLK = 32


def touch_ends(entries, stream_key, low, largest):
    longest = entries.shape.index(max(entries.shape))
    spots = []
    for shift in (0, 1):
        where = [jax.random.randint(jax.random.fold_in(stream_key, axis), (), 0, length) for axis, length in enumerate(entries.shape)]
        where[longest] = (where[longest] + shift) % entries.shape[longest]
        spots.append(tuple(where))
    return entries.at[spots[0]].set(low).at[spots[1]].set(largest)


def steps_of(key, dims, shards, smallest, high):
    def one(axis_at, parts):
        heights = jax.random.uniform(jax.random.fold_in(jax.random.fold_in(key, 6), axis_at), (parts,), jnp.float32, smallest / len(shards), high / len(shards))
        return jnp.repeat(jnp.exp(heights), dims[axis_at] // parts).reshape((-1,) + (1,) * (len(dims) - axis_at - 1))

    loudness = one(*shards[0])
    for cut in shards[1:]:
        loudness = loudness * one(*cut)
    return loudness


def split_up(count, total, most, lean):
    loads = [(1 << 20) // math.isqrt(grade ** lean) + 1 for grade in range(2, count + 1)]
    surplus, counts = total - most - (count - 1), [1] * (count - 1)
    while surplus > 0:
        movable = [i for i in range(count - 1) if counts[i] < most]
        mass, budget = sum([loads[i] for i in movable]), surplus
        for i in movable:
            addition = min(most - counts[i], max(1, budget * loads[i] // mass), surplus)
            counts[i] = counts[i] + addition
            surplus = surplus - addition
    return np.array([most] + counts)


def uneven_parts(own_key, number_of, total, most, skew):
    if number_of == 2:
        one = jax.random.randint(own_key, (), max(1, total - most), min(most, total - 1) + 1)
        return jnp.stack([one, total - one])
    tallies = jnp.asarray(split_up(number_of, total, most, skew), jnp.int32)
    pairs = (number_of - 1) // 2
    source_of, taker = tallies[1:1 + 2 * pairs:2], tallies[2:2 + 2 * pairs:2]
    margin = jnp.minimum(source_of - 1, most - taker)
    shifted = jax.random.randint(jax.random.fold_in(own_key, 1), (pairs,), 0, 1 << 20) % (margin + 1)
    tallies = tallies.at[1:1 + 2 * pairs:2].set(source_of - shifted).at[2:2 + 2 * pairs:2].set(taker + shifted)
    return tallies[jax.random.permutation(jax.random.fold_in(own_key, 2), number_of)]


def bell_draw(key, shape, spread, reach, split=(), kind=jnp.bfloat16):
    drawn = spread * jax.random.normal(key, shape, jnp.float32)
    if split:
        drawn = drawn * steps_of(key, shape, split, -0.22, 0.18)
    return jnp.clip(drawn, -reach, reach).astype(kind)


def setup_inputs(seed: int = 0) -> dict:
    arg_keys = jax.random.split(jax.random.key(seed), 10)
    return {
        "queries": bell_draw(arg_keys[0], (SEQ, HEADS * D_HEAD), 1.0, 6.0, ((0, 8), (1, 4))),
        "keys": bell_draw(arg_keys[1], (SEQ, KV_HEADS * D_HEAD), 1.0, 6.0, ((0, 32),)),
        "values": bell_draw(arg_keys[2], (SEQ, KV_HEADS * D_HEAD), 0.5, 3.0, ((0, 32),)),
        "attn_out": bell_draw(arg_keys[3], (SEQ, HEADS * D_HEAD), 0.3, 1.796875, ((0, 8), (1, 4))),
        "out_grad": bell_draw(arg_keys[4], (SEQ, HEADS * D_HEAD), 1.0, 6.0, ((0, 8), (1, 4))),
        "log_norm": jnp.clip(3.5 + 2.0 * jax.random.uniform(arg_keys[5], (HEADS, SEQ), jnp.float32) ** steps_of(arg_keys[5], (HEADS, SEQ), ((0, 4), (1, 8)), -0.2, 0.2), 3.5, 5.5),
        "block_layout": touch_ends((jax.random.randint(arg_keys[6], (HEADS, NBLK, NBLK), 0, 4) < 3).astype(jnp.int32), jax.random.fold_in(arg_keys[6], 1), 0, 1),
        "document_ids": jnp.searchsorted(jnp.cumsum(uneven_parts(arg_keys[7], DOCS, SEQ, SEQ // 2, 2)), jnp.arange(SEQ), side="right").astype(jnp.int32),
        "block_order": jax.random.permutation(arg_keys[8], NBLK).astype(jnp.int32),
    }


def stored_positions(block_order, document_ids):
    stored = jnp.arange(SEQ, dtype=jnp.int32)
    position = block_order[stored // BLOCK].astype(jnp.int32) * BLOCK + stored % BLOCK
    return position, document_ids[position]


def reference(queries, keys, values, attn_out, out_grad, log_norm, block_layout, document_ids, block_order):
    position, docs = stored_positions(block_order, document_ids)
    blocks = position // BLOCK
    scaling = D_HEAD ** -0.5
    allowed = (position[None, :] <= position[:, None]) & (docs[:, None] == docs[None, :])
    query_heads = queries.reshape(SEQ, HEADS, D_HEAD).transpose(1, 0, 2)
    grad_heads = out_grad.reshape(SEQ, HEADS, D_HEAD).transpose(1, 0, 2)
    out_heads = attn_out.reshape(SEQ, HEADS, D_HEAD).transpose(1, 0, 2)
    key_heads = keys.reshape(SEQ, KV_HEADS, D_HEAD).transpose(1, 0, 2)
    value_heads = values.reshape(SEQ, KV_HEADS, D_HEAD).transpose(1, 0, 2)

    def one_head(head_index):
        query_one = query_heads[head_index]
        grad_one = grad_heads[head_index]
        out_one = out_heads[head_index]
        key_one = key_heads[head_index // GROUP]
        value_one = value_heads[head_index // GROUP]
        layout_one = block_layout[head_index][blocks[:, None], blocks[None, :]] == 1
        visible = allowed & layout_one
        scores = jnp.dot(query_one, key_one.T, preferred_element_type=jnp.float32) * scaling
        weights = jnp.where(visible, jnp.exp(scores - log_norm[head_index][:, None]), 0.0)
        weights_low = weights.astype(jnp.bfloat16)
        value_part = jnp.dot(weights_low.T, grad_one, preferred_element_type=jnp.float32)
        grad_scores = jnp.dot(grad_one, value_one.T, preferred_element_type=jnp.float32)
        delta = jnp.sum(grad_one.astype(jnp.float32) * out_one.astype(jnp.float32), axis=1)
        score_grad = (weights * (grad_scores - delta[:, None])).astype(jnp.bfloat16)
        query_part = jnp.dot(score_grad, key_one, preferred_element_type=jnp.float32)
        key_part = jnp.dot(score_grad.T, query_one, preferred_element_type=jnp.float32)
        return query_part, key_part, value_part

    query_all, key_all, value_all = lax.map(one_head, jnp.arange(HEADS, dtype=jnp.int32))
    query_grad = (query_all * scaling).transpose(1, 0, 2).reshape(SEQ, HEADS * D_HEAD)
    key_sum = key_all.reshape(KV_HEADS, GROUP, SEQ, D_HEAD).sum(axis=1) * scaling
    value_sum = value_all.reshape(KV_HEADS, GROUP, SEQ, D_HEAD).sum(axis=1)
    key_grad = key_sum.transpose(1, 0, 2).reshape(SEQ, KV_HEADS * D_HEAD)
    value_grad = value_sum.transpose(1, 0, 2).reshape(SEQ, KV_HEADS * D_HEAD)
    return (query_grad, key_grad, value_grad)
```

```python
import functools
import math

import jax
import jax.numpy as jnp
from jax import lax
from jax.experimental import pallas as pl
from jax.experimental.pallas import tpu as pltpu
from jax.sharding import PartitionSpec as P

D_HEAD = 128
GROUP = 4
BLOCK = 128
DOCS = 8
CORES = 2
LOG2E = math.log2(math.e)
SCALE = D_HEAD ** -0.5
NT = (((1,), (1,)), ((), ()))
TN = (((0,), (0,)), ((), ()))


def place(share):
    seq, head = lax.axis_index("seq"), lax.axis_index("head")
    return seq // CORES, seq % CORES, head // share, head % share


def remote(src, dst, send, recv, seq, head):
    return pltpu.make_async_remote_copy(
        src_ref=src, dst_ref=dst, send_sem=send, recv_sem=recv,
        device_id={"seq": seq, "head": head}, device_id_type=pl.DeviceIdType.MESH)


def landed(where, sem):
    pltpu.make_async_copy(where, where, sem).wait()


def when(there, run):
    if there is True:
        run()
    else:
        pl.when(there)(run)


def span(index, rows):
    return pl.ds(pl.multiple_of(index * rows, rows), rows)


def near(deep, kv_heads, share):
    z, c, g, x = place(share)
    seq, head = z * CORES + c, g * share + x
    peers = [(z * CORES + (c + d) % CORES, head, True) for d in range(1, CORES)]
    peers += [(seq, g * share + (x + d) % share, True) for d in range(1, share)]
    peers += [(seq, (g + d) % kv_heads * share + x, True) for d in range(1, kv_heads)]
    if deep > 1:
        peers += [(seq + CORES, head, z + 1 < deep), (seq - CORES, head, z > 0)]
    return peers


def signal(sem, peers):
    for seq, head, there in peers:
        when(there, lambda: pl.semaphore_signal(
            sem, inc=1, device_id={"seq": seq, "head": head},
            device_id_type=pl.DeviceIdType.MESH))


def count(peers):
    total = 0
    for _, _, there in peers:
        total = total + (1 if there is True else there.astype(jnp.int32))
    return total


def unit_row(u, unit, rows, kv_heads, share):
    z, c, g, x = place(share)
    per = rows // unit
    piece, sub = u // per, u % per
    depth, group = piece // kv_heads, piece % kv_heads
    owner = (depth * CORES + c) * kv_heads * share + group * share + x
    return owner * rows + sub * unit


def gather_kernel(
    deep, kv_heads, share, q_in, do_in, o_in, ln_in, k_in, v_in, lay_in, docs_in, order_in,
    kv, q_all, do_all, stats, lows, tops, lay_far,
    k_buf, v_buf, o_buf, ln_buf, docs, order, layout,
    local, kv_send, kv_recv, v_recv, x_send, x_recv, core_send, core_recv,
):
    z, c, g, x = place(share)
    seq, head = z * CORES + c, g * share + x
    heads, q_rows = ln_in.shape
    rows = k_in.shape[0]
    own = q_rows // BLOCK
    unit = min(rows, BLOCK)
    mine = z * kv_heads + g

    def cols(index):
        return pl.ds(pl.multiple_of(index * D_HEAD, D_HEAD), D_HEAD)

    here = span(c, q_rows)
    pulls = [
        (k_in, k_buf), (v_in, v_buf),
        (k_in.at[:, cols(g)], kv.at[0, span(mine, rows), :]),
        (v_in.at[:, cols(g)], kv.at[1, span(mine, rows), :]),
        (q_in, q_all.at[x, here, :]), (do_in, do_all.at[x, here, :]),
        (o_in, o_buf), (ln_in, ln_buf), (docs_in, docs), (order_in, order),
        (lay_in, layout.at[x]),
    ]
    pulls = [pltpu.make_async_copy(src, dst, local.at[n]) for n, (src, dst) in enumerate(pulls)]
    for pull in pulls:
        pull.start()
    peers = near(deep, kv_heads, share)
    barrier = pltpu.get_barrier_semaphore()
    signal(barrier, peers)
    for pull in pulls[:6]:
        pull.wait()
    pl.semaphore_wait(barrier, count(peers))

    sent = []

    def send(make, there=True):
        sent.append((there, make))
        when(there, lambda: make().start())

    kv_slots = [0]

    def send_kv(src, dst, arrival, to_seq, to_head, there=True):
        slot = kv_slots[0]
        kv_slots[0] += 1
        send(lambda: remote(src, dst, kv_send.at[slot], arrival, to_seq, to_head), there)

    def whole(index):
        return kv.at[:, span(index, rows), :]

    def onward(index, step, there):
        send_kv(whole(index), whole(index), kv_recv.at[index], seq + step * CORES, head, there)

    for d in range(1, kv_heads):
        other = (g + d) % kv_heads
        for n, (ref, arrival) in enumerate(((k_buf, kv_recv.at[mine]), (v_buf, v_recv.at[d - 1]))):
            send_kv(ref.at[:, cols(other)], kv.at[n, span(mine, rows), :], arrival,
                    seq, other * share + x)

    def chunk_of(lane, core, n):
        return [ref.at[lane, pl.ds(core * q_rows + n * BLOCK, BLOCK), :] for ref in (q_all, do_all)]

    def x_slot(d, n, t):
        return ((d - 1) * own + n) * 2 + t

    far_at = (share - 1) * own * 2
    for n in range(own):
        for d in range(1, share):
            for t, part in enumerate(chunk_of(x, c, n)):
                slot = x_slot(d, n, t)
                send(functools.partial(remote, part, part, x_send.at[slot], x_recv.at[slot], seq,
                                       g * share + (x + d) % share))
        if n == 0:
            onward(mine, 1, z + 1 < deep)
            onward(mine, -1, z > 0)
    for d in range(1, share):
        slot = far_at + (d - 1) * 2
        send(functools.partial(remote, lay_in, lay_far.at[d - 1], x_send.at[slot],
                               x_recv.at[slot], seq, g * share + (x + d) % share))
    partner = z * CORES + 1 - c
    for n, ref in enumerate((q_all, do_all)):
        part = ref.at[x, here, :]
        send(functools.partial(remote, part, part, core_send.at[n], core_recv.at[n],
                               partner, head))

    for pull in pulls[6:]:
        pull.wait()
    mine_stats = stats.at[x, pl.ds(c * own, own)]
    for n in range(own):
        part = slice(n * BLOCK, (n + 1) * BLOCK)
        at = pl.ds(c * q_rows + n * BLOCK, BLOCK)
        for h in range(heads):
            lanes = slice(h * D_HEAD, (h + 1) * D_HEAD)
            product = (do_all[x, at, lanes].astype(jnp.float32)
                       * o_buf[part, lanes].astype(jnp.float32))
            stats[x, c * own + n, h:h + 1, :] = ln_buf[h:h + 1, part] * LOG2E
            stats[x, c * own + n, heads + h:heads + h + 1, :] = jnp.sum(
                product.T, axis=0, keepdims=True)
    ids = docs[...]
    low = jnp.zeros_like(ids)
    for d in range(1, DOCS):
        before = jnp.sum(jnp.where(ids < d, 1.0, 0.0), axis=1, keepdims=True)
        before = jnp.sum(before, axis=0, keepdims=True).astype(jnp.int32)
        low = jnp.where(ids >= d, before, low)
    lows[...] = low
    for d in range(1, share):
        slot = far_at + (d - 1) * 2 + 1
        send(functools.partial(remote, mine_stats, mine_stats, x_send.at[slot], x_recv.at[slot],
                               seq, g * share + (x + d) % share))
    send(functools.partial(remote, mine_stats, mine_stats, core_send.at[2], core_recv.at[2],
                           partner, head))

    def relay(part, slot):
        landed(part, x_recv.at[slot])
        send(functools.partial(remote, part, part, core_send.at[3 + slot],
                               core_recv.at[3 + slot], partner, head))

    def relay_chunk(n):
        for d in range(1, share):
            for t, part in enumerate(chunk_of((x - d + share) % share, c, n)):
                relay(part, x_slot(d, n, t))

    for j in range(1, kv_heads):
        index = z * kv_heads + (g + j) % kv_heads
        for n, sem in enumerate((kv_recv.at[index], v_recv.at[kv_heads - j - 1])):
            landed(kv.at[n, span(index, rows), :], sem)
        onward(index, 1, z + 1 < deep)
        onward(index, -1, z > 0)
    chunks = 0
    for d in range(1, deep):
        for j in range(kv_heads):
            for depth, step, here_too in ((z - d, 1, z - d >= 0), (z + d, -1, z + d < deep)):
                index = depth * kv_heads + (g + j) % kv_heads
                when(here_too, functools.partial(
                    lambda index: landed(whole(index), kv_recv.at[index]), index))
                if d < deep - 1:
                    more = z + 1 < deep if step == 1 else z > 0
                    onward(index, step, here_too & more)
        if d == 1:
            for e in range(1, share):
                lane = (x - e + share) % share
                landed(lay_far.at[e - 1], x_recv.at[far_at + (e - 1) * 2])
                pull = pltpu.make_async_copy(lay_far.at[e - 1], layout.at[lane],
                                             local.at[len(pulls) + e - 1])
                pull.start()
                pull.wait()
                slot = far_at + (e - 1) * 2 + 1
                relay(stats.at[lane, pl.ds(c * own, own)], slot)

            lane_of = lax.broadcasted_iota(jnp.int32, (1, BLOCK), 1)

            def top_row(i, _):
                qb = order[z * CORES * own + i]

                def top_unit(u, _):
                    kb = order[unit_row(u, unit, rows, kv_heads, share) // BLOCK]
                    for s in range(share):
                        for h in range(heads):
                            on = layout[s, h, qb, kb] == 1
                            tops[i, u, :, (s * heads + h) * BLOCK:(s * heads + h + 1) * BLOCK] = (
                                jnp.where(on, lane_of + qb * BLOCK, -1))
                    return 0

                return lax.fori_loop(0, tops.shape[1], top_unit, 0)

            lax.fori_loop(0, tops.shape[0], top_row, 0)
        if chunks < own:
            relay_chunk(chunks)
            chunks += 1
    for n in range(chunks, own):
        relay_chunk(n)
    there = span(1 - c, q_rows)
    for n, ref in enumerate((q_all, do_all)):
        landed(ref.at[x, there, :], core_recv.at[n])
    landed(stats.at[x, pl.ds((1 - c) * own, own)], core_recv.at[2])
    for d in range(1, share):
        lane = (x - d + share) % share
        for n in range(own):
            for t, part in enumerate(chunk_of(lane, 1 - c, n)):
                landed(part, core_recv.at[3 + x_slot(d, n, t)])
        landed(stats.at[lane, pl.ds((1 - c) * own, own)],
               core_recv.at[3 + far_at + (d - 1) * 2 + 1])
    for there, make in sent:
        when(there, functools.partial(lambda make: make().wait_send(), make))


def gather(queries, out_grad, attn_out, log_norm, keys, values, block_layout, document_ids,
           block_order, deep, kv_heads, share):
    rows = keys.shape[0]
    heads, q_rows = log_norm.shape
    blocks = block_order.shape[0]
    own = q_rows // BLOCK
    unit = min(rows, BLOCK)
    pieces = deep * kv_heads
    kv_rows = pieces * rows
    hbm = pl.BlockSpec(memory_space=pltpu.HBM)
    vmem = pl.BlockSpec(memory_space=pltpu.VMEM)
    lanes = share - 1
    x_copies = max(1, lanes * own * 2 + lanes * 2)
    kv_copies = max(1, 2 * (kv_heads - 1) + 2 * kv_heads * (deep - 1))
    dma = pltpu.SemaphoreType.DMA
    every = jax.ShapeDtypeStruct((share, CORES * q_rows, heads * D_HEAD), queries.dtype)
    return pl.pallas_call(
        functools.partial(gather_kernel, deep, kv_heads, share),
        out_shape=(
            jax.ShapeDtypeStruct((2, kv_rows, D_HEAD), keys.dtype),
            every,
            every,
            jax.ShapeDtypeStruct((share, CORES * own, 2 * heads, BLOCK), jnp.float32),
            jax.ShapeDtypeStruct((blocks, BLOCK), jnp.int32),
            jax.ShapeDtypeStruct(
                (CORES * own, kv_rows // unit, 1, share * heads * BLOCK), jnp.int32),
            jax.ShapeDtypeStruct((max(1, lanes),) + block_layout.shape, jnp.int32),
        ),
        in_specs=[hbm] * 9,
        out_specs=(vmem,) * 6 + (hbm,),
        scratch_shapes=[
            pltpu.VMEM(keys.shape, keys.dtype),
            pltpu.VMEM(values.shape, values.dtype),
            pltpu.VMEM(attn_out.shape, attn_out.dtype),
            pltpu.VMEM(log_norm.shape, jnp.float32),
            pltpu.VMEM((blocks, BLOCK), jnp.int32),
            pltpu.SMEM((blocks,), jnp.int32),
            pltpu.SMEM((share,) + block_layout.shape, jnp.int32),
            dma((11 + max(1, lanes),)),
            dma((kv_copies,)),
            dma((pieces,)),
            dma((max(1, kv_heads - 1),)),
            dma((x_copies,)),
            dma((x_copies,)),
            dma((3 + x_copies,)),
            dma((3 + x_copies,)),
        ],
        compiler_params=pltpu.CompilerParams(collective_id=0, has_side_effects=True,
            vmem_limit_bytes=16 << 20),
        name="gather",
    )(queries, out_grad, attn_out, log_norm, keys, values, block_layout,
      document_ids.reshape(blocks, BLOCK), block_order)


def grads_kernel(
    kv_heads, share, rows, order, docs, q_all, do_all, stats, kv, lows, tops,
    dqt, acc, unit_pos, item_q, item_u,
):
    z, c, g, x = place(share)
    queries = dqt.shape[1]
    heads = q_all.shape[2] // D_HEAD
    unit = min(rows, BLOCK)
    units = kv.shape[1] // unit
    wide = share * heads * BLOCK
    first = z * queries

    for u in range(units):
        row = unit_row(u, unit, rows, kv_heads, share)
        unit_pos[u] = order[row // BLOCK] * BLOCK + row % BLOCK

    def listing(i, n):
        qb = order[first + i]
        doc = docs[qb * BLOCK]
        for s in range(share):
            dqt[s, pl.ds(i, 1)] = jnp.zeros((1,) + dqt.shape[2:], jnp.float32)
        for u in range(units):
            pos = unit_pos[u]
            seen = (pos <= qb * BLOCK + BLOCK - 1) & (docs[pos + unit - 1] >= doc)
            item_q[n] = i
            item_u[n] = u
            n = n + seen.astype(jnp.int32)
        return n

    total = lax.fori_loop(0, queries, listing, 0)
    item_q[total] = 0
    item_u[total] = 0
    acc[...] = jnp.zeros_like(acc)
    sub = lax.broadcasted_iota(jnp.int32, (unit, wide), 0)

    def stacked(ref, i):
        at = pl.ds(pl.multiple_of(i * BLOCK, BLOCK), BLOCK)
        return jnp.concatenate(
            [ref[s, at, h * D_HEAD:(h + 1) * D_HEAD] for s in range(share) for h in range(heads)],
            axis=0)

    def one(n):
        i, u = item_q[n], item_u[n]
        pos = unit_pos[u]
        at = pl.ds(pl.multiple_of(u * unit, unit), unit)
        k, v = kv[0, at, :], kv[1, at, :]
        q4, do4 = stacked(q_all, i), stacked(do_all, i)
        rowed = [stats[s, i] for s in range(share)]
        norm = jnp.concatenate([r[h:h + 1] for r in rowed for h in range(heads)], axis=1)
        delta = jnp.concatenate(
            [r[heads + h:heads + h + 1] for r in rowed for h in range(heads)], axis=1)
        low = jnp.concatenate([lows[pl.ds(order[first + i], 1), :]] * (share * heads), axis=1)
        top = tops[i, u]
        top = jnp.where(n < total, top, -1)
        keep = (sub >= low - pos) & (sub <= top - pos)
        st = lax.dot_general(k, q4, NT, preferred_element_type=jnp.float32)
        dpt = lax.dot_general(v, do4, NT, preferred_element_type=jnp.float32)
        w = jnp.where(keep, jnp.exp2(st * (SCALE * LOG2E) - norm), 0.0)
        ds = (w * (dpt - delta)).astype(jnp.bfloat16)
        dv = jnp.dot(w.astype(jnp.bfloat16), do4, preferred_element_type=jnp.float32)
        dk = jnp.dot(ds, q4, preferred_element_type=jnp.float32)
        dq = lax.dot_general(k, ds, TN, preferred_element_type=jnp.float32)
        return i, at, dk, dv, dq

    def step(t, _):
        done = [one(2 * t), one(2 * t + 1)]
        for i, at, dk, dv, dq in done:
            acc[0, at, :] += dk
            acc[1, at, :] += dv
            for s in range(share):
                dqt[s, i] += dq[:, s * heads * BLOCK:(s + 1) * heads * BLOCK]
        return 0

    lax.fori_loop(0, (total + 1) // 2, step, 0)


def local_grads(block_order, document_ids, q_all, do_all, stats, kv, lows, tops, rows, kv_heads,
                share):
    heads = q_all.shape[2] // D_HEAD
    queries, units = tops.shape[:2]
    smem = pl.BlockSpec(memory_space=pltpu.SMEM)
    vmem = pl.BlockSpec(memory_space=pltpu.VMEM)
    return pl.pallas_call(
        functools.partial(grads_kernel, kv_heads, share, rows),
        out_shape=(
            jax.ShapeDtypeStruct((share, queries, D_HEAD, heads * BLOCK), jnp.float32),
            jax.ShapeDtypeStruct(kv.shape, jnp.float32),
        ),
        in_specs=[smem] * 2 + [vmem] * 6,
        out_specs=(vmem, vmem),
        scratch_shapes=[
            pltpu.SMEM((units,), jnp.int32),
            pltpu.SMEM((queries * units + 2,), jnp.int32),
            pltpu.SMEM((queries * units + 2,), jnp.int32),
        ],
        compiler_params=pltpu.CompilerParams(vmem_limit_bytes=24 << 20),
        name="grads",
    )(block_order, document_ids, q_all, do_all, stats, kv, lows, tops)


def scatter_kernel(
    deep, kv_heads, share, rows, acc, dqt, kv_in, dq_sum, dq_in,
    kv_out, dq_core, dq_out, ready, kv_send, kv_recv, core_send, core_recv, x_send, x_recv,
):
    z, c, g, x = place(share)
    seq, head = z * CORES + c, g * share + x
    partner = z * CORES + 1 - c
    own = dqt.shape[1] // CORES
    heads = dqt.shape[3] // BLOCK
    mine = z * kv_heads + g
    peers = near(deep, kv_heads, share)
    barrier = pltpu.get_barrier_semaphore()
    signal(barrier, peers)
    for p in range(deep * kv_heads):
        part = slice(p * rows, (p + 1) * rows)
        kv_out[p, 0] = (acc[0, part, :] * SCALE).astype(jnp.bfloat16)
        kv_out[p, 1] = acc[1, part, :].astype(jnp.bfloat16)
    kv_in[mine] = kv_out[mine]
    pl.semaphore_wait(barrier, count(peers))

    sent = []

    def send(make, there=True):
        sent.append((there, make))
        when(there, lambda: make().start())

    slots = [0]

    def give(step, turn, there=True):
        slot = slots[0]
        slots[0] += 1
        depth, group = z + step, (g + turn) % kv_heads
        index = depth * kv_heads + group
        send(functools.partial(remote, kv_out.at[index], kv_in.at[mine], kv_send.at[slot],
                               kv_recv.at[mine], depth * CORES + c, group * share + x), there)

    def blocks_of(core, n):
        return dqt.at[:, pl.ds(core * own + n, 1)]

    for step, there in ((1, z + 1 < deep), (-1, z > 0)):
        if deep > 1:
            give(step, 0, there)
    for turn in range(1, kv_heads):
        give(0, turn)
    for n in range(own):
        send(functools.partial(remote, blocks_of(1 - c, n), dq_core.at[:, pl.ds(n, 1)],
                               core_send.at[n], core_recv.at[n], partner, head))
    along = [(s, h, t) for s, h, t in peers[-2:]] if deep > 1 else []
    for d in range(1, deep):
        signal(ready.at[d - 1], along)
        pl.semaphore_wait(ready.at[d - 1], count(along))
        for step in (d, -d):
            there = z + step < deep if step > 0 else z + step >= 0
            if d > 1:
                pass
            for turn in range(1, kv_heads):
                give(step, turn, there)
        if d + 1 < deep:
            for step in (d + 1, -d - 1):
                give(step, 0, z + step < deep if step > 0 else z + step >= 0)

    for n in range(own):
        landed(dq_core.at[:, pl.ds(n, 1)], core_recv.at[n])
        at = slice(n * BLOCK, (n + 1) * BLOCK)
        for d in range(share):
            lane = (x + d) % share
            total = (dqt[lane, c * own + n] + dq_core[lane, n]) * SCALE
            for h in range(heads):
                flat = total[:, h * BLOCK:(h + 1) * BLOCK].T
                if d:
                    dq_out[d - 1, at, h * D_HEAD:(h + 1) * D_HEAD] = flat.astype(jnp.bfloat16)
                else:
                    dq_sum[at, h * D_HEAD:(h + 1) * D_HEAD] = flat
            if d:
                slot = (d - 1) * own + n
                send(functools.partial(
                    remote, dq_out.at[d - 1, at, :], dq_in.at[d - 1, at, :], x_send.at[slot],
                    x_recv.at[slot], seq, g * share + lane))
    for depth in range(deep):
        for turn in range(kv_heads):
            index = depth * kv_heads + (g + turn) % kv_heads
            get = functools.partial(
                lambda index: landed(kv_in.at[index], kv_recv.at[index]), index)
            when(True if turn else depth != z, get)
    for d in range(1, share):
        for n in range(own):
            at = slice(n * BLOCK, (n + 1) * BLOCK)
            landed(dq_in.at[d - 1, at, :], x_recv.at[(d - 1) * own + n])
    for there, make in sent:
        when(there, functools.partial(lambda make: make().wait_send(), make))


def finish_kernel(deep, kv_heads, share, kv_in, dq_sum, dq_in, dq, dk, dv):
    total = dq_sum[...]
    for d in range(share - 1):
        total += dq_in[d].astype(jnp.float32)
    dq[...] = total
    for j in range(kv_heads):
        for n, ref in enumerate((dk, dv)):
            total = kv_in[j, n].astype(jnp.float32)
            for depth in range(1, deep):
                total += kv_in[depth * kv_heads + j, n].astype(jnp.float32)
            ref[:, j * D_HEAD:(j + 1) * D_HEAD] = total


def scatter(dqt, acc, rows, deep, kv_heads, share):
    pieces = deep * kv_heads
    queries, heads = dqt.shape[1], dqt.shape[3] // BLOCK
    own = queries // CORES
    q_rows = own * BLOCK
    vmem = pl.BlockSpec(memory_space=pltpu.VMEM)
    dma = pltpu.SemaphoreType.DMA
    lanes = max(1, share - 1)
    kv_in, dq_sum, dq_in = pl.pallas_call(
        functools.partial(scatter_kernel, deep, kv_heads, share, rows),
        out_shape=(
            jax.ShapeDtypeStruct((pieces, 2, rows, D_HEAD), jnp.bfloat16),
            jax.ShapeDtypeStruct((q_rows, heads * D_HEAD), jnp.float32),
            jax.ShapeDtypeStruct((lanes, q_rows, heads * D_HEAD), jnp.bfloat16),
        ),
        in_specs=[vmem] * 2,
        out_specs=(vmem,) * 3,
        scratch_shapes=[
            pltpu.VMEM((pieces, 2, rows, D_HEAD), jnp.bfloat16),
            pltpu.VMEM((dqt.shape[0], own) + dqt.shape[2:], jnp.float32),
            pltpu.VMEM((lanes, q_rows, heads * D_HEAD), jnp.bfloat16),
            pltpu.SemaphoreType.REGULAR((max(1, deep - 1),)),
            dma((2 * pieces,)),
            dma((pieces,)),
            dma((own,)),
            dma((own,)),
            dma((lanes * own,)),
            dma((lanes * own,)),
        ],
        compiler_params=pltpu.CompilerParams(collective_id=1, has_side_effects=True,
            vmem_limit_bytes=20 << 20),
        name="scatter",
    )(acc, dqt)
    grad = jax.ShapeDtypeStruct((rows, kv_heads * D_HEAD), jnp.float32)
    return pl.pallas_call(
        functools.partial(finish_kernel, deep, kv_heads, share),
        out_shape=(jax.ShapeDtypeStruct(dq_sum.shape, jnp.float32), grad, grad),
        in_specs=[vmem] * 3,
        out_specs=(vmem,) * 3,
        compiler_params=pltpu.CompilerParams(vmem_limit_bytes=8 << 20),
        name="finish",
    )(kv_in, dq_sum, dq_in)


def body(
    queries, keys, values, attn_out, out_grad, log_norm, block_layout, document_ids, block_order
):
    share = GROUP // log_norm.shape[0]
    kv_heads = lax.axis_size("head") // share
    deep = lax.axis_size("seq") // CORES
    rows = keys.shape[0]
    kv, q_all, do_all, stats, lows, tops, _ = gather(
        queries, out_grad, attn_out, log_norm, keys, values, block_layout, document_ids,
        block_order, deep, kv_heads, share)
    dqt, acc = local_grads(block_order, document_ids, q_all, do_all, stats, kv, lows, tops, rows,
                           kv_heads, share)
    return tuple(scatter(dqt, acc, rows, deep, kv_heads, share))


def solution(mesh):
    in_specs = (
        P("seq", "head"),
        P(("seq", "head"), None),
        P(("seq", "head"), None),
        P("seq", "head"),
        P("seq", "head"),
        P("head", "seq"),
        P("head", None, None),
        P(),
        P(),
    )
    out_specs = (P("seq", "head"), P(("seq", "head"), None), P(("seq", "head"), None))
    return jax.shard_map(body, mesh=mesh, in_specs=in_specs, out_specs=out_specs, check_vma=False)
```

```python
import functools
import math

import jax
import jax.numpy as jnp
from jax import lax
from jax.experimental import pallas as pl
from jax.experimental.pallas import tpu as pltpu
from jax.sharding import PartitionSpec as P

D_HEAD = 128
GROUP = 4
BLOCK = 128
DOCS = 8
CORES = 2
PAIR = 2
REACH = 3
LOG2E = math.log2(math.e)
SCALE = D_HEAD ** -0.5
NT = (((1,), (1,)), ((), ()))
TN = (((0,), (0,)), ((), ()))


def place(share):
    seq, head = lax.axis_index("seq"), lax.axis_index("head")
    return seq // CORES, seq % CORES, head // share, head % share


def remote(src, dst, send, recv, seq, head):
    return pltpu.make_async_remote_copy(
        src_ref=src, dst_ref=dst, send_sem=send, recv_sem=recv,
        device_id={"seq": seq, "head": head}, device_id_type=pl.DeviceIdType.MESH)


def landed(where, sem):
    pltpu.make_async_copy(where, where, sem).wait()


def when(there, run):
    if there is True:
        run()
    else:
        pl.when(there)(run)


def span(index, rows):
    return pl.ds(pl.multiple_of(index * rows, rows), rows)


def near(deep, kv_heads, share):
    z, c, g, x = place(share)
    seq, head = z * CORES + c, g * share + x
    peers = [(z * CORES + (c + d) % CORES, head, True) for d in range(1, CORES)]
    peers += [(seq, g * share + (x + d) % share, True) for d in range(1, share)]
    peers += [(seq, (g + d) % kv_heads * share + x, True) for d in range(1, kv_heads)]
    if deep > 1:
        peers += [(seq + CORES, head, z + 1 < deep), (seq - CORES, head, z > 0)]
    return peers


def signal(sem, peers):
    for seq, head, there in peers:
        when(there, lambda: pl.semaphore_signal(
            sem, inc=1, device_id={"seq": seq, "head": head},
            device_id_type=pl.DeviceIdType.MESH))


def count(peers):
    total = 0
    for _, _, there in peers:
        total = total + (1 if there is True else there.astype(jnp.int32))
    return total


def unit_row(u, unit, rows, kv_heads, share):
    z, c, g, x = place(share)
    per = rows // unit
    piece, sub = u // per, u % per
    depth, group = piece // kv_heads, piece % kv_heads
    owner = (depth * CORES + c) * kv_heads * share + group * share + x
    return owner * rows + sub * unit


def gather_kernel(
    deep, kv_heads, share, q_in, do_in, o_in, ln_in, k_in, v_in, lay_in, docs_in, order_in,
    kv, q_all, do_all, stats, lows, tops, lay_far,
    k_buf, v_buf, o_buf, ln_buf, docs, order, layout,
    local, kv_send, kv_recv, v_recv, x_send, x_recv, core_send, core_recv,
):
    z, c, g, x = place(share)
    seq, head = z * CORES + c, g * share + x
    heads, q_rows = ln_in.shape
    rows = k_in.shape[0]
    own = q_rows // BLOCK
    unit = min(rows, BLOCK)
    mine = z * kv_heads + g

    def cols(index):
        return pl.ds(pl.multiple_of(index * D_HEAD, D_HEAD), D_HEAD)

    here = span(c, q_rows)
    pulls = [
        (k_in, k_buf), (v_in, v_buf),
        (k_in.at[:, cols(g)], kv.at[0, span(mine, rows), :]),
        (v_in.at[:, cols(g)], kv.at[1, span(mine, rows), :]),
        (q_in, q_all.at[x, here, :]), (do_in, do_all.at[x, here, :]),
        (o_in, o_buf), (ln_in, ln_buf), (docs_in, docs), (order_in, order),
        (lay_in, layout.at[x]),
    ]
    pulls = [pltpu.make_async_copy(src, dst, local.at[n]) for n, (src, dst) in enumerate(pulls)]
    for pull in pulls:
        pull.start()
    peers = near(deep, kv_heads, share)
    barrier = pltpu.get_barrier_semaphore()
    signal(barrier, peers)
    for pull in pulls[:6]:
        pull.wait()
    pl.semaphore_wait(barrier, count(peers))

    sent = []

    def send(make, there=True):
        sent.append((there, make))
        when(there, lambda: make().start())

    kv_slots = [0]

    def send_kv(src, dst, arrival, to_seq, to_head, there=True):
        slot = kv_slots[0]
        kv_slots[0] += 1
        send(lambda: remote(src, dst, kv_send.at[slot], arrival, to_seq, to_head), there)

    def whole(index):
        return kv.at[:, span(index, rows), :]

    def onward(index, step, there):
        send_kv(whole(index), whole(index), kv_recv.at[index], seq + step * CORES, head, there)

    for d in range(1, kv_heads):
        other = (g + d) % kv_heads
        for n, (ref, arrival) in enumerate(((k_buf, kv_recv.at[mine]), (v_buf, v_recv.at[d - 1]))):
            send_kv(ref.at[:, cols(other)], kv.at[n, span(mine, rows), :], arrival,
                    seq, other * share + x)

    def chunk_of(lane, core, n):
        return [ref.at[lane, pl.ds(core * q_rows + n * BLOCK, BLOCK), :] for ref in (q_all, do_all)]

    def x_slot(d, n, t):
        return ((d - 1) * own + n) * 2 + t

    far_at = (share - 1) * own * 2

    def send_chunk(n):
        for d in range(1, share):
            for t, part in enumerate(chunk_of(x, c, n)):
                slot = x_slot(d, n, t)
                send(functools.partial(remote, part, part, x_send.at[slot], x_recv.at[slot], seq,
                                       g * share + (x + d) % share))

    onward(mine, 1, z + 1 < deep)
    onward(mine, -1, z > 0)
    for d in range(1, share):
        slot = far_at + (d - 1) * 2
        send(functools.partial(remote, lay_in, lay_far.at[d - 1], x_send.at[slot],
                               x_recv.at[slot], seq, g * share + (x + d) % share))
    send_chunk(0)
    partner = z * CORES + 1 - c
    for n, ref in enumerate((q_all, do_all)):
        part = ref.at[x, here, :]
        send(functools.partial(remote, part, part, core_send.at[n], core_recv.at[n],
                               partner, head))

    for pull in pulls[6:]:
        pull.wait()
    mine_stats = stats.at[x, pl.ds(c * own, own)]
    for n in range(own):
        part = slice(n * BLOCK, (n + 1) * BLOCK)
        at = pl.ds(c * q_rows + n * BLOCK, BLOCK)
        for h in range(heads):
            lanes = slice(h * D_HEAD, (h + 1) * D_HEAD)
            product = (do_all[x, at, lanes].astype(jnp.float32)
                       * o_buf[part, lanes].astype(jnp.float32))
            stats[x, c * own + n, h:h + 1, :] = ln_buf[h:h + 1, part] * LOG2E
            stats[x, c * own + n, heads + h:heads + h + 1, :] = jnp.sum(
                product.T, axis=0, keepdims=True)
    for d in range(1, share):
        slot = far_at + (d - 1) * 2 + 1
        send(functools.partial(remote, mine_stats, mine_stats, x_send.at[slot], x_recv.at[slot],
                               seq, g * share + (x + d) % share))
    send(functools.partial(remote, mine_stats, mine_stats, core_send.at[2], core_recv.at[2],
                           partner, head))
    for n in range(1, own):
        send_chunk(n)

    lane_of = lax.broadcasted_iota(jnp.int32, (1, BLOCK), 1)

    def fill_tops(lane):
        def top_row(i, _):
            qb = order[z * CORES * own + i]

            def top_unit(u, _):
                kb = order[unit_row(u, unit, rows, kv_heads, share) // BLOCK]
                for h in range(heads):
                    on = layout[lane, h, qb, kb] == 1
                    at = pl.ds(pl.multiple_of((lane * heads + h) * BLOCK, BLOCK), BLOCK)
                    tops[i, u, :, at] = jnp.where(on, lane_of + qb * BLOCK, -1)
                return 0

            return lax.fori_loop(0, tops.shape[1], top_unit, 0)

        lax.fori_loop(0, tops.shape[0], top_row, 0)

    ids = docs[...]
    low = jnp.zeros_like(ids)
    for d in range(1, DOCS):
        before = jnp.sum(jnp.where(ids < d, 1.0, 0.0), axis=1, keepdims=True)
        before = jnp.sum(before, axis=0, keepdims=True).astype(jnp.int32)
        low = jnp.where(ids >= d, before, low)
    lows[...] = low

    def relay(part, slot):
        landed(part, x_recv.at[slot])
        send(functools.partial(remote, part, part, core_send.at[3 + slot],
                               core_recv.at[3 + slot], partner, head))

    def relay_chunk(n):
        for d in range(1, share):
            for t, part in enumerate(chunk_of((x - d + share) % share, c, n)):
                relay(part, x_slot(d, n, t))

    for j in range(1, kv_heads):
        index = z * kv_heads + (g + j) % kv_heads
        for n, sem in enumerate((kv_recv.at[index], v_recv.at[kv_heads - j - 1])):
            landed(kv.at[n, span(index, rows), :], sem)
        onward(index, 1, z + 1 < deep)
        onward(index, -1, z > 0)
    chunks = 0
    for d in range(1, deep):
        for j in range(kv_heads):
            for depth, step, here_too in ((z - d, 1, z - d >= 0), (z + d, -1, z + d < deep)):
                index = depth * kv_heads + (g + j) % kv_heads
                when(here_too, functools.partial(
                    lambda index: landed(whole(index), kv_recv.at[index]), index))
                if d < deep - 1:
                    more = z + 1 < deep if step == 1 else z > 0
                    onward(index, step, here_too & more)
        if d == 1:
            fill_tops(x)
        if d == min(2, deep - 1):
            for e in range(1, share):
                lane = (x - e + share) % share
                landed(lay_far.at[e - 1], x_recv.at[far_at + (e - 1) * 2])
                pull = pltpu.make_async_copy(lay_far.at[e - 1], layout.at[lane],
                                             local.at[len(pulls) + e - 1])
                pull.start()
                pull.wait()
                relay(stats.at[lane, pl.ds(c * own, own)], far_at + (e - 1) * 2 + 1)
                fill_tops(lane)
        if chunks < own:
            relay_chunk(chunks)
            chunks += 1
    for n in range(chunks, own):
        relay_chunk(n)
    there = span(1 - c, q_rows)
    for n, ref in enumerate((q_all, do_all)):
        landed(ref.at[x, there, :], core_recv.at[n])
    landed(stats.at[x, pl.ds((1 - c) * own, own)], core_recv.at[2])
    for d in range(1, share):
        lane = (x - d + share) % share
        for n in range(own):
            for t, part in enumerate(chunk_of(lane, 1 - c, n)):
                landed(part, core_recv.at[3 + x_slot(d, n, t)])
        landed(stats.at[lane, pl.ds((1 - c) * own, own)],
               core_recv.at[3 + far_at + (d - 1) * 2 + 1])
    for there, make in sent:
        when(there, functools.partial(lambda make: make().wait_send(), make))


def gather(queries, out_grad, attn_out, log_norm, keys, values, block_layout, document_ids,
           block_order, deep, kv_heads, share):
    rows = keys.shape[0]
    heads, q_rows = log_norm.shape
    blocks = block_order.shape[0]
    own = q_rows // BLOCK
    unit = min(rows, BLOCK)
    pieces = deep * kv_heads
    kv_rows = pieces * rows
    hbm = pl.BlockSpec(memory_space=pltpu.HBM)
    vmem = pl.BlockSpec(memory_space=pltpu.VMEM)
    lanes = share - 1
    x_copies = max(1, lanes * own * 2 + lanes * 2)
    kv_copies = max(1, 2 * (kv_heads - 1) + 2 * kv_heads * (deep - 1))
    dma = pltpu.SemaphoreType.DMA
    every = jax.ShapeDtypeStruct((share, CORES * q_rows, heads * D_HEAD), queries.dtype)
    return pl.pallas_call(
        functools.partial(gather_kernel, deep, kv_heads, share),
        out_shape=(
            jax.ShapeDtypeStruct((2, kv_rows, D_HEAD), keys.dtype),
            every,
            every,
            jax.ShapeDtypeStruct((share, CORES * own, 2 * heads, BLOCK), jnp.float32),
            jax.ShapeDtypeStruct((blocks, BLOCK), jnp.int32),
            jax.ShapeDtypeStruct(
                (CORES * own, kv_rows // unit, 1, share * heads * BLOCK), jnp.int32),
            jax.ShapeDtypeStruct((max(1, lanes),) + block_layout.shape, jnp.int32),
        ),
        in_specs=[hbm] * 9,
        out_specs=(vmem,) * 6 + (hbm,),
        scratch_shapes=[
            pltpu.VMEM(keys.shape, keys.dtype),
            pltpu.VMEM(values.shape, values.dtype),
            pltpu.VMEM(attn_out.shape, attn_out.dtype),
            pltpu.VMEM(log_norm.shape, jnp.float32),
            pltpu.VMEM((blocks, BLOCK), jnp.int32),
            pltpu.SMEM((blocks,), jnp.int32),
            pltpu.SMEM((share,) + block_layout.shape, jnp.int32),
            dma((11 + max(1, lanes),)),
            dma((kv_copies,)),
            dma((pieces,)),
            dma((max(1, kv_heads - 1),)),
            dma((x_copies,)),
            dma((x_copies,)),
            dma((3 + x_copies,)),
            dma((3 + x_copies,)),
        ],
        compiler_params=pltpu.CompilerParams(collective_id=0, has_side_effects=True,
            vmem_limit_bytes=16 << 20),
        name="gather",
    )(*[pltpu.with_memory_space_constraint(array, pltpu.HBM) for array in (
        queries, out_grad, attn_out, log_norm, keys, values, block_layout,
        document_ids.reshape(blocks, BLOCK), block_order)])


def grads_kernel(
    kv_heads, share, rows, order_in, docs_in, q_all, do_all, stats, kv, lows, tops,
    dqt, acc, order, docs, unit_pos, item_q, item_u, low_bits, local,
):
    z, c, g, x = place(share)
    queries = dqt.shape[1]
    heads = q_all.shape[2] // D_HEAD
    unit = min(rows, BLOCK)
    units = kv.shape[1] // unit
    first = z * queries
    pulls = [pltpu.make_async_copy(order_in, order, local.at[0]),
             pltpu.make_async_copy(docs_in, docs, local.at[1])]
    for pull in pulls:
        pull.start()
    acc[...] = jnp.zeros_like(acc)

    def clear(i, _):
        for s in range(share):
            dqt[s, pl.ds(i, 1)] = jnp.zeros((1,) + dqt.shape[2:], jnp.float32)
        return 0

    lax.fori_loop(0, queries, clear, 0)
    for pull in pulls:
        pull.wait()

    for u in range(units):
        row = unit_row(u, unit, rows, kv_heads, share)
        unit_pos[u] = order[row // BLOCK] * BLOCK + row % BLOCK

    def listing(i, n):
        qb = order[first + i]
        doc = docs[qb * BLOCK]
        for u in range(units):
            pos = unit_pos[u]
            seen = (pos <= qb * BLOCK + BLOCK - 1) & (docs[pos + unit - 1] >= doc)
            item_q[n] = i
            item_u[n] = u
            n = n + seen.astype(jnp.int32)
        return n

    total = lax.fori_loop(0, queries, listing, 0)
    wide = share * heads * BLOCK
    sub = lax.broadcasted_iota(jnp.int32, (unit, wide), 0)
    low_bits[...] = jnp.zeros_like(low_bits)
    for n in range(2 * PAIR):
        item_q[total + n] = 0
        item_u[total + n] = 0

    def stacked(ref, i):
        at = pl.ds(pl.multiple_of(i * BLOCK, BLOCK), BLOCK)
        return jnp.concatenate(
            [ref[s, at, h * D_HEAD:(h + 1) * D_HEAD] for s in range(share) for h in range(heads)],
            axis=0)

    def weigh(n, slot):
        i, u = item_q[n], item_u[n]
        pos = unit_pos[u]
        at = pl.ds(pl.multiple_of(u * unit, unit), unit)
        k, v = kv[0, at, :], kv[1, at, :]
        q4, do4 = stacked(q_all, i), stacked(do_all, i)
        rowed = [stats[s, i] for s in range(share)]
        norm = jnp.concatenate([r[h:h + 1] for r in rowed for h in range(heads)], axis=1)
        delta = jnp.concatenate(
            [r[heads + h:heads + h + 1] for r in rowed for h in range(heads)], axis=1)
        low = jnp.concatenate([lows[pl.ds(order[first + i], 1), :]] * (share * heads), axis=1)
        top = jnp.where(n < total, tops[i, u], -1)
        keep = (sub >= low - pos) & (sub <= top - pos)
        st = lax.dot_general(k, q4, NT, preferred_element_type=jnp.float32)
        dpt = lax.dot_general(v, do4, NT, preferred_element_type=jnp.float32)
        w = jnp.where(keep, jnp.exp2(st * (SCALE * LOG2E) - norm), 0.0)
        low_bits[slot, 0] = w.astype(jnp.bfloat16)
        low_bits[slot, 1] = (w * (dpt - delta)).astype(jnp.bfloat16)

    def collect(n, slot):
        i, u = item_q[n], item_u[n]
        at = pl.ds(pl.multiple_of(u * unit, unit), unit)
        q4, do4 = stacked(q_all, i), stacked(do_all, i)
        ds = low_bits[slot, 1]
        dv = jnp.dot(low_bits[slot, 0], do4, preferred_element_type=jnp.float32)
        dk = jnp.dot(ds, q4, preferred_element_type=jnp.float32)
        dq = lax.dot_general(kv[0, at, :], ds, TN, preferred_element_type=jnp.float32)
        return i, at, dk, dv, dq

    def step(t, _):
        before = jnp.maximum(t - 1, 0) * PAIR
        done = [collect(before + n, n) for n in range(PAIR)]
        for n in range(PAIR):
            weigh(t * PAIR + n, n)
        for i, at, dk, dv, dq in done:
            acc[0, at, :] += dk
            acc[1, at, :] += dv
            for s in range(share):
                dqt[s, i] += dq[:, s * heads * BLOCK:(s + 1) * heads * BLOCK]
        return 0

    lax.fori_loop(0, (total + PAIR - 1) // PAIR + 1, step, 0)


def local_grads(block_order, document_ids, q_all, do_all, stats, kv, lows, tops, rows, kv_heads,
                share):
    heads = q_all.shape[2] // D_HEAD
    queries, units = tops.shape[:2]
    hbm = pl.BlockSpec(memory_space=pltpu.HBM)
    vmem = pl.BlockSpec(memory_space=pltpu.VMEM)
    return pl.pallas_call(
        functools.partial(grads_kernel, kv_heads, share, rows),
        out_shape=(
            jax.ShapeDtypeStruct((share, queries, D_HEAD, heads * BLOCK), jnp.float32),
            jax.ShapeDtypeStruct(kv.shape, jnp.float32),
        ),
        in_specs=[hbm] * 2 + [vmem] * 6,
        out_specs=(vmem, vmem),
        scratch_shapes=[
            pltpu.SMEM(block_order.shape, jnp.int32),
            pltpu.SMEM(document_ids.shape, jnp.int32),
            pltpu.SMEM((units,), jnp.int32),
            pltpu.SMEM((queries * units + 2 * PAIR,), jnp.int32),
            pltpu.SMEM((queries * units + 2 * PAIR,), jnp.int32),
            pltpu.VMEM((PAIR, 2, min(rows, BLOCK), share * heads * BLOCK), jnp.bfloat16),
            pltpu.SemaphoreType.DMA((2,)),
        ],
        compiler_params=pltpu.CompilerParams(vmem_limit_bytes=24 << 20),
        name="grads",
    )(pltpu.with_memory_space_constraint(block_order, pltpu.HBM),
      pltpu.with_memory_space_constraint(document_ids, pltpu.HBM),
      q_all, do_all, stats, kv, lows, tops)


def scatter_kernel(
    deep, kv_heads, share, rows, acc, dqt, kv_in, dq_sum, dq_in,
    kv_out, joined, dq_core, dq_out, ready, kv_send, kv_recv, join_recv, core_send, core_recv,
    x_send, x_recv,
):
    z, c, g, x = place(share)
    seq, head = z * CORES + c, g * share + x
    partner = z * CORES + 1 - c
    own = dqt.shape[1] // CORES
    heads = dqt.shape[3] // BLOCK
    mine = z * kv_heads + g
    peers = near(deep, kv_heads, share)
    barrier = pltpu.get_barrier_semaphore()
    signal(barrier, peers)
    for p in range(deep * kv_heads):
        part = slice(p * rows, (p + 1) * rows)
        kv_out[p, 0] = (acc[0, part, :] * SCALE).astype(jnp.bfloat16)
        kv_out[p, 1] = acc[1, part, :].astype(jnp.bfloat16)
    kv_in[mine] = kv_out[mine]
    for depth in range(deep):
        def unused(depth=depth):
            at = pl.ds(depth * kv_heads, kv_heads)
            kv_in[at] = jnp.zeros((kv_heads,) + kv_in.shape[1:], kv_in.dtype)

        if depth >= REACH or depth < deep - REACH:
            pl.when((depth - z >= REACH) | (z - depth >= REACH))(unused)
    pl.semaphore_wait(barrier, count(peers))

    sent = []

    def send(make, there=True):
        sent.append((there, make))
        when(there, lambda: make().start())

    slots = [0]

    def slot_of():
        slots[0] += 1
        return slots[0] - 1

    def inside(depth):
        return (depth >= 0) & (depth < deep)

    def give(step, turn, there=True):
        slot = slot_of()
        depth, group = z + step, (g + turn) % kv_heads
        index = depth * kv_heads + group
        send(functools.partial(remote, kv_out.at[index], kv_in.at[mine], kv_send.at[slot],
                               kv_recv.at[mine], depth * CORES + c, group * share + x), there)

    def join(index):
        landed(joined.at[index], join_recv.at[index])
        at = span(index, rows)
        for n, factor in enumerate((SCALE, 1.0)):
            kv_out[index, n] = (acc[n, at, :] * factor
                                + joined[index, n].astype(jnp.float32)).astype(jnp.bfloat16)

    def blocks_of(core, n):
        return dqt.at[:, pl.ds(core * own + n, 1)]

    for far in range(deep - 1, REACH - 1, -1):
        for depth, step in ((far, 1), (deep - 1 - far, -1)):
            away = (depth - z) * step >= REACH
            behind = (z > 0) if step == 1 else (z + 1 < deep)
            for turn in range(kv_heads):
                index = depth * kv_heads + (g + turn) % kv_heads
                if far > REACH:
                    pl.when(away & behind)(functools.partial(join, index))
                slot = slot_of()
                send(functools.partial(remote, kv_out.at[index], joined.at[index],
                                       kv_send.at[slot], join_recv.at[index],
                                       (z + step) * CORES + c, head), away)
    if deep > 1:
        give(1, 0, z + 1 < deep)
        give(-1, 0, z > 0)
    for turn in range(1, kv_heads):
        give(0, turn)
    for n in range(own):
        send(functools.partial(remote, blocks_of(1 - c, n), dq_core.at[:, pl.ds(n, 1)],
                               core_send.at[n], core_recv.at[n], partner, head))
    along = peers[-2:] if deep > 1 else []
    near_end = {1: z == 0, -1: z == deep - 1}
    for d in range(1, min(REACH, deep)):
        signal(ready.at[d - 1], along)
        pl.semaphore_wait(ready.at[d - 1], count(along))
        for step in (1, -1):
            for turn in range(1, kv_heads):
                there = inside(z + step * d)
                give(step * d, turn, there & near_end[step] if d == REACH - 1 else there)
            if d + 1 < min(REACH, deep):
                there = inside(z + step * (d + 1))
                give(step * (d + 1), 0, there & near_end[step] if d == REACH - 2 else there)

    def query_block(n):
        landed(dq_core.at[:, pl.ds(n, 1)], core_recv.at[n])
        at = slice(n * BLOCK, (n + 1) * BLOCK)
        for d in range(share - 1, -1, -1):
            lane = (x + d) % share
            total = (dqt[lane, c * own + n] + dq_core[lane, n]) * SCALE
            for h in range(heads):
                flat = total[:, h * BLOCK:(h + 1) * BLOCK].T
                if d:
                    dq_out[d - 1, at, h * D_HEAD:(h + 1) * D_HEAD] = flat.astype(jnp.bfloat16)
                else:
                    dq_sum[at, h * D_HEAD:(h + 1) * D_HEAD] = flat
            if d:
                slot = (d - 1) * own + n
                send(functools.partial(
                    remote, dq_out.at[d - 1, at, :], dq_in.at[d - 1, at, :], x_send.at[slot],
                    x_recv.at[slot], seq, g * share + lane))

    early = min(2, own)
    for n in range(early):
        query_block(n)
    if deep >= REACH:
        for turn in range(kv_heads):
            for step in (1, -1):
                depth = z + step * (REACH - 1)
                there = inside(depth) & ~near_end[step]
                index = depth * kv_heads + (g + turn) % kv_heads
                pl.when(there)(functools.partial(join, index))
                give(step * (REACH - 1), turn, there)
    for n in range(early, own):
        query_block(n)
    for depth in range(deep):
        for turn in range(kv_heads):
            index = depth * kv_heads + (g + turn) % kv_heads
            close = (depth - z < REACH) & (z - depth < REACH)
            get = functools.partial(
                lambda index: landed(kv_in.at[index], kv_recv.at[index]), index)
            when(close if turn else close & (depth != z), get)
    for d in range(1, share):
        for n in range(own):
            at = slice(n * BLOCK, (n + 1) * BLOCK)
            landed(dq_in.at[d - 1, at, :], x_recv.at[(d - 1) * own + n])
    for there, make in sent:
        when(there, functools.partial(lambda make: make().wait_send(), make))


def finish_kernel(deep, kv_heads, share, kv_in, dq_sum, dq_in, dq, dk, dv):
    total = dq_sum[...]
    for d in range(share - 1):
        total += dq_in[d].astype(jnp.float32)
    dq[...] = total
    for j in range(kv_heads):
        for n, ref in enumerate((dk, dv)):
            total = kv_in[j, n].astype(jnp.float32)
            for depth in range(1, deep):
                total += kv_in[depth * kv_heads + j, n].astype(jnp.float32)
            ref[:, j * D_HEAD:(j + 1) * D_HEAD] = total


def scatter(dqt, acc, rows, deep, kv_heads, share):
    pieces = deep * kv_heads
    queries, heads = dqt.shape[1], dqt.shape[3] // BLOCK
    own = queries // CORES
    q_rows = own * BLOCK
    vmem = pl.BlockSpec(memory_space=pltpu.VMEM)
    dma = pltpu.SemaphoreType.DMA
    lanes = max(1, share - 1)
    kv_in, dq_sum, dq_in = pl.pallas_call(
        functools.partial(scatter_kernel, deep, kv_heads, share, rows),
        out_shape=(
            jax.ShapeDtypeStruct((pieces, 2, rows, D_HEAD), jnp.bfloat16),
            jax.ShapeDtypeStruct((q_rows, heads * D_HEAD), jnp.float32),
            jax.ShapeDtypeStruct((lanes, q_rows, heads * D_HEAD), jnp.bfloat16),
        ),
        in_specs=[vmem] * 2,
        out_specs=(vmem,) * 3,
        scratch_shapes=[
            pltpu.VMEM((pieces, 2, rows, D_HEAD), jnp.bfloat16),
            pltpu.VMEM((pieces, 2, rows, D_HEAD), jnp.bfloat16),
            pltpu.VMEM((dqt.shape[0], own) + dqt.shape[2:], jnp.float32),
            pltpu.VMEM((lanes, q_rows, heads * D_HEAD), jnp.bfloat16),
            pltpu.SemaphoreType.REGULAR((max(1, deep - 1),)),
            dma((6 * pieces,)),
            dma((pieces,)),
            dma((pieces,)),
            dma((own,)),
            dma((own,)),
            dma((lanes * own,)),
            dma((lanes * own,)),
        ],
        compiler_params=pltpu.CompilerParams(collective_id=1, has_side_effects=True,
            vmem_limit_bytes=20 << 20),
        name="scatter",
    )(acc, dqt)
    grad = jax.ShapeDtypeStruct((rows, kv_heads * D_HEAD), jnp.float32)
    return pl.pallas_call(
        functools.partial(finish_kernel, deep, kv_heads, share),
        out_shape=(jax.ShapeDtypeStruct(dq_sum.shape, jnp.float32), grad, grad),
        in_specs=[vmem] * 3,
        out_specs=(vmem,) * 3,
        compiler_params=pltpu.CompilerParams(vmem_limit_bytes=8 << 20),
        name="finish",
    )(kv_in, dq_sum, dq_in)


def body(
    queries, keys, values, attn_out, out_grad, log_norm, block_layout, document_ids, block_order
):
    share = GROUP // log_norm.shape[0]
    kv_heads = lax.axis_size("head") // share
    deep = lax.axis_size("seq") // CORES
    rows = keys.shape[0]
    kv, q_all, do_all, stats, lows, tops, _ = gather(
        queries, out_grad, attn_out, log_norm, keys, values, block_layout, document_ids,
        block_order, deep, kv_heads, share)
    dqt, acc = local_grads(block_order, document_ids, q_all, do_all, stats, kv, lows, tops, rows,
                           kv_heads, share)
    return tuple(scatter(dqt, acc, rows, deep, kv_heads, share))


def solution(mesh):
    in_specs = (
        P("seq", "head"),
        P(("seq", "head"), None),
        P(("seq", "head"), None),
        P("seq", "head"),
        P("seq", "head"),
        P("head", "seq"),
        P("head", None, None),
        P(),
        P(),
    )
    out_specs = (P("seq", "head"), P(("seq", "head"), None), P(("seq", "head"), None))
    return jax.shard_map(body, mesh=mesh, in_specs=in_specs, out_specs=out_specs, check_vma=False)
```

```python
import functools
import math

import jax
import jax.numpy as jnp
from jax import lax
from jax.experimental import pallas as pl
from jax.experimental.pallas import tpu as pltpu
from jax.sharding import PartitionSpec as P

D_HEAD = 128
GROUP = 4
BLOCK = 128
DOCS = 8
CORES = 2
PAIR = 4
SPAN = 2
REACH = 3
LOG2E = math.log2(math.e)
SCALE = D_HEAD ** -0.5
NT = (((1,), (1,)), ((), ()))
TN = (((0,), (0,)), ((), ()))


def place(share):
    seq, head = lax.axis_index("seq"), lax.axis_index("head")
    return seq // CORES, seq % CORES, head // share, head % share


def remote(src, dst, send, recv, seq, head):
    return pltpu.make_async_remote_copy(
        src_ref=src, dst_ref=dst, send_sem=send, recv_sem=recv,
        device_id={"seq": seq, "head": head}, device_id_type=pl.DeviceIdType.MESH)


def landed(where, sem):
    pltpu.make_async_copy(where, where, sem).wait()


def when(there, run):
    if there is True:
        run()
    else:
        pl.when(there)(run)


def span(index, rows):
    return pl.ds(pl.multiple_of(index * rows, rows), rows)


def near(deep, kv_heads, share):
    z, c, g, x = place(share)
    seq, head = z * CORES + c, g * share + x
    peers = [(z * CORES + (c + d) % CORES, head, True) for d in range(1, CORES)]
    peers += [(seq, g * share + (x + d) % share, True) for d in range(1, share)]
    peers += [(seq, (g + d) % kv_heads * share + x, True) for d in range(1, kv_heads)]
    if deep > 1:
        peers += [(seq + CORES, head, z + 1 < deep), (seq - CORES, head, z > 0)]
    return peers


def signal(sem, peers):
    for seq, head, there in peers:
        when(there, lambda: pl.semaphore_signal(
            sem, inc=1, device_id={"seq": seq, "head": head},
            device_id_type=pl.DeviceIdType.MESH))


def count(peers):
    total = 0
    for _, _, there in peers:
        total = total + (1 if there is True else there.astype(jnp.int32))
    return total


def unit_row(u, unit, rows, kv_heads, share):
    z, c, g, x = place(share)
    per = rows // unit
    piece, sub = u // per, u % per
    depth, group = piece // kv_heads, piece % kv_heads
    owner = (depth * CORES + c) * kv_heads * share + group * share + x
    return owner * rows + sub * unit


def gather_kernel(
    deep, kv_heads, share, q_in, do_in, o_in, ln_in, k_in, v_in, lay_in, docs_in, order_in,
    kv, q_all, do_all, stats, lows, tops, acc, dq_own,
    stage, o_buf, ln_buf, docs, order, layout, seen, own_tops, low_bits,
    local, ready, kv_send, kv_recv, x_send, x_recv, core_send, core_recv,
):
    z, c, g, x = place(share)
    seq, head = z * CORES + c, g * share + x
    heads, q_rows = ln_in.shape
    rows = k_in.shape[0]
    own = q_rows // BLOCK
    unit = min(rows, BLOCK)
    mine = z * kv_heads + g

    def cols(index):
        return pl.ds(pl.multiple_of(index * D_HEAD, D_HEAD), D_HEAD)

    here = span(c, q_rows)
    pulls = [(k_in.at[:, cols(g)], kv.at[0, span(mine, rows), :]),
             (v_in.at[:, cols(g)], kv.at[1, span(mine, rows), :])]
    for d in range(1, kv_heads):
        other = cols((g + d) % kv_heads)
        pulls += [(k_in.at[:, other], stage.at[d - 1, 0]), (v_in.at[:, other], stage.at[d - 1, 1])]
    pulls += [(q_in, q_all.at[x, here, :]), (do_in, do_all.at[x, here, :])]
    urgent = len(pulls)
    pulls += [(order_in, order), (lay_in, layout), (o_in, o_buf), (ln_in, ln_buf), (docs_in, docs)]
    pulls = [pltpu.make_async_copy(src, dst, local.at[n]) for n, (src, dst) in enumerate(pulls)]
    for pull in pulls:
        pull.start()
    peers = near(deep, kv_heads, share)
    barrier = pltpu.get_barrier_semaphore()
    signal(barrier, peers)
    for pull in pulls[:urgent]:
        pull.wait()
    pl.semaphore_wait(barrier, count(peers))

    sent = []

    def send(make, there=True):
        sent.append((there, make))
        when(there, lambda: make().start())

    kv_slots = [0]

    def send_kv(src, dst, arrival, to_seq, to_head, there=True):
        slot = kv_slots[0]
        kv_slots[0] += 1
        send(lambda: remote(src, dst, kv_send.at[slot], arrival, to_seq, to_head), there)

    def whole(index):
        return kv.at[:, span(index, rows), :]

    def onward(index, step, there):
        send_kv(whole(index), whole(index), kv_recv.at[index], seq + step * CORES, head, there)

    def reach(index, step):
        there = inside(z + step)
        send_kv(whole(index), whole(index), kv_recv.at[index], seq + step * CORES, head, there)

    def inside(depth):
        return (depth >= 0) & (depth < deep)

    for turn in range(1, kv_heads):
        send_kv(stage.at[turn - 1], whole(mine), kv_recv.at[mine], seq,
                (g + turn) % kv_heads * share + x)
    along = peers[-2:] if deep > 1 else []
    if deep > 1:
        reach(mine, 1)
        reach(mine, -1)
        signal(ready.at[0], along)

    def chunk_of(lane, core, n):
        return [ref.at[lane, pl.ds(core * q_rows + n * BLOCK, BLOCK), :] for ref in (q_all, do_all)]

    def x_slot(d, n, t):
        return ((d - 1) * own + n) * 2 + t

    far_at = (share - 1) * own * 2

    def send_chunk(n):
        for d in range(1, share):
            for t, part in enumerate(chunk_of(x, c, n)):
                slot = x_slot(d, n, t)
                send(functools.partial(remote, part, part, x_send.at[slot], x_recv.at[slot], seq,
                                       g * share + (x + d) % share))

    send_chunk(0)
    partner = z * CORES + 1 - c
    for n, ref in enumerate((q_all, do_all)):
        part = ref.at[x, here, :]
        send(functools.partial(remote, part, part, core_send.at[n], core_recv.at[n],
                               partner, head))

    for pull in pulls[urgent:urgent + 2]:
        pull.wait()
    queries, blocks = CORES * own, order.shape[0]
    units = own_tops.shape[0]
    row_of = lax.broadcasted_iota(jnp.int32, (queries, BLOCK), 0)
    at_block = jnp.zeros((queries, BLOCK), jnp.int32)
    for i in range(queries):
        at_block = jnp.where(row_of == i, order[z * queries + i], at_block)
    column = lax.broadcasted_iota(jnp.int32, (queries, blocks), 1)
    picked = jnp.where(column == at_block[:, :blocks], 1.0, 0.0).astype(jnp.bfloat16)
    for h in range(heads):
        seen[0, h] = jnp.dot(picked, layout[h].astype(jnp.float32).astype(jnp.bfloat16),
                             preferred_element_type=jnp.float32)
    for d in range(1, share):
        slot = far_at + (d - 1) * 2
        send(functools.partial(remote, seen.at[0], seen.at[d], x_send.at[slot], x_recv.at[slot],
                               seq, g * share + (x + d) % share))
    for d in range(1, min(REACH, deep) - 1):
        pl.semaphore_wait(ready.at[d - 1], count(along))
        if d + 2 < min(REACH, deep):
            signal(ready.at[d], along)
        reach(mine, d + 1)
        reach(mine, -d - 1)
    for pull in pulls[urgent + 2:]:
        pull.wait()
    mine_stats = stats.at[x, pl.ds(c * own, own)]
    for n in range(own):
        part = slice(n * BLOCK, (n + 1) * BLOCK)
        at = pl.ds(c * q_rows + n * BLOCK, BLOCK)
        for h in range(heads):
            lanes = slice(h * D_HEAD, (h + 1) * D_HEAD)
            product = (do_all[x, at, lanes].astype(jnp.float32)
                       * o_buf[part, lanes].astype(jnp.float32))
            stats[x, c * own + n, h:h + 1, :] = ln_buf[h:h + 1, part] * LOG2E
            stats[x, c * own + n, heads + h:heads + h + 1, :] = jnp.sum(
                product.T, axis=0, keepdims=True)
    for d in range(1, share):
        slot = far_at + (d - 1) * 2 + 1
        send(functools.partial(remote, mine_stats, mine_stats, x_send.at[slot], x_recv.at[slot],
                               seq, g * share + (x + d) % share))
    send(functools.partial(remote, mine_stats, mine_stats, core_send.at[2], core_recv.at[2],
                           partner, head))
    for n in range(1, own):
        send_chunk(n)

    block_of = lax.broadcasted_iota(jnp.int32, (blocks, BLOCK), 0)
    chosen = jnp.concatenate([
        jnp.where(block_of == order[unit_row(u, unit, rows, kv_heads, share) // BLOCK], 1.0, 0.0)
        for u in range(units)], axis=1).astype(jnp.bfloat16)
    at_query = at_block * BLOCK + lax.broadcasted_iota(jnp.int32, (queries, BLOCK), 1)

    def fill_tops(ref, slot, source):
        for h in range(heads):
            on = jnp.dot(seen[source, h].astype(jnp.bfloat16), chosen,
                         preferred_element_type=jnp.float32)
            at = slice((slot * heads + h) * BLOCK, (slot * heads + h + 1) * BLOCK)
            for u in range(units):
                ref[u, :, at] = jnp.where(on[:, u * BLOCK:(u + 1) * BLOCK] > 0.5, at_query, -1)

    ids = docs[...]
    low = jnp.zeros_like(ids)
    for d in range(1, DOCS):
        before = jnp.sum(jnp.where(ids < d, 1.0, 0.0), axis=1, keepdims=True)
        before = jnp.sum(before, axis=0, keepdims=True).astype(jnp.int32)
        low = jnp.where(ids >= d, before, low)
    lows[...] = low
    fill_tops(own_tops, 0, 0)
    acc[...] = jnp.zeros_like(acc)
    dq_own[...] = jnp.zeros_like(dq_own)
    low_bits[...] = jnp.zeros_like(low_bits)

    sub = lax.broadcasted_iota(jnp.int32, (unit, SPAN * heads * BLOCK), 0)
    both = [(j, h) for j in range(SPAN) for h in range(heads)]

    def stacked(ref, t):
        return jnp.concatenate(
            [ref[x, pl.ds(pl.multiple_of((t * SPAN + j) * BLOCK, BLOCK), BLOCK),
                 h * D_HEAD:(h + 1) * D_HEAD] for j, h in both], axis=0)

    def joint(n, batch):
        return jnp.concatenate([kv[n, span(index, rows), :] for index in batch], axis=0)

    def weigh(t, batch):
        st = lax.dot_general(joint(0, batch), stacked(q_all, t), NT,
                             preferred_element_type=jnp.float32)
        dpt = lax.dot_general(joint(1, batch), stacked(do_all, t), NT,
                              preferred_element_type=jnp.float32)
        rowed = [stats[x, t * SPAN + j] for j in range(SPAN)]
        norm = jnp.concatenate([rowed[j][h:h + 1] for j, h in both], axis=1)
        delta = jnp.concatenate([rowed[j][heads + h:heads + h + 1] for j, h in both], axis=1)
        lowed = [lows[pl.ds(order[z * CORES * own + t * SPAN + j], 1), :] for j in range(SPAN)]
        low = jnp.concatenate([lowed[j] for j, _ in both], axis=1)
        keeps = []
        for u in [index * (rows // unit) + n for index in batch for n in range(rows // unit)]:
            row = unit_row(u, unit, rows, kv_heads, share)
            pos = order[row // BLOCK] * BLOCK + row % BLOCK
            top = jnp.concatenate([own_tops[u, pl.ds(t * SPAN + j, 1), :] for j in range(SPAN)], axis=1)
            keeps.append((sub >= low - pos) & (sub <= top - pos))
        keep = jnp.concatenate(keeps, axis=0)
        w = jnp.where(keep, jnp.exp2(st * (SCALE * LOG2E) - norm), 0.0)
        low_bits[0] = w.astype(jnp.bfloat16)
        low_bits[1] = (w * (dpt - delta)).astype(jnp.bfloat16)

    def collect(t, batch):
        ds = low_bits[1]
        dv = jnp.dot(low_bits[0], stacked(do_all, t), preferred_element_type=jnp.float32)
        dk = jnp.dot(ds, stacked(q_all, t), preferred_element_type=jnp.float32)
        dq = lax.dot_general(joint(0, batch), ds, TN, preferred_element_type=jnp.float32)
        for n, index in enumerate(batch):
            at, part = span(index, rows), slice(n * rows, (n + 1) * rows)
            acc[0, at, :] += dk[part]
            acc[1, at, :] += dv[part]
        for j in range(SPAN):
            dq_own[t * SPAN + j] += dq[:, j * heads * BLOCK:(j + 1) * heads * BLOCK]

    turns = queries // SPAN

    def nearest(k):
        short = jnp.minimum(z, deep - 1 - z)
        beyond = jnp.where(z < deep - 1 - z, k, deep - 1 - k)
        return jnp.where(k <= 2 * short, z + (k + 1) // 2 * (1 - 2 * (k % 2)), beyond)

    def of(k, turn):
        return nearest(k) * kv_heads + (g + turn) % kv_heads

    order_of = [[(0, turn) for turn in range(kv_heads)]]
    late = 1
    if kv_heads == 2 and deep > 2:
        order_of += [[(1, turn), (2, turn)] for turn in range(kv_heads)]
        late = 3
    order_of += [[(k, turn) for turn in range(kv_heads)] for k in range(late, deep)]
    batches = [[of(*entry) for entry in batch] for batch in order_of]

    def attend(k, midway=None):
        batch, before = batches[k], batches[max(k - 1, 0)]

        def turn(t, _):
            first = t == 0
            collect(jnp.where(first, 0 if k == 0 else turns - 1, t - 1),
                    [jnp.where(first, old, new) for old, new in zip(before, batch)])
            weigh(t, batch)
            return 0

        lax.fori_loop(0, turns // 2, turn, 0)
        if midway is not None:
            midway()
        lax.fori_loop(turns // 2, turns, turn, 0)

    def relay(part, slot):
        landed(part, x_recv.at[slot])
        send(functools.partial(remote, part, part, core_send.at[3 + slot],
                               core_recv.at[3 + slot], partner, head))

    def relay_chunk(n):
        for d in range(1, share):
            for t, part in enumerate(chunk_of((x - d + share) % share, c, n)):
                relay(part, x_slot(d, n, t))

    for j in range(1, kv_heads):
        index = z * kv_heads + (g + j) % kv_heads
        landed(whole(index), kv_recv.at[index])
        for d in range(1, min(REACH, deep)):
            reach(index, d)
            reach(index, -d)
    there = span(1 - c, q_rows)
    for n, ref in enumerate((q_all, do_all)):
        landed(ref.at[x, there, :], core_recv.at[n])
    landed(stats.at[x, pl.ds((1 - c) * own, own)], core_recv.at[2])
    attend(0)

    def arrive(d, turns_in):
        for turn in turns_in:
            for depth, step in ((z - d, 1), (z + d, -1)):
                index = depth * kv_heads + (g + turn) % kv_heads
                when(inside(depth), functools.partial(
                    lambda index: landed(whole(index), kv_recv.at[index]), index))
                if REACH - 1 <= d < deep - 1:
                    onward(index, step, inside(depth) & inside(z + step))

    chunks = list(range(own))

    def relay_next():
        if chunks:
            relay_chunk(chunks.pop(0))

    def relay_rest():
        while chunks:
            relay_chunk(chunks.pop(0))

    done = 1
    for turns_in in ([0], list(range(1, kv_heads))):
        for d in range(1, min(REACH, deep)):
            arrive(d, turns_in)
        if turns_in == [0]:
            for e in range(1, share):
                landed(seen.at[e], x_recv.at[far_at + (e - 1) * 2])
                fill_tops(tops, e - 1, e)
                relay(stats.at[(x - e + share) % share, pl.ds(c * own, own)],
                      far_at + (e - 1) * 2 + 1)
        relay_next()
        if late == 3:
            attend(done)
            done += 1
    for d in range(REACH, deep):
        arrive(d, range(kv_heads))
    relay_next()
    for k in range(done, deep):
        attend(k, relay_rest if k == deep - 1 else None)
    relay_rest()
    collect(turns - 1, batches[deep - 1])
    for d in range(1, share):
        lane = (x - d + share) % share
        for n in range(own):
            for t, part in enumerate(chunk_of(lane, 1 - c, n)):
                landed(part, core_recv.at[3 + x_slot(d, n, t)])
        landed(stats.at[lane, pl.ds((1 - c) * own, own)],
               core_recv.at[3 + far_at + (d - 1) * 2 + 1])
    for there, make in sent:
        when(there, functools.partial(lambda make: make().wait_send(), make))


def gather(queries, out_grad, attn_out, log_norm, keys, values, block_layout, document_ids,
           block_order, deep, kv_heads, share):
    rows = keys.shape[0]
    heads, q_rows = log_norm.shape
    blocks = block_order.shape[0]
    own = q_rows // BLOCK
    unit = min(rows, BLOCK)
    pieces = deep * kv_heads
    kv_rows = pieces * rows
    hbm = pl.BlockSpec(memory_space=pltpu.HBM)
    vmem = pl.BlockSpec(memory_space=pltpu.VMEM)
    lanes = share - 1
    x_copies = max(1, lanes * own * 2 + lanes * 2)
    kv_copies = 2 * kv_heads * (deep + REACH)
    dma = pltpu.SemaphoreType.DMA
    every = jax.ShapeDtypeStruct((share, CORES * q_rows, heads * D_HEAD), queries.dtype)
    return pl.pallas_call(
        functools.partial(gather_kernel, deep, kv_heads, share),
        out_shape=(
            jax.ShapeDtypeStruct((2, kv_rows, D_HEAD), keys.dtype),
            every,
            every,
            jax.ShapeDtypeStruct((share, CORES * own, 2 * heads, BLOCK), jnp.float32),
            jax.ShapeDtypeStruct((blocks, BLOCK), jnp.int32),
            jax.ShapeDtypeStruct(
                (kv_rows // unit, CORES * own, max(1, lanes) * heads * BLOCK), jnp.int32),
            jax.ShapeDtypeStruct((2, kv_rows, D_HEAD), jnp.float32),
            jax.ShapeDtypeStruct((CORES * own, D_HEAD, heads * BLOCK), jnp.float32),
        ),
        in_specs=[hbm] * 9,
        out_specs=(vmem,) * 8,
        scratch_shapes=[
            pltpu.VMEM((max(1, kv_heads - 1), 2, rows, D_HEAD), keys.dtype),
            pltpu.VMEM(attn_out.shape, attn_out.dtype),
            pltpu.VMEM(log_norm.shape, jnp.float32),
            pltpu.VMEM((blocks, BLOCK), jnp.int32),
            pltpu.SMEM((blocks,), jnp.int32),
            pltpu.VMEM(block_layout.shape, jnp.int32),
            pltpu.VMEM((share, heads, CORES * own, blocks), jnp.float32),
            pltpu.VMEM((kv_rows // unit, CORES * own, heads * BLOCK), jnp.int32),
            pltpu.VMEM((2, kv_heads * rows, SPAN * heads * BLOCK), jnp.bfloat16),
            dma((2 * kv_heads + 7,)),
            pltpu.SemaphoreType.REGULAR((REACH,)),
            dma((kv_copies,)),
            dma((pieces,)),
            dma((x_copies,)),
            dma((x_copies,)),
            dma((3 + x_copies,)),
            dma((3 + x_copies,)),
        ],
        compiler_params=pltpu.CompilerParams(collective_id=0, has_side_effects=True,
            vmem_limit_bytes=16 << 20),
        name="gather",
    )(*[pltpu.with_memory_space_constraint(array, pltpu.HBM) for array in (
        queries, out_grad, attn_out, log_norm, keys, values, block_layout,
        document_ids.reshape(blocks, BLOCK), block_order)])


def grads_kernel(
    kv_heads, share, rows, order_in, docs_in, q_all, do_all, stats, kv, lows, tops, acc_in,
    dqt, acc, order, docs, unit_pos, item_q, item_u, low_bits, local,
):
    z, c, g, x = place(share)
    queries = dqt.shape[1]
    heads = q_all.shape[2] // D_HEAD
    unit = min(rows, BLOCK)
    units = kv.shape[1] // unit
    first = z * queries
    others = [(x - d + share) % share for d in range(1, share)]
    pulls = [pltpu.make_async_copy(order_in, order, local.at[0]),
             pltpu.make_async_copy(docs_in, docs, local.at[1])]
    for pull in pulls:
        pull.start()
    acc[...] = acc_in[...]

    def clear(i, _):
        for s in range(share - 1):
            dqt[s, pl.ds(i, 1)] = jnp.zeros((1,) + dqt.shape[2:], jnp.float32)
        return 0

    lax.fori_loop(0, queries, clear, 0)
    for pull in pulls:
        pull.wait()

    for u in range(units):
        row = unit_row(u, unit, rows, kv_heads, share)
        unit_pos[u] = order[row // BLOCK] * BLOCK + row % BLOCK

    def listing(i, n):
        qb = order[first + i]
        doc = docs[qb * BLOCK]
        for u in range(units):
            pos = unit_pos[u]
            seen = (pos <= qb * BLOCK + BLOCK - 1) & (docs[pos + unit - 1] >= doc)
            item_q[n] = i
            item_u[n] = u
            n = n + seen.astype(jnp.int32)
        return n

    total = lax.fori_loop(0, queries, listing, 0)
    wide = (share - 1) * heads * BLOCK
    sub = lax.broadcasted_iota(jnp.int32, (unit, wide), 0)
    low_bits[...] = jnp.zeros_like(low_bits)
    for n in range(2 * PAIR):
        item_q[total + n] = 0
        item_u[total + n] = 0

    def stacked(ref, i):
        at = pl.ds(pl.multiple_of(i * BLOCK, BLOCK), BLOCK)
        return jnp.concatenate(
            [ref[s, at, h * D_HEAD:(h + 1) * D_HEAD] for s in others for h in range(heads)],
            axis=0)

    def weigh(n, slot):
        i, u = item_q[n], item_u[n]
        pos = unit_pos[u]
        at = pl.ds(pl.multiple_of(u * unit, unit), unit)
        k, v = kv[0, at, :], kv[1, at, :]
        q4, do4 = stacked(q_all, i), stacked(do_all, i)
        rowed = [stats[s, i] for s in others]
        norm = jnp.concatenate([r[h:h + 1] for r in rowed for h in range(heads)], axis=1)
        delta = jnp.concatenate(
            [r[heads + h:heads + h + 1] for r in rowed for h in range(heads)], axis=1)
        low = jnp.concatenate([lows[pl.ds(order[first + i], 1), :]] * ((share - 1) * heads), axis=1)
        top = jnp.where(n < total, tops[u, pl.ds(i, 1), :], -1)
        keep = (sub >= low - pos) & (sub <= top - pos)
        st = lax.dot_general(k, q4, NT, preferred_element_type=jnp.float32)
        dpt = lax.dot_general(v, do4, NT, preferred_element_type=jnp.float32)
        w = jnp.where(keep, jnp.exp2(st * (SCALE * LOG2E) - norm), 0.0)
        low_bits[slot, 0] = w.astype(jnp.bfloat16)
        low_bits[slot, 1] = (w * (dpt - delta)).astype(jnp.bfloat16)

    def collect(n, slot):
        i, u = item_q[n], item_u[n]
        at = pl.ds(pl.multiple_of(u * unit, unit), unit)
        q4, do4 = stacked(q_all, i), stacked(do_all, i)
        ds = low_bits[slot, 1]
        dv = jnp.dot(low_bits[slot, 0], do4, preferred_element_type=jnp.float32)
        dk = jnp.dot(ds, q4, preferred_element_type=jnp.float32)
        dq = lax.dot_general(kv[0, at, :], ds, TN, preferred_element_type=jnp.float32)
        return i, at, dk, dv, dq

    def step(t, _):
        before = jnp.maximum(t - 1, 0) * PAIR
        done = [collect(before + n, n) for n in range(PAIR)]
        for n in range(PAIR):
            weigh(t * PAIR + n, n)
        for i, at, dk, dv, dq in done:
            acc[0, at, :] += dk
            acc[1, at, :] += dv
            for s in range(share - 1):
                dqt[s, i] += dq[:, s * heads * BLOCK:(s + 1) * heads * BLOCK]
        return 0

    lax.fori_loop(0, (total + PAIR - 1) // PAIR + 1, step, 0)


def local_grads(block_order, document_ids, q_all, do_all, stats, kv, lows, tops, acc, rows,
                kv_heads, share):
    heads = q_all.shape[2] // D_HEAD
    units, queries = tops.shape[:2]
    hbm = pl.BlockSpec(memory_space=pltpu.HBM)
    vmem = pl.BlockSpec(memory_space=pltpu.VMEM)
    return pl.pallas_call(
        functools.partial(grads_kernel, kv_heads, share, rows),
        out_shape=(
            jax.ShapeDtypeStruct((share - 1, queries, D_HEAD, heads * BLOCK), jnp.float32),
            jax.ShapeDtypeStruct(kv.shape, jnp.float32),
        ),
        in_specs=[hbm] * 2 + [vmem] * 7,
        out_specs=(vmem, vmem),
        scratch_shapes=[
            pltpu.SMEM(block_order.shape, jnp.int32),
            pltpu.SMEM(document_ids.shape, jnp.int32),
            pltpu.SMEM((units,), jnp.int32),
            pltpu.SMEM((queries * units + 2 * PAIR,), jnp.int32),
            pltpu.SMEM((queries * units + 2 * PAIR,), jnp.int32),
            pltpu.VMEM((PAIR, 2, min(rows, BLOCK), (share - 1) * heads * BLOCK),
                       jnp.bfloat16),
            pltpu.SemaphoreType.DMA((2,)),
        ],
        compiler_params=pltpu.CompilerParams(vmem_limit_bytes=24 << 20),
        name="grads",
    )(pltpu.with_memory_space_constraint(block_order, pltpu.HBM),
      pltpu.with_memory_space_constraint(document_ids, pltpu.HBM),
      q_all, do_all, stats, kv, lows, tops, acc)


def scatter_kernel(
    deep, kv_heads, share, rows, acc, dq_own, dqt, kv_in, dq_sum, dq_in,
    kv_out, joined, own_core, dq_core, dq_out, ready, kv_send, kv_recv, join_recv, core_send, core_recv,
    x_send, x_recv,
):
    z, c, g, x = place(share)
    seq, head = z * CORES + c, g * share + x
    partner = z * CORES + 1 - c
    own = dqt.shape[1] // CORES
    heads = dqt.shape[3] // BLOCK
    mine = z * kv_heads + g
    peers = near(deep, kv_heads, share)
    barrier = pltpu.get_barrier_semaphore()
    signal(barrier, peers)
    for p in range(deep * kv_heads):
        part = slice(p * rows, (p + 1) * rows)
        kv_out[p, 0] = (acc[0, part, :] * SCALE).astype(jnp.bfloat16)
        kv_out[p, 1] = acc[1, part, :].astype(jnp.bfloat16)
    kv_in[mine] = kv_out[mine]
    for depth in range(deep):
        def unused(depth=depth):
            at = pl.ds(depth * kv_heads, kv_heads)
            kv_in[at] = jnp.zeros((kv_heads,) + kv_in.shape[1:], kv_in.dtype)

        if depth >= REACH or depth < deep - REACH:
            pl.when((depth - z >= REACH) | (z - depth >= REACH))(unused)
    pl.semaphore_wait(barrier, count(peers))

    sent = []

    def send(make, there=True):
        sent.append((there, make))
        when(there, lambda: make().start())

    slots = [0]

    def slot_of():
        slots[0] += 1
        return slots[0] - 1

    def inside(depth):
        return (depth >= 0) & (depth < deep)

    def give(step, turn, there=True):
        slot = slot_of()
        depth, group = z + step, (g + turn) % kv_heads
        index = depth * kv_heads + group
        send(functools.partial(remote, kv_out.at[index], kv_in.at[mine], kv_send.at[slot],
                               kv_recv.at[mine], depth * CORES + c, group * share + x), there)

    def join(index):
        landed(joined.at[index], join_recv.at[index])
        at = span(index, rows)
        for n, factor in enumerate((SCALE, 1.0)):
            kv_out[index, n] = (acc[n, at, :] * factor
                                + joined[index, n].astype(jnp.float32)).astype(jnp.bfloat16)

    def crossing(core, n):
        at = pl.ds(core * own + n, 1)
        return ((dqt.at[:, at], dq_core.at[:, pl.ds(n, 1)]), (dq_own.at[at], own_core.at[pl.ds(n, 1)]))

    for far in range(deep - 1, REACH - 1, -1):
        for depth, step in ((far, 1), (deep - 1 - far, -1)):
            away = (depth - z) * step >= REACH
            behind = (z > 0) if step == 1 else (z + 1 < deep)
            for turn in range(kv_heads):
                index = depth * kv_heads + (g + turn) % kv_heads
                if far > REACH:
                    pl.when(away & behind)(functools.partial(join, index))
                slot = slot_of()
                send(functools.partial(remote, kv_out.at[index], joined.at[index],
                                       kv_send.at[slot], join_recv.at[index],
                                       (z + step) * CORES + c, head), away)
    if deep > 1:
        give(1, 0, z + 1 < deep)
        give(-1, 0, z > 0)
    for turn in range(1, kv_heads):
        give(0, turn)
    for n in range(own):
        for m, (src, dst) in enumerate(crossing(1 - c, n)):
            send(functools.partial(remote, src, dst, core_send.at[2 * n + m],
                                   core_recv.at[2 * n + m], partner, head))
    along = peers[-2:] if deep > 1 else []
    near_end = {1: z == 0, -1: z == deep - 1}
    for d in range(1, min(REACH, deep)):
        signal(ready.at[d - 1], along)
        pl.semaphore_wait(ready.at[d - 1], count(along))
        for step in (1, -1):
            for turn in range(1, kv_heads):
                there = inside(z + step * d)
                give(step * d, turn, there & near_end[step] if d == REACH - 1 else there)
            if d + 1 < min(REACH, deep):
                there = inside(z + step * (d + 1))
                give(step * (d + 1), 0, there & near_end[step] if d == REACH - 2 else there)

    def query_block(n):
        for m, (_, dst) in enumerate(crossing(1 - c, n)):
            landed(dst, core_recv.at[2 * n + m])
        at = slice(n * BLOCK, (n + 1) * BLOCK)
        for d in range(share - 1, -1, -1):
            lane = (x - d + share) % share
            if d:
                total = (dqt[d - 1, c * own + n] + dq_core[d - 1, n]) * SCALE
            else:
                total = (dq_own[c * own + n] + own_core[n]) * SCALE
            for h in range(heads):
                flat = total[:, h * BLOCK:(h + 1) * BLOCK].T
                if d:
                    dq_out[d - 1, at, h * D_HEAD:(h + 1) * D_HEAD] = flat.astype(jnp.bfloat16)
                else:
                    dq_sum[at, h * D_HEAD:(h + 1) * D_HEAD] = flat
            if d:
                slot = (d - 1) * own + n
                send(functools.partial(
                    remote, dq_out.at[d - 1, at, :], dq_in.at[d - 1, at, :], x_send.at[slot],
                    x_recv.at[slot], seq, g * share + lane))

    early = min(2, own)
    for n in range(early):
        query_block(n)
    if deep >= REACH:
        for turn in range(kv_heads):
            for step in (1, -1):
                depth = z + step * (REACH - 1)
                there = inside(depth) & ~near_end[step]
                index = depth * kv_heads + (g + turn) % kv_heads
                pl.when(there)(functools.partial(join, index))
                give(step * (REACH - 1), turn, there)
    for n in range(early, own):
        query_block(n)
    for depth in range(deep):
        for turn in range(kv_heads):
            index = depth * kv_heads + (g + turn) % kv_heads
            close = (depth - z < REACH) & (z - depth < REACH)
            get = functools.partial(
                lambda index: landed(kv_in.at[index], kv_recv.at[index]), index)
            when(close if turn else close & (depth != z), get)
    for d in range(1, share):
        for n in range(own):
            at = slice(n * BLOCK, (n + 1) * BLOCK)
            landed(dq_in.at[d - 1, at, :], x_recv.at[(d - 1) * own + n])
    for there, make in sent:
        when(there, functools.partial(lambda make: make().wait_send(), make))


def finish_kernel(deep, kv_heads, share, kv_in, dq_sum, dq_in, dq, dk, dv):
    total = dq_sum[...]
    for d in range(share - 1):
        total += dq_in[d].astype(jnp.float32)
    dq[...] = total
    for j in range(kv_heads):
        for n, ref in enumerate((dk, dv)):
            total = kv_in[j, n].astype(jnp.float32)
            for depth in range(1, deep):
                total += kv_in[depth * kv_heads + j, n].astype(jnp.float32)
            ref[:, j * D_HEAD:(j + 1) * D_HEAD] = total


def scatter(dq_own, dqt, acc, rows, deep, kv_heads, share):
    pieces = deep * kv_heads
    queries, heads = dqt.shape[1], dqt.shape[3] // BLOCK
    own = queries // CORES
    q_rows = own * BLOCK
    vmem = pl.BlockSpec(memory_space=pltpu.VMEM)
    dma = pltpu.SemaphoreType.DMA
    lanes = max(1, share - 1)
    kv_in, dq_sum, dq_in = pl.pallas_call(
        functools.partial(scatter_kernel, deep, kv_heads, share, rows),
        out_shape=(
            jax.ShapeDtypeStruct((pieces, 2, rows, D_HEAD), jnp.bfloat16),
            jax.ShapeDtypeStruct((q_rows, heads * D_HEAD), jnp.float32),
            jax.ShapeDtypeStruct((lanes, q_rows, heads * D_HEAD), jnp.bfloat16),
        ),
        in_specs=[vmem] * 3,
        out_specs=(vmem,) * 3,
        scratch_shapes=[
            pltpu.VMEM((pieces, 2, rows, D_HEAD), jnp.bfloat16),
            pltpu.VMEM((pieces, 2, rows, D_HEAD), jnp.bfloat16),
            pltpu.VMEM((own,) + dqt.shape[2:], jnp.float32),
            pltpu.VMEM((dqt.shape[0], own) + dqt.shape[2:], jnp.float32),
            pltpu.VMEM((lanes, q_rows, heads * D_HEAD), jnp.bfloat16),
            pltpu.SemaphoreType.REGULAR((max(1, deep - 1),)),
            dma((6 * pieces,)),
            dma((pieces,)),
            dma((pieces,)),
            dma((2 * own,)),
            dma((2 * own,)),
            dma((lanes * own,)),
            dma((lanes * own,)),
        ],
        compiler_params=pltpu.CompilerParams(collective_id=1, has_side_effects=True,
            vmem_limit_bytes=20 << 20),
        name="scatter",
    )(acc, dq_own, dqt)
    grad = jax.ShapeDtypeStruct((rows, kv_heads * D_HEAD), jnp.float32)
    return pl.pallas_call(
        functools.partial(finish_kernel, deep, kv_heads, share),
        out_shape=(jax.ShapeDtypeStruct(dq_sum.shape, jnp.float32), grad, grad),
        in_specs=[vmem] * 3,
        out_specs=(vmem,) * 3,
        compiler_params=pltpu.CompilerParams(vmem_limit_bytes=8 << 20),
        name="finish",
    )(kv_in, dq_sum, dq_in)


def body(
    queries, keys, values, attn_out, out_grad, log_norm, block_layout, document_ids, block_order
):
    share = GROUP // log_norm.shape[0]
    kv_heads = lax.axis_size("head") // share
    deep = lax.axis_size("seq") // CORES
    rows = keys.shape[0]
    kv, q_all, do_all, stats, lows, tops, acc, dq_own = gather(
        queries, out_grad, attn_out, log_norm, keys, values, block_layout, document_ids,
        block_order, deep, kv_heads, share)
    dqt, acc = local_grads(block_order, document_ids, q_all, do_all, stats, kv, lows, tops, acc,
                           rows, kv_heads, share)
    return tuple(scatter(dq_own, dqt, acc, rows, deep, kv_heads, share))


def solution(mesh):
    in_specs = (
        P("seq", "head"),
        P(("seq", "head"), None),
        P(("seq", "head"), None),
        P("seq", "head"),
        P("seq", "head"),
        P("head", "seq"),
        P("head", None, None),
        P(),
        P(),
    )
    out_specs = (P("seq", "head"), P(("seq", "head"), None), P(("seq", "head"), None))
    return jax.shard_map(body, mesh=mesh, in_specs=in_specs, out_specs=out_specs, check_vma=False)
```

```python
import functools
import math

import jax
import jax.numpy as jnp
from jax import lax
from jax.experimental import pallas as pl
from jax.experimental.pallas import tpu as pltpu
from jax.sharding import PartitionSpec as P

D_HEAD = 128
GROUP = 4
BLOCK = 128
DOCS = 8
CORES = 2
PAIR = 4
SPAN = 2
REACH = 3
WORD = 16
LOG2E = math.log2(math.e)
SCALE = D_HEAD ** -0.5
NT = (((1,), (1,)), ((), ()))
TN = (((0,), (0,)), ((), ()))


def place(share):
    seq, head = lax.axis_index("seq"), lax.axis_index("head")
    return seq // CORES, seq % CORES, head // share, head % share


def remote(src, dst, send, recv, seq, head):
    return pltpu.make_async_remote_copy(
        src_ref=src, dst_ref=dst, send_sem=send, recv_sem=recv,
        device_id={"seq": seq, "head": head}, device_id_type=pl.DeviceIdType.MESH)


def landed(where, sem):
    pltpu.make_async_copy(where, where, sem).wait()


def when(there, run):
    if there is True:
        run()
    else:
        pl.when(there)(run)


def span(index, rows):
    return pl.ds(pl.multiple_of(index * rows, rows), rows)


def near(deep, kv_heads, share):
    z, c, g, x = place(share)
    seq, head = z * CORES + c, g * share + x
    peers = [(z * CORES + (c + d) % CORES, head, True) for d in range(1, CORES)]
    peers += [(seq, g * share + (x + d) % share, True) for d in range(1, share)]
    peers += [(seq, (g + d) % kv_heads * share + x, True) for d in range(1, kv_heads)]
    if deep > 1:
        peers += [(seq + CORES, head, z + 1 < deep), (seq - CORES, head, z > 0)]
    return peers


def signal(sem, peers):
    for seq, head, there in peers:
        when(there, lambda: pl.semaphore_signal(
            sem, inc=1, device_id={"seq": seq, "head": head},
            device_id_type=pl.DeviceIdType.MESH))


def count(peers):
    total = 0
    for _, _, there in peers:
        total = total + (1 if there is True else there.astype(jnp.int32))
    return total


def unit_row(u, unit, rows, kv_heads, share):
    z, c, g, x = place(share)
    per = rows // unit
    piece, sub = u // per, u % per
    depth, group = piece // kv_heads, piece % kv_heads
    owner = (depth * CORES + c) * kv_heads * share + group * share + x
    return owner * rows + sub * unit


def gather_kernel(
    deep, kv_heads, share, q_in, do_in, o_in, ln_in, k_in, v_in, lay_in, docs_in, order_in,
    kv, qd, stats, lows, tops, flags, acc, dq_own,
    stage, o_buf, ln_buf, docs, order, layout, seen, own_tops, low_bits,
    local, ready, kv_send, kv_recv, x_send, x_recv, core_send, core_recv,
):
    z, c, g, x = place(share)
    seq, head = z * CORES + c, g * share + x
    heads, q_rows = ln_in.shape
    rows = k_in.shape[0]
    own = q_rows // BLOCK
    unit = min(rows, BLOCK)
    mine = z * kv_heads + g

    def cols(index):
        return pl.ds(pl.multiple_of(index * D_HEAD, D_HEAD), D_HEAD)

    here = span(c, q_rows)
    head_rows = pl.ds(c * q_rows, BLOCK)
    tail_rows = pl.ds(c * q_rows + BLOCK, q_rows - BLOCK)
    pulls = [(ref.at[pl.ds(0, BLOCK), :], qd.at[x, n, head_rows, :])
             for n, ref in enumerate((q_in, do_in))]
    pulls += [(k_in.at[:, cols(g)], kv.at[0, span(mine, rows), :]),
              (v_in.at[:, cols(g)], kv.at[1, span(mine, rows), :])]
    for d in range(1, kv_heads):
        other = cols((g + d) % kv_heads)
        pulls += [(k_in.at[:, other], stage.at[d - 1, 0]), (v_in.at[:, other], stage.at[d - 1, 1])]
    urgent = len(pulls)
    if own > 1:
        pulls += [(ref.at[pl.ds(BLOCK, q_rows - BLOCK), :], qd.at[x, n, tail_rows, :])
                  for n, ref in enumerate((q_in, do_in))]
    pulls += [(order_in, order), (lay_in, layout), (o_in, o_buf), (ln_in, ln_buf), (docs_in, docs)]
    pulls = [pltpu.make_async_copy(src, dst, local.at[n]) for n, (src, dst) in enumerate(pulls)]
    for pull in pulls:
        pull.start()
    peers = near(deep, kv_heads, share)
    barrier = pltpu.get_barrier_semaphore()
    signal(barrier, peers)
    for pull in pulls[:urgent]:
        pull.wait()
    pl.semaphore_wait(barrier, count(peers))

    sent = []

    def send(make, there=True):
        sent.append((there, make))
        when(there, lambda: make().start())

    kv_slots = [0]

    def send_kv(src, dst, arrival, to_seq, to_head, there=True):
        slot = kv_slots[0]
        kv_slots[0] += 1
        send(lambda: remote(src, dst, kv_send.at[slot], arrival, to_seq, to_head), there)

    def whole(index):
        return kv.at[:, span(index, rows), :]

    def onward(index, step, there):
        send_kv(whole(index), whole(index), kv_recv.at[index], seq + step * CORES, head, there)

    def reach(index, step):
        there = inside(z + step)
        send_kv(whole(index), whole(index), kv_recv.at[index], seq + step * CORES, head, there)

    def inside(depth):
        return (depth >= 0) & (depth < deep)

    for turn in range(1, kv_heads):
        send_kv(stage.at[turn - 1], whole(mine), kv_recv.at[mine], seq,
                (g + turn) % kv_heads * share + x)
    along = peers[-2:] if deep > 1 else []
    if deep > 1:
        reach(mine, 1)
        reach(mine, -1)
        signal(ready.at[0], along)

    def chunk_of(lane, core, n):
        return qd.at[lane, :, pl.ds(core * q_rows + n * BLOCK, BLOCK), :]

    def send_chunk(n):
        for d in range(1, share):
            part, slot = chunk_of(x, c, n), (d - 1) * own + n
            send(functools.partial(remote, part, part, x_send.at[slot], x_recv.at[slot], seq,
                                   g * share + (x + d) % share))

    stats_at = (share - 1) * own
    seen_at = stats_at + share - 1
    send_chunk(0)
    for pull in pulls[urgent:-3]:
        pull.wait()
    partner = z * CORES + 1 - c
    mine_rows = qd.at[x, :, here, :]
    send(functools.partial(remote, mine_rows, mine_rows, core_send.at[0], core_recv.at[0],
                           partner, head))
    queries, blocks = CORES * own, order.shape[0]
    units = own_tops.shape[0]
    row_of = lax.broadcasted_iota(jnp.int32, (queries, BLOCK), 0)
    at_block = jnp.zeros((queries, BLOCK), jnp.int32)
    for i in range(queries):
        at_block = jnp.where(row_of == i, order[z * queries + i], at_block)
    column = lax.broadcasted_iota(jnp.int32, (queries, blocks), 1)
    picked = jnp.where(column == at_block[:, :blocks], 1.0, 0.0).astype(jnp.bfloat16)
    for h in range(heads):
        seen[0, h] = jnp.dot(picked, layout[h].astype(jnp.float32).astype(jnp.bfloat16),
                             preferred_element_type=jnp.float32)
    for d in range(1, share):
        slot = seen_at + d - 1
        send(functools.partial(remote, seen.at[0], seen.at[d], x_send.at[slot], x_recv.at[slot],
                               seq, g * share + (x + d) % share))
    for d in range(1, min(REACH, deep) - 1):
        pl.semaphore_wait(ready.at[d - 1], count(along))
        if d + 2 < min(REACH, deep):
            signal(ready.at[d], along)
        reach(mine, d + 1)
        reach(mine, -d - 1)
    for pull in pulls[-3:]:
        pull.wait()
    mine_stats = stats.at[x, pl.ds(c * own, own)]
    for n in range(own):
        part = slice(n * BLOCK, (n + 1) * BLOCK)
        at = pl.ds(c * q_rows + n * BLOCK, BLOCK)
        for h in range(heads):
            lanes = slice(h * D_HEAD, (h + 1) * D_HEAD)
            product = (qd[x, 1, at, lanes].astype(jnp.float32)
                       * o_buf[part, lanes].astype(jnp.float32))
            stats[x, c * own + n, h:h + 1, :] = ln_buf[h:h + 1, part] * LOG2E
            stats[x, c * own + n, heads + h:heads + h + 1, :] = jnp.sum(
                product.T, axis=0, keepdims=True)
    for d in range(1, share):
        slot = stats_at + d - 1
        send(functools.partial(remote, mine_stats, mine_stats, x_send.at[slot], x_recv.at[slot],
                               seq, g * share + (x + d) % share))
    send(functools.partial(remote, mine_stats, mine_stats, core_send.at[1], core_recv.at[1],
                           partner, head))
    for n in range(1, own):
        send_chunk(n)

    block_of = lax.broadcasted_iota(jnp.int32, (blocks, BLOCK), 0)
    stored = [unit_row(u, unit, rows, kv_heads, share) for u in range(units)]
    kept = [order[row // BLOCK] for row in stored]
    starts = [block * BLOCK + row % BLOCK for block, row in zip(kept, stored)]
    chosen = jnp.concatenate([jnp.where(block_of == block, 1.0, 0.0) for block in kept],
                             axis=1).astype(jnp.bfloat16)
    at_query = at_block * BLOCK + lax.broadcasted_iota(jnp.int32, (queries, BLOCK), 1)

    def fill_tops(ref, slot, source):
        for h in range(heads):
            on = jnp.dot(seen[source, h].astype(jnp.bfloat16), chosen,
                         preferred_element_type=jnp.float32)
            at = slice((slot * heads + h) * BLOCK, (slot * heads + h + 1) * BLOCK)
            for u in range(units):
                ref[u, :, at] = jnp.where(on[:, u * BLOCK:(u + 1) * BLOCK] > 0.5, at_query - starts[u], -1)

    ids = docs[...]
    low = jnp.zeros_like(ids)
    for d in range(1, DOCS):
        before = jnp.sum(jnp.where(ids < d, 1.0, 0.0), axis=1, keepdims=True)
        before = jnp.sum(before, axis=0, keepdims=True).astype(jnp.int32)
        low = jnp.where(ids >= d, before, low)
    docs[...] = low
    first = jnp.concatenate(
        [docs[pl.ds(order[z * queries + i], 1), :] for i in range(queries)], axis=0)
    lane_of = lax.broadcasted_iota(jnp.int32, (queries, BLOCK), 1)
    start = jnp.zeros((queries, BLOCK), jnp.int32)
    for u in range(units):
        lows[u] = first - starts[u]
        start = jnp.where(lane_of == u, starts[u], start)
    flags[...] = jnp.where(
        (lane_of < units) & (start < (at_block + 1) * BLOCK) & (first[:, :1] < start + unit),
        1.0, 0.0)
    fill_tops(own_tops, 0, 0)
    acc[...] = jnp.zeros_like(acc)
    dq_own[...] = jnp.zeros_like(dq_own)
    low_bits[...] = jnp.zeros_like(low_bits)

    sub = lax.broadcasted_iota(jnp.int32, (unit, SPAN * heads * BLOCK), 0)
    both = [(j, h) for j in range(SPAN) for h in range(heads)]

    def stacked(n, t):
        return jnp.concatenate(
            [qd[x, n, pl.ds(pl.multiple_of((t * SPAN + j) * BLOCK, BLOCK), BLOCK),
                 h * D_HEAD:(h + 1) * D_HEAD] for j, h in both], axis=0)

    def joint(n, batch):
        return jnp.concatenate([kv[n, span(index, rows), :] for index in batch], axis=0)

    def weigh(t, batch):
        st = lax.dot_general(joint(0, batch), stacked(0, t), NT,
                             preferred_element_type=jnp.float32)
        dpt = lax.dot_general(joint(1, batch), stacked(1, t), NT,
                              preferred_element_type=jnp.float32)
        rowed = [stats[x, t * SPAN + j] for j in range(SPAN)]
        norm = jnp.concatenate([rowed[j][h:h + 1] for j, h in both], axis=1)
        delta = jnp.concatenate([rowed[j][heads + h:heads + h + 1] for j, h in both], axis=1)
        keeps = []
        for u in [index * (rows // unit) + n for index in batch for n in range(rows // unit)]:
            rowed_low = [lows[u, pl.ds(t * SPAN + j, 1), :] for j in range(SPAN)]
            low = jnp.concatenate([rowed_low[j] for j, _ in both], axis=1)
            top = jnp.concatenate(
                [own_tops[u, pl.ds(t * SPAN + j, 1), :] for j in range(SPAN)], axis=1)
            keeps.append((sub >= low) & (sub <= top))
        keep = jnp.concatenate(keeps, axis=0)
        w = jnp.where(keep, jnp.exp2(st * (SCALE * LOG2E) - norm), 0.0)
        low_bits[0] = w.astype(jnp.bfloat16)
        low_bits[1] = (w * (dpt - delta)).astype(jnp.bfloat16)

    def collect(t, batch):
        ds = low_bits[1]
        dv = jnp.dot(low_bits[0], stacked(1, t), preferred_element_type=jnp.float32)
        dk = jnp.dot(ds, stacked(0, t), preferred_element_type=jnp.float32)
        dq = lax.dot_general(joint(0, batch), ds, TN, preferred_element_type=jnp.float32)
        for n, index in enumerate(batch):
            at, part = span(index, rows), slice(n * rows, (n + 1) * rows)
            acc[0, at, :] += dk[part]
            acc[1, at, :] += dv[part]
        for j in range(SPAN):
            dq_own[t * SPAN + j] += dq[:, j * heads * BLOCK:(j + 1) * heads * BLOCK]

    turns = queries // SPAN

    def nearest(k):
        short = jnp.minimum(z, deep - 1 - z)
        beyond = jnp.where(z < deep - 1 - z, k, deep - 1 - k)
        return jnp.where(k <= 2 * short, z + (k + 1) // 2 * (1 - 2 * (k % 2)), beyond)

    def of(k, turn):
        return nearest(k) * kv_heads + (g + turn) % kv_heads

    order_of = [[(0, turn) for turn in range(kv_heads)]]
    late = 1
    if kv_heads == 2 and deep > 2:
        order_of += [[(1, turn), (2, turn)] for turn in range(kv_heads)]
        late = 3
    order_of += [[(k, turn) for turn in range(kv_heads)] for k in range(late, deep)]
    batches = [[of(*entry) for entry in batch] for batch in order_of]

    def attend(k, midway=None):
        batch, before = batches[k], batches[max(k - 1, 0)]

        def turn(t, _):
            first = t == 0
            collect(jnp.where(first, 0 if k == 0 else turns - 1, t - 1),
                    [jnp.where(first, old, new) for old, new in zip(before, batch)])
            weigh(t, batch)
            return 0

        lax.fori_loop(0, turns // 2, turn, 0)
        if midway is not None:
            midway()
        lax.fori_loop(turns // 2, turns, turn, 0)

    def relay(part, slot):
        landed(part, x_recv.at[slot])
        send(functools.partial(remote, part, part, core_send.at[2 + slot],
                               core_recv.at[2 + slot], partner, head))

    def relay_chunk(n):
        for d in range(1, share):
            relay(chunk_of((x - d + share) % share, c, n), (d - 1) * own + n)

    for j in range(1, kv_heads):
        index = z * kv_heads + (g + j) % kv_heads
        landed(whole(index), kv_recv.at[index])
        for d in range(1, min(REACH, deep)):
            reach(index, d)
            reach(index, -d)
    there = span(1 - c, q_rows)
    landed(qd.at[x, :, there, :], core_recv.at[0])
    landed(stats.at[x, pl.ds((1 - c) * own, own)], core_recv.at[1])
    attend(0)

    def arrive(d, turns_in):
        for turn in turns_in:
            for depth, step in ((z - d, 1), (z + d, -1)):
                index = depth * kv_heads + (g + turn) % kv_heads
                when(inside(depth), functools.partial(
                    lambda index: landed(whole(index), kv_recv.at[index]), index))
                if REACH - 1 <= d < deep - 1:
                    onward(index, step, inside(depth) & inside(z + step))

    chunks = list(range(own))

    def relay_next():
        if chunks:
            relay_chunk(chunks.pop(0))

    def relay_rest():
        while chunks:
            relay_chunk(chunks.pop(0))

    done = 1
    for turns_in in ([0], list(range(1, kv_heads))):
        for d in range(1, min(REACH, deep)):
            arrive(d, turns_in)
        if turns_in == [0]:
            for e in range(1, share):
                landed(seen.at[e], x_recv.at[seen_at + e - 1])
                fill_tops(tops, e - 1, e)
                relay(stats.at[(x - e + share) % share, pl.ds(c * own, own)], stats_at + e - 1)
        relay_next()
        if late == 3:
            attend(done)
            done += 1
    for d in range(REACH, deep):
        arrive(d, range(kv_heads))
    relay_next()
    for k in range(done, deep):
        attend(k, relay_rest if k == deep - 1 else None)
    relay_rest()
    collect(turns - 1, batches[deep - 1])
    for d in range(1, share):
        lane = (x - d + share) % share
        for n in range(own):
            landed(chunk_of(lane, 1 - c, n), core_recv.at[2 + (d - 1) * own + n])
        landed(stats.at[lane, pl.ds((1 - c) * own, own)], core_recv.at[2 + stats_at + d - 1])
    for there, make in sent:
        when(there, functools.partial(lambda make: make().wait_send(), make))


def gather(queries, out_grad, attn_out, log_norm, keys, values, block_layout, document_ids,
           block_order, deep, kv_heads, share):
    rows = keys.shape[0]
    heads, q_rows = log_norm.shape
    blocks = block_order.shape[0]
    own = q_rows // BLOCK
    unit = min(rows, BLOCK)
    pieces = deep * kv_heads
    kv_rows = pieces * rows
    hbm = pl.BlockSpec(memory_space=pltpu.HBM)
    vmem = pl.BlockSpec(memory_space=pltpu.VMEM)
    lanes = share - 1
    x_copies = max(1, lanes * (own + 2))
    steps = min(REACH, deep) - 1
    kv_copies = max(1, kv_heads - 1 + 2 * kv_heads * (steps + max(0, deep - REACH)))
    dma = pltpu.SemaphoreType.DMA
    return pl.pallas_call(
        functools.partial(gather_kernel, deep, kv_heads, share),
        out_shape=(
            jax.ShapeDtypeStruct((2, kv_rows, D_HEAD), keys.dtype),
            jax.ShapeDtypeStruct((share, 2, CORES * q_rows, heads * D_HEAD), queries.dtype),
            jax.ShapeDtypeStruct((share, CORES * own, 2 * heads, BLOCK), jnp.float32),
            jax.ShapeDtypeStruct((kv_rows // unit, CORES * own, BLOCK), jnp.int32),
            jax.ShapeDtypeStruct(
                (kv_rows // unit, CORES * own, max(1, lanes) * heads * BLOCK), jnp.int32),
            jax.ShapeDtypeStruct((CORES * own, BLOCK), jnp.float32),
            jax.ShapeDtypeStruct((2, kv_rows, D_HEAD), jnp.float32),
            jax.ShapeDtypeStruct((CORES * own, D_HEAD, heads * BLOCK), jnp.float32),
        ),
        in_specs=[hbm] * 9,
        out_specs=(vmem,) * 8,
        scratch_shapes=[
            pltpu.VMEM((max(1, kv_heads - 1), 2, rows, D_HEAD), keys.dtype),
            pltpu.VMEM(attn_out.shape, attn_out.dtype),
            pltpu.VMEM(log_norm.shape, jnp.float32),
            pltpu.VMEM((blocks, BLOCK), jnp.int32),
            pltpu.SMEM((blocks,), jnp.int32),
            pltpu.VMEM(block_layout.shape, jnp.int32),
            pltpu.VMEM((share, heads, CORES * own, blocks), jnp.float32),
            pltpu.VMEM((kv_rows // unit, CORES * own, heads * BLOCK), jnp.int32),
            pltpu.VMEM((2, kv_heads * rows, SPAN * heads * BLOCK), jnp.bfloat16),
            dma((2 * kv_heads + (9 if own > 1 else 7),)),
            pltpu.SemaphoreType.REGULAR((max(1, steps - 1),)),
            dma((kv_copies,)),
            dma((pieces,)),
            dma((x_copies,)),
            dma((x_copies,)),
            dma((2 + x_copies - lanes,)),
            dma((2 + x_copies - lanes,)),
        ],
        compiler_params=pltpu.CompilerParams(collective_id=0, has_side_effects=True,
            vmem_limit_bytes=16 << 20),
        name="gather",
    )(*[pltpu.with_memory_space_constraint(array, pltpu.HBM) for array in (
        queries, out_grad, attn_out, log_norm, keys, values, block_layout,
        document_ids.reshape(blocks, BLOCK), block_order)])


def grads_kernel(
    kv_heads, share, rows, qd, stats, kv, lows, tops, flags, acc_in,
    dqt, acc, items, low_bits,
):
    x = place(share)[3]
    queries = dqt.shape[1]
    heads = qd.shape[3] // D_HEAD
    unit = min(rows, BLOCK)
    units = kv.shape[1] // unit
    others = [(x - d + share) % share for d in range(1, share)]
    lane_of = lax.broadcasted_iota(jnp.int32, (1, BLOCK), 1)
    marks = [jnp.zeros((1, BLOCK), jnp.float32) for _ in range(0, units, WORD)]
    for u in range(units):
        marks[u // WORD] = jnp.where(lane_of == u, float(1 << u % WORD), marks[u // WORD])
    words = [[jnp.sum(flags[i:i + 1, :] * mark).astype(jnp.int32) for mark in marks]
             for i in range(queries)]
    acc[...] = acc_in[...]

    def clear(i, _):
        for s in range(share - 1):
            dqt[s, pl.ds(i, 1)] = jnp.zeros((1,) + dqt.shape[2:], jnp.float32)
        return 0

    lax.fori_loop(0, queries, clear, 0)
    total = jnp.int32(0)
    for i in range(queries):
        for u in range(units):
            items[total] = i * units + u
            total = total + ((words[i][u // WORD] >> (u % WORD)) & 1)
    wide = (share - 1) * heads * BLOCK
    sub = lax.broadcasted_iota(jnp.int32, (unit, wide), 0)
    low_bits[...] = jnp.zeros_like(low_bits)
    for n in range(2 * PAIR):
        items[total + n] = 0

    def stacked(n, i):
        at = pl.ds(pl.multiple_of(i * BLOCK, BLOCK), BLOCK)
        return jnp.concatenate(
            [qd[s, n, at, h * D_HEAD:(h + 1) * D_HEAD] for s in others for h in range(heads)],
            axis=0)

    def weigh(n, slot):
        i, u = items[n] // units, items[n] % units
        at = pl.ds(pl.multiple_of(u * unit, unit), unit)
        k, v = kv[0, at, :], kv[1, at, :]
        q4, do4 = stacked(0, i), stacked(1, i)
        rowed = [stats[s, i] for s in others]
        norm = jnp.concatenate([r[h:h + 1] for r in rowed for h in range(heads)], axis=1)
        delta = jnp.concatenate(
            [r[heads + h:heads + h + 1] for r in rowed for h in range(heads)], axis=1)
        low = jnp.concatenate([lows[u, pl.ds(i, 1), :]] * ((share - 1) * heads), axis=1)
        top = jnp.where(n < total, tops[u, pl.ds(i, 1), :], -1)
        keep = (sub >= low) & (sub <= top)
        st = lax.dot_general(k, q4, NT, preferred_element_type=jnp.float32)
        dpt = lax.dot_general(v, do4, NT, preferred_element_type=jnp.float32)
        w = jnp.where(keep, jnp.exp2(st * (SCALE * LOG2E) - norm), 0.0)
        low_bits[slot, 0] = w.astype(jnp.bfloat16)
        low_bits[slot, 1] = (w * (dpt - delta)).astype(jnp.bfloat16)

    def collect(n, slot):
        i, u = items[n] // units, items[n] % units
        at = pl.ds(pl.multiple_of(u * unit, unit), unit)
        q4, do4 = stacked(0, i), stacked(1, i)
        ds = low_bits[slot, 1]
        dv = jnp.dot(low_bits[slot, 0], do4, preferred_element_type=jnp.float32)
        dk = jnp.dot(ds, q4, preferred_element_type=jnp.float32)
        dq = lax.dot_general(kv[0, at, :], ds, TN, preferred_element_type=jnp.float32)
        return i, at, dk, dv, dq

    def step(t, _):
        before = jnp.maximum(t - 1, 0) * PAIR
        done = [collect(before + n, n) for n in range(PAIR)]
        for n in range(PAIR):
            weigh(t * PAIR + n, n)
        for i, at, dk, dv, dq in done:
            acc[0, at, :] += dk
            acc[1, at, :] += dv
            for s in range(share - 1):
                dqt[s, i] += dq[:, s * heads * BLOCK:(s + 1) * heads * BLOCK]
        return 0

    lax.fori_loop(0, (total + PAIR - 1) // PAIR + 1, step, 0)


def local_grads(qd, stats, kv, lows, tops, flags, acc, rows, kv_heads, share):
    heads = qd.shape[3] // D_HEAD
    units, queries = tops.shape[:2]
    vmem = pl.BlockSpec(memory_space=pltpu.VMEM)
    return pl.pallas_call(
        functools.partial(grads_kernel, kv_heads, share, rows),
        out_shape=(
            jax.ShapeDtypeStruct((share - 1, queries, D_HEAD, heads * BLOCK), jnp.float32),
            jax.ShapeDtypeStruct(kv.shape, jnp.float32),
        ),
        in_specs=[vmem] * 7,
        out_specs=(vmem, vmem),
        scratch_shapes=[
            pltpu.SMEM((queries * units + 2 * PAIR,), jnp.int32),
            pltpu.VMEM((PAIR, 2, min(rows, BLOCK), (share - 1) * heads * BLOCK),
                       jnp.bfloat16),
        ],
        compiler_params=pltpu.CompilerParams(vmem_limit_bytes=24 << 20),
        name="grads",
    )(qd, stats, kv, lows, tops, flags, acc)


def scatter_kernel(
    deep, kv_heads, share, rows, acc, dq_own, dqt, kv_in, dq_sum, dq_in,
    kv_out, joined, own_core, dq_core, dq_out, ready, kv_send, kv_recv, join_recv, core_send, core_recv,
    x_send, x_recv,
):
    z, c, g, x = place(share)
    seq, head = z * CORES + c, g * share + x
    partner = z * CORES + 1 - c
    own = dqt.shape[1] // CORES
    heads = dqt.shape[3] // BLOCK
    mine = z * kv_heads + g
    peers = near(deep, kv_heads, share)
    barrier = pltpu.get_barrier_semaphore()
    signal(barrier, peers)
    for p in range(deep * kv_heads):
        part = slice(p * rows, (p + 1) * rows)
        kv_out[p, 0] = (acc[0, part, :] * SCALE).astype(jnp.bfloat16)
        kv_out[p, 1] = acc[1, part, :].astype(jnp.bfloat16)
    kv_in[mine] = kv_out[mine]
    for depth in range(deep):
        def unused(depth=depth):
            at = pl.ds(depth * kv_heads, kv_heads)
            kv_in[at] = jnp.zeros((kv_heads,) + kv_in.shape[1:], kv_in.dtype)

        if depth >= REACH or depth < deep - REACH:
            pl.when((depth - z >= REACH) | (z - depth >= REACH))(unused)
    pl.semaphore_wait(barrier, count(peers))

    sent = []

    def send(make, there=True):
        sent.append((there, make))
        when(there, lambda: make().start())

    def inside(depth):
        return (depth >= 0) & (depth < deep)

    def give(step, turn, there=True):
        depth, group = z + step, (g + turn) % kv_heads
        index = depth * kv_heads + group
        send(functools.partial(remote, kv_out.at[index], kv_in.at[mine], kv_send.at[index],
                               kv_recv.at[mine], depth * CORES + c, group * share + x), there)

    def spare(index):
        return index if deep > REACH + 1 else index % kv_heads

    def join(index):
        where = spare(index)
        landed(joined.at[where], join_recv.at[where])
        at = span(index, rows)
        for n, factor in enumerate((SCALE, 1.0)):
            kv_out[index, n] = (acc[n, at, :] * factor
                                + joined[where, n].astype(jnp.float32)).astype(jnp.bfloat16)

    bulk = 2 - own % 2

    def crossing(core, n):
        at, to = pl.ds(core * own + n * bulk, bulk), pl.ds(n * bulk, bulk)
        return (dqt.at[:, at], dq_core.at[:, to]), (dq_own.at[at], own_core.at[to])

    for far in range(deep - 1, REACH - 1, -1):
        for depth, step in ((far, 1), (deep - 1 - far, -1)):
            away = (depth - z) * step >= REACH
            behind = (z > 0) if step == 1 else (z + 1 < deep)
            for turn in range(kv_heads):
                index = depth * kv_heads + (g + turn) % kv_heads
                if far > REACH:
                    pl.when(away & behind)(functools.partial(join, index))
                where = spare(index)
                send(functools.partial(remote, kv_out.at[index], joined.at[where],
                                       kv_send.at[index], join_recv.at[where],
                                       (z + step) * CORES + c, head), away)
    if deep > 1:
        give(1, 0, z + 1 < deep)
        give(-1, 0, z > 0)
    for turn in range(1, kv_heads):
        give(0, turn)
    for n in range(own // bulk):
        for m, (src, dst) in enumerate(crossing(1 - c, n)):
            send(functools.partial(remote, src, dst, core_send.at[2 * n + m],
                                   core_recv.at[2 * n + m], partner, head))
    along = peers[-2:] if deep > 1 else []
    near_end = {1: z == 0, -1: z == deep - 1}
    for d in range(1, min(REACH, deep)):
        signal(ready.at[d - 1], along)
        pl.semaphore_wait(ready.at[d - 1], count(along))
        for step in (1, -1):
            for turn in range(1, kv_heads):
                there = inside(z + step * d)
                give(step * d, turn, there & near_end[step] if d == REACH - 1 else there)
            if d + 1 < min(REACH, deep):
                there = inside(z + step * (d + 1))
                give(step * (d + 1), 0, there & near_end[step] if d == REACH - 2 else there)

    def query_block(n):
        for m, (_, dst) in enumerate(crossing(1 - c, n)):
            landed(dst, core_recv.at[2 * n + m])
        for d in range(share - 1, -1, -1):
            for block in range(n * bulk, (n + 1) * bulk):
                at = slice(block * BLOCK, (block + 1) * BLOCK)
                if d:
                    total = (dqt[d - 1, c * own + block] + dq_core[d - 1, block]) * SCALE
                else:
                    total = (dq_own[c * own + block] + own_core[block]) * SCALE
                for h in range(heads):
                    flat = total[:, h * BLOCK:(h + 1) * BLOCK].T
                    if d:
                        dq_out[d - 1, at, h * D_HEAD:(h + 1) * D_HEAD] = flat.astype(jnp.bfloat16)
                    else:
                        dq_sum[at, h * D_HEAD:(h + 1) * D_HEAD] = flat
            if d:
                at, slot = pl.ds(n * bulk * BLOCK, bulk * BLOCK), (d - 1) * (own // bulk) + n
                send(functools.partial(
                    remote, dq_out.at[d - 1, at, :], dq_in.at[d - 1, at, :], x_send.at[slot],
                    x_recv.at[slot], seq, g * share + (x - d + share) % share))

    query_block(0)
    if deep >= REACH:
        for turn in range(kv_heads):
            for step in (1, -1):
                depth = z + step * (REACH - 1)
                there = inside(depth) & ~near_end[step]
                index = depth * kv_heads + (g + turn) % kv_heads
                pl.when(there)(functools.partial(join, index))
                give(step * (REACH - 1), turn, there)
    for n in range(1, own // bulk):
        query_block(n)
    for depth in range(deep):
        for turn in range(kv_heads):
            index = depth * kv_heads + (g + turn) % kv_heads
            close = (depth - z < REACH) & (z - depth < REACH)
            get = functools.partial(
                lambda index: landed(kv_in.at[index], kv_recv.at[index]), index)
            when(close if turn else close & (depth != z), get)
    for d in range(1, share):
        for n in range(own // bulk):
            at = pl.ds(n * bulk * BLOCK, bulk * BLOCK)
            landed(dq_in.at[d - 1, at, :], x_recv.at[(d - 1) * (own // bulk) + n])
    for there, make in sent:
        when(there, functools.partial(lambda make: make().wait_send(), make))


def finish_kernel(deep, kv_heads, share, kv_in, dq_sum, dq_in, dq, dk, dv):
    total = dq_sum[...]
    for d in range(share - 1):
        total += dq_in[d].astype(jnp.float32)
    dq[...] = total
    for j in range(kv_heads):
        for n, ref in enumerate((dk, dv)):
            total = kv_in[j, n].astype(jnp.float32)
            for depth in range(1, deep):
                total += kv_in[depth * kv_heads + j, n].astype(jnp.float32)
            ref[:, j * D_HEAD:(j + 1) * D_HEAD] = total


def scatter(dq_own, dqt, acc, rows, deep, kv_heads, share):
    pieces = deep * kv_heads
    queries, heads = dqt.shape[1], dqt.shape[3] // BLOCK
    own = queries // CORES
    q_rows = own * BLOCK
    vmem = pl.BlockSpec(memory_space=pltpu.VMEM)
    dma = pltpu.SemaphoreType.DMA
    lanes = max(1, share - 1)
    bulks = own // (2 - own % 2)
    spare = pieces if deep > REACH + 1 else kv_heads
    kv_in, dq_sum, dq_in = pl.pallas_call(
        functools.partial(scatter_kernel, deep, kv_heads, share, rows),
        out_shape=(
            jax.ShapeDtypeStruct((pieces, 2, rows, D_HEAD), jnp.bfloat16),
            jax.ShapeDtypeStruct((q_rows, heads * D_HEAD), jnp.float32),
            jax.ShapeDtypeStruct((lanes, q_rows, heads * D_HEAD), jnp.bfloat16),
        ),
        in_specs=[vmem] * 3,
        out_specs=(vmem,) * 3,
        scratch_shapes=[
            pltpu.VMEM((pieces, 2, rows, D_HEAD), jnp.bfloat16),
            pltpu.VMEM((spare, 2, rows, D_HEAD), jnp.bfloat16),
            pltpu.VMEM((own,) + dqt.shape[2:], jnp.float32),
            pltpu.VMEM((dqt.shape[0], own) + dqt.shape[2:], jnp.float32),
            pltpu.VMEM((lanes, q_rows, heads * D_HEAD), jnp.bfloat16),
            pltpu.SemaphoreType.REGULAR((max(1, min(REACH, deep) - 1),)),
            dma((pieces,)),
            dma((pieces,)),
            dma((spare,)),
            dma((2 * bulks,)),
            dma((2 * bulks,)),
            dma((lanes * bulks,)),
            dma((lanes * bulks,)),
        ],
        compiler_params=pltpu.CompilerParams(collective_id=1, has_side_effects=True,
            vmem_limit_bytes=20 << 20),
        name="scatter",
    )(acc, dq_own, dqt)
    grad = jax.ShapeDtypeStruct((rows, kv_heads * D_HEAD), jnp.float32)
    return pl.pallas_call(
        functools.partial(finish_kernel, deep, kv_heads, share),
        out_shape=(jax.ShapeDtypeStruct(dq_sum.shape, jnp.float32), grad, grad),
        in_specs=[vmem] * 3,
        out_specs=(vmem,) * 3,
        compiler_params=pltpu.CompilerParams(vmem_limit_bytes=8 << 20),
        name="finish",
    )(kv_in, dq_sum, dq_in)


def body(
    queries, keys, values, attn_out, out_grad, log_norm, block_layout, document_ids, block_order
):
    share = GROUP // log_norm.shape[0]
    kv_heads = lax.axis_size("head") // share
    deep = lax.axis_size("seq") // CORES
    rows = keys.shape[0]
    kv, qd, stats, lows, tops, flags, acc, dq_own = gather(
        queries, out_grad, attn_out, log_norm, keys, values, block_layout, document_ids,
        block_order, deep, kv_heads, share)
    dqt, acc = local_grads(qd, stats, kv, lows, tops, flags, acc, rows, kv_heads, share)
    return tuple(scatter(dq_own, dqt, acc, rows, deep, kv_heads, share))


def solution(mesh):
    in_specs = (
        P("seq", "head"),
        P(("seq", "head"), None),
        P(("seq", "head"), None),
        P("seq", "head"),
        P("seq", "head"),
        P("head", "seq"),
        P("head", None, None),
        P(),
        P(),
    )
    out_specs = (P("seq", "head"), P(("seq", "head"), None), P(("seq", "head"), None))
    return jax.shard_map(body, mesh=mesh, in_specs=in_specs, out_specs=out_specs, check_vma=False)
```

```python
import functools
import math

import jax
import jax.numpy as jnp
from jax import lax
from jax.experimental import pallas as pl
from jax.experimental.pallas import tpu as pltpu
from jax.sharding import PartitionSpec as P

D_HEAD = 128
GROUP = 4
BLOCK = 128
DOCS = 8
CORES = 2
PAIR = 4
SPAN = 2
REACH = 3
WORD = 16
SHIFT = 10
LOG2E = math.log2(math.e)
SCALE = D_HEAD ** -0.5
NT = (((1,), (1,)), ((), ()))
TN = (((0,), (0,)), ((), ()))


def place(share):
    seq, head = lax.axis_index("seq"), lax.axis_index("head")
    return seq // CORES, seq % CORES, head // share, head % share


def remote(src, dst, send, recv, seq, head):
    return pltpu.make_async_remote_copy(
        src_ref=src, dst_ref=dst, send_sem=send, recv_sem=recv,
        device_id={"seq": seq, "head": head}, device_id_type=pl.DeviceIdType.MESH)


def landed(where, sem):
    pltpu.make_async_copy(where, where, sem).wait()


def when(there, run):
    if there is True:
        run()
    else:
        pl.when(there)(run)


def span(index, rows):
    return pl.ds(pl.multiple_of(index * rows, rows), rows)


def near(deep, kv_heads, share):
    z, c, g, x = place(share)
    seq, head = z * CORES + c, g * share + x
    peers = [(z * CORES + (c + d) % CORES, head, True) for d in range(1, CORES)]
    peers += [(seq, g * share + (x + d) % share, True) for d in range(1, share)]
    peers += [(seq, (g + d) % kv_heads * share + x, True) for d in range(1, kv_heads)]
    if deep > 1:
        peers += [(seq + CORES, head, z + 1 < deep), (seq - CORES, head, z > 0)]
    return peers


def signal(sem, peers):
    for seq, head, there in peers:
        when(there, lambda: pl.semaphore_signal(
            sem, inc=1, device_id={"seq": seq, "head": head},
            device_id_type=pl.DeviceIdType.MESH))


def count(peers):
    total = 0
    for _, _, there in peers:
        total = total + (1 if there is True else there.astype(jnp.int32))
    return total


def unit_row(u, unit, rows, kv_heads, share):
    z, c, g, x = place(share)
    per = rows // unit
    piece, sub = u // per, u % per
    depth, group = piece // kv_heads, piece % kv_heads
    owner = (depth * CORES + c) * kv_heads * share + group * share + x
    return owner * rows + sub * unit


def gather_kernel(
    deep, kv_heads, share, q_in, do_in, o_in, ln_in, k_in, v_in, lay_in, docs_in, order_in,
    kv, qd, stats, lows, tops, flags, acc, dq_own,
    stage, o_buf, ln_buf, docs, order, layout, seen, own_tops, low_bits,
    local, ready, kv_send, kv_recv, x_send, x_recv, core_send, core_recv,
):
    z, c, g, x = place(share)
    seq, head = z * CORES + c, g * share + x
    heads, q_rows = ln_in.shape
    rows = k_in.shape[0]
    own = q_rows // BLOCK
    unit = min(rows, BLOCK)
    mine = z * kv_heads + g

    def cols(index):
        return pl.ds(pl.multiple_of(index * D_HEAD, D_HEAD), D_HEAD)

    here = span(c, q_rows)
    head_rows = pl.ds(c * q_rows, BLOCK)
    tail_rows = pl.ds(c * q_rows + BLOCK, q_rows - BLOCK)
    pulls = [(ref.at[pl.ds(0, BLOCK), :], qd.at[x, n, head_rows, :])
             for n, ref in enumerate((q_in, do_in))]
    pulls += [(k_in.at[:, cols(g)], kv.at[0, span(mine, rows), :]),
              (v_in.at[:, cols(g)], kv.at[1, span(mine, rows), :])]
    for d in range(1, kv_heads):
        other = cols((g + d) % kv_heads)
        pulls += [(k_in.at[:, other], stage.at[d - 1, 0]), (v_in.at[:, other], stage.at[d - 1, 1])]
    urgent = len(pulls)
    if own > 1:
        pulls += [(ref.at[pl.ds(BLOCK, q_rows - BLOCK), :], qd.at[x, n, tail_rows, :])
                  for n, ref in enumerate((q_in, do_in))]
    pulls += [(order_in, order), (lay_in, layout), (o_in, o_buf), (ln_in, ln_buf), (docs_in, docs)]
    pulls = [pltpu.make_async_copy(src, dst, local.at[n]) for n, (src, dst) in enumerate(pulls)]
    for pull in pulls:
        pull.start()
    peers = near(deep, kv_heads, share)
    barrier = pltpu.get_barrier_semaphore()
    signal(barrier, peers)
    for pull in pulls[:urgent]:
        pull.wait()
    pl.semaphore_wait(barrier, count(peers))

    sent = []

    def send(make, there=True):
        sent.append((there, make))
        when(there, lambda: make().start())

    kv_slots = [0]

    def send_kv(src, dst, arrival, to_seq, to_head, there=True):
        slot = kv_slots[0]
        kv_slots[0] += 1
        send(lambda: remote(src, dst, kv_send.at[slot], arrival, to_seq, to_head), there)

    def whole(index):
        return kv.at[:, span(index, rows), :]

    def onward(index, step, there):
        send_kv(whole(index), whole(index), kv_recv.at[index], seq + step * CORES, head, there)

    def reach(index, step):
        there = inside(z + step)
        send_kv(whole(index), whole(index), kv_recv.at[index], seq + step * CORES, head, there)

    def inside(depth):
        return (depth >= 0) & (depth < deep)

    for turn in range(1, kv_heads):
        send_kv(stage.at[turn - 1], whole(mine), kv_recv.at[mine], seq,
                (g + turn) % kv_heads * share + x)
    along = peers[-2:] if deep > 1 else []
    if deep > 1:
        reach(mine, 1)
        reach(mine, -1)
        signal(ready.at[0], along)

    def chunk_of(lane, core, n):
        return qd.at[lane, :, pl.ds(core * q_rows + n * BLOCK, BLOCK), :]

    def send_chunk(n):
        for d in range(1, share):
            part, slot = chunk_of(x, c, n), (d - 1) * own + n
            send(functools.partial(remote, part, part, x_send.at[slot], x_recv.at[slot], seq,
                                   g * share + (x + d) % share))

    stats_at = (share - 1) * own
    seen_at = stats_at + share - 1
    send_chunk(0)
    for pull in pulls[urgent:-3]:
        pull.wait()
    partner = z * CORES + 1 - c
    mine_rows = qd.at[x, :, here, :]
    send(functools.partial(remote, mine_rows, mine_rows, core_send.at[0], core_recv.at[0],
                           partner, head))
    queries, blocks = CORES * own, order.shape[0]
    units = own_tops.shape[0]
    row_of = lax.broadcasted_iota(jnp.int32, (queries, BLOCK), 0)
    at_block = jnp.zeros((queries, BLOCK), jnp.int32)
    for i in range(queries):
        at_block = jnp.where(row_of == i, order[z * queries + i], at_block)
    column = lax.broadcasted_iota(jnp.int32, (queries, blocks), 1)
    picked = jnp.where(column == at_block[:, :blocks], 1.0, 0.0).astype(jnp.bfloat16)
    for h in range(heads):
        seen[0, h] = jnp.dot(picked, layout[h].astype(jnp.float32).astype(jnp.bfloat16),
                             preferred_element_type=jnp.float32)
    for d in range(1, share):
        slot = seen_at + d - 1
        send(functools.partial(remote, seen.at[0], seen.at[d], x_send.at[slot], x_recv.at[slot],
                               seq, g * share + (x + d) % share))
    for d in range(1, min(REACH, deep) - 1):
        pl.semaphore_wait(ready.at[d - 1], count(along))
        if d + 2 < min(REACH, deep):
            signal(ready.at[d], along)
        reach(mine, d + 1)
        reach(mine, -d - 1)
    for pull in pulls[-3:]:
        pull.wait()
    mine_stats = stats.at[x, pl.ds(c * own, own)]
    for n in range(own):
        part = slice(n * BLOCK, (n + 1) * BLOCK)
        at = pl.ds(c * q_rows + n * BLOCK, BLOCK)
        for h in range(heads):
            lanes = slice(h * D_HEAD, (h + 1) * D_HEAD)
            product = (qd[x, 1, at, lanes].astype(jnp.float32)
                       * o_buf[part, lanes].astype(jnp.float32))
            stats[x, c * own + n, h:h + 1, :] = ln_buf[h:h + 1, part] * LOG2E
            stats[x, c * own + n, heads + h:heads + h + 1, :] = jnp.sum(
                product.T, axis=0, keepdims=True)
    for d in range(1, share):
        slot = stats_at + d - 1
        send(functools.partial(remote, mine_stats, mine_stats, x_send.at[slot], x_recv.at[slot],
                               seq, g * share + (x + d) % share))
    send(functools.partial(remote, mine_stats, mine_stats, core_send.at[1], core_recv.at[1],
                           partner, head))
    for n in range(1, own):
        send_chunk(n)

    block_of = lax.broadcasted_iota(jnp.int32, (blocks, BLOCK), 0)
    stored = [unit_row(u, unit, rows, kv_heads, share) for u in range(units)]
    kept = [order[row // BLOCK] for row in stored]
    starts = [block * BLOCK + row % BLOCK for block, row in zip(kept, stored)]
    chosen = jnp.concatenate([jnp.where(block_of == block, 1.0, 0.0) for block in kept],
                             axis=1).astype(jnp.bfloat16)
    at_query = at_block * BLOCK + lax.broadcasted_iota(jnp.int32, (queries, BLOCK), 1)

    def fill_tops(ref, slot, source):
        for h in range(heads):
            on = jnp.dot(seen[source, h].astype(jnp.bfloat16), chosen,
                         preferred_element_type=jnp.float32)
            at = slice((slot * heads + h) * BLOCK, (slot * heads + h + 1) * BLOCK)
            for u in range(units):
                ref[u, :, at] = jnp.where(on[:, u * BLOCK:(u + 1) * BLOCK] > 0.5, at_query - starts[u], -1)

    ids = docs[...]
    low = jnp.zeros_like(ids)
    for d in range(1, DOCS):
        before = jnp.sum(jnp.where(ids < d, 1.0, 0.0), axis=1, keepdims=True)
        before = jnp.sum(before, axis=0, keepdims=True).astype(jnp.int32)
        low = jnp.where(ids >= d, before, low)
    docs[...] = low
    first = jnp.concatenate(
        [docs[pl.ds(order[z * queries + i], 1), :] for i in range(queries)], axis=0)
    lane_of = lax.broadcasted_iota(jnp.int32, (queries, BLOCK), 1)
    start = jnp.zeros((queries, BLOCK), jnp.int32)
    for u in range(units):
        lows[u] = first - starts[u]
        start = jnp.where(lane_of == u, starts[u], start)
    flags[...] = jnp.where(
        (lane_of < units) & (start < (at_block + 1) * BLOCK) & (first[:, :1] < start + unit),
        1.0, 0.0)
    fill_tops(own_tops, 0, 0)
    acc[...] = jnp.zeros_like(acc)
    dq_own[...] = jnp.zeros_like(dq_own)

    sub = lax.broadcasted_iota(jnp.int32, (unit, SPAN * heads * BLOCK), 0)
    both = [(j, h) for j in range(SPAN) for h in range(heads)]

    def stacked(n, t):
        return jnp.concatenate(
            [qd[x, n, pl.ds(pl.multiple_of((t * SPAN + j) * BLOCK, BLOCK), BLOCK),
                 h * D_HEAD:(h + 1) * D_HEAD] for j, h in both], axis=0)

    def joint(n, batch):
        return jnp.concatenate([kv[n, span(index, rows), :] for index in batch], axis=0)

    def weigh(t, batch):
        st = lax.dot_general(joint(0, batch), stacked(0, t), NT,
                             preferred_element_type=jnp.float32)
        dpt = lax.dot_general(joint(1, batch), stacked(1, t), NT,
                              preferred_element_type=jnp.float32)
        rowed = [stats[x, t * SPAN + j] for j in range(SPAN)]
        norm = jnp.concatenate([rowed[j][h:h + 1] for j, h in both], axis=1)
        delta = jnp.concatenate([rowed[j][heads + h:heads + h + 1] for j, h in both], axis=1)
        keeps = []
        for u in [index * (rows // unit) + n for index in batch for n in range(rows // unit)]:
            rowed_low = [lows[u, pl.ds(t * SPAN + j, 1), :] for j in range(SPAN)]
            low = jnp.concatenate([rowed_low[j] for j, _ in both], axis=1)
            top = jnp.concatenate(
                [own_tops[u, pl.ds(t * SPAN + j, 1), :] for j in range(SPAN)], axis=1)
            keeps.append((sub >= low) & (sub <= top))
        keep = jnp.concatenate(keeps, axis=0)
        w = jnp.where(keep, jnp.exp2(st * (SCALE * LOG2E) - norm), 0.0)
        low_bits[0] = w.astype(jnp.bfloat16)
        low_bits[1] = (w * (dpt - delta)).astype(jnp.bfloat16)

    def collect(t, batch):
        ds = low_bits[1]
        dv = jnp.dot(low_bits[0], stacked(1, t), preferred_element_type=jnp.float32)
        dk = jnp.dot(ds, stacked(0, t), preferred_element_type=jnp.float32)
        dq = lax.dot_general(joint(0, batch), ds, TN, preferred_element_type=jnp.float32)
        for n, index in enumerate(batch):
            at, part = span(index, rows), slice(n * rows, (n + 1) * rows)
            acc[0, at, :] += dk[part]
            acc[1, at, :] += dv[part]
        for j in range(SPAN):
            dq_own[t * SPAN + j] += dq[:, j * heads * BLOCK:(j + 1) * heads * BLOCK]

    turns = queries // SPAN

    def nearest(k):
        short = jnp.minimum(z, deep - 1 - z)
        beyond = jnp.where(z < deep - 1 - z, k, deep - 1 - k)
        return jnp.where(k <= 2 * short, z + (k + 1) // 2 * (1 - 2 * (k % 2)), beyond)

    def of(k, turn):
        return nearest(k) * kv_heads + (g + turn) % kv_heads

    order_of = [[(0, turn) for turn in range(kv_heads)]]
    late = 1
    if kv_heads == 2 and deep > 2:
        order_of += [[(1, turn), (2, turn)] for turn in range(kv_heads)]
        late = 3
    order_of += [[(k, turn) for turn in range(kv_heads)] for k in range(late, deep)]
    batches = [[of(*entry) for entry in batch] for batch in order_of]

    def attend(k, midway=None):
        batch, before = batches[k], batches[max(k - 1, 0)]

        def turn(t, _):
            first = t == 0
            collect(jnp.where(first, turns - 1, t - 1),
                    [jnp.where(first, old, new) for old, new in zip(before, batch)])
            weigh(t, batch)
            return 0

        if k == 0:
            weigh(0, batch)
        lax.fori_loop(1 if k == 0 else 0, turns // 2, turn, 0)
        if midway is not None:
            midway()
        lax.fori_loop(turns // 2, turns, turn, 0)

    def relay(part, slot):
        landed(part, x_recv.at[slot])
        send(functools.partial(remote, part, part, core_send.at[2 + slot],
                               core_recv.at[2 + slot], partner, head))

    def relay_chunk(n):
        for d in range(1, share):
            relay(chunk_of((x - d + share) % share, c, n), (d - 1) * own + n)

    for j in range(1, kv_heads):
        index = z * kv_heads + (g + j) % kv_heads
        landed(whole(index), kv_recv.at[index])
        for d in range(1, min(REACH, deep)):
            reach(index, d)
            reach(index, -d)
    there = span(1 - c, q_rows)
    landed(qd.at[x, :, there, :], core_recv.at[0])
    landed(stats.at[x, pl.ds((1 - c) * own, own)], core_recv.at[1])
    attend(0)

    def arrive(d, turns_in):
        for turn in turns_in:
            for depth, step in ((z - d, 1), (z + d, -1)):
                index = depth * kv_heads + (g + turn) % kv_heads
                when(inside(depth), functools.partial(
                    lambda index: landed(whole(index), kv_recv.at[index]), index))
                if REACH - 1 <= d < deep - 1:
                    onward(index, step, inside(depth) & inside(z + step))

    chunks = list(range(own))

    def relay_next():
        if chunks:
            relay_chunk(chunks.pop(0))

    def relay_rest():
        while chunks:
            relay_chunk(chunks.pop(0))

    done = 1
    for turns_in in ([0], list(range(1, kv_heads))):
        for d in range(1, min(REACH, deep)):
            arrive(d, turns_in)
        if turns_in == [0]:
            for e in range(1, share):
                landed(seen.at[e], x_recv.at[seen_at + e - 1])
                fill_tops(tops, e - 1, e)
                relay(stats.at[(x - e + share) % share, pl.ds(c * own, own)], stats_at + e - 1)
        relay_next()
        if late == 3:
            attend(done)
            done += 1
    for d in range(REACH, deep):
        arrive(d, range(kv_heads))
    relay_next()
    for k in range(done, deep):
        attend(k, relay_rest if k == deep - 1 else None)
    relay_rest()
    collect(turns - 1, batches[deep - 1])
    for d in range(1, share):
        lane = (x - d + share) % share
        for n in range(own):
            landed(chunk_of(lane, 1 - c, n), core_recv.at[2 + (d - 1) * own + n])
        landed(stats.at[lane, pl.ds((1 - c) * own, own)], core_recv.at[2 + stats_at + d - 1])
    for there, make in sent:
        when(there, functools.partial(lambda make: make().wait_send(), make))


def gather(queries, out_grad, attn_out, log_norm, keys, values, block_layout, document_ids,
           block_order, deep, kv_heads, share):
    rows = keys.shape[0]
    heads, q_rows = log_norm.shape
    blocks = block_order.shape[0]
    own = q_rows // BLOCK
    unit = min(rows, BLOCK)
    pieces = deep * kv_heads
    kv_rows = pieces * rows
    hbm = pl.BlockSpec(memory_space=pltpu.HBM)
    vmem = pl.BlockSpec(memory_space=pltpu.VMEM)
    lanes = share - 1
    x_copies = max(1, lanes * (own + 2))
    steps = min(REACH, deep) - 1
    kv_copies = max(1, kv_heads - 1 + 2 * kv_heads * (steps + max(0, deep - REACH)))
    dma = pltpu.SemaphoreType.DMA
    return pl.pallas_call(
        functools.partial(gather_kernel, deep, kv_heads, share),
        out_shape=(
            jax.ShapeDtypeStruct((2, kv_rows, D_HEAD), keys.dtype),
            jax.ShapeDtypeStruct((share, 2, CORES * q_rows, heads * D_HEAD), queries.dtype),
            jax.ShapeDtypeStruct((share, CORES * own, 2 * heads, BLOCK), jnp.float32),
            jax.ShapeDtypeStruct((kv_rows // unit, CORES * own, BLOCK), jnp.int32),
            jax.ShapeDtypeStruct(
                (kv_rows // unit, CORES * own, max(1, lanes) * heads * BLOCK), jnp.int32),
            jax.ShapeDtypeStruct((CORES * own, BLOCK), jnp.float32),
            jax.ShapeDtypeStruct((2, kv_rows, D_HEAD), jnp.float32),
            jax.ShapeDtypeStruct((CORES * own, D_HEAD, heads * BLOCK), jnp.float32),
        ),
        in_specs=[hbm] * 9,
        out_specs=(vmem,) * 8,
        scratch_shapes=[
            pltpu.VMEM((max(1, kv_heads - 1), 2, rows, D_HEAD), keys.dtype),
            pltpu.VMEM(attn_out.shape, attn_out.dtype),
            pltpu.VMEM(log_norm.shape, jnp.float32),
            pltpu.VMEM((blocks, BLOCK), jnp.int32),
            pltpu.SMEM((blocks,), jnp.int32),
            pltpu.VMEM(block_layout.shape, jnp.int32),
            pltpu.VMEM((share, heads, CORES * own, blocks), jnp.float32),
            pltpu.VMEM((kv_rows // unit, CORES * own, heads * BLOCK), jnp.int32),
            pltpu.VMEM((2, kv_heads * rows, SPAN * heads * BLOCK), jnp.bfloat16),
            dma((2 * kv_heads + (9 if own > 1 else 7),)),
            pltpu.SemaphoreType.REGULAR((max(1, steps - 1),)),
            dma((kv_copies,)),
            dma((pieces,)),
            dma((x_copies,)),
            dma((x_copies,)),
            dma((2 + x_copies - lanes,)),
            dma((2 + x_copies - lanes,)),
        ],
        compiler_params=pltpu.CompilerParams(collective_id=0, has_side_effects=True,
            vmem_limit_bytes=16 << 20),
        name="gather",
    )(*[pltpu.with_memory_space_constraint(array, pltpu.HBM) for array in (
        queries, out_grad, attn_out, log_norm, keys, values, block_layout,
        document_ids.reshape(blocks, BLOCK), block_order)])


def grads_kernel(
    kv_heads, share, rows, qd, stats, kv, lows, tops, flags, acc_in,
    dqt, acc, items, low_bits,
):
    x = place(share)[3]
    queries = dqt.shape[1]
    heads = qd.shape[3] // D_HEAD
    unit = min(rows, BLOCK)
    units = kv.shape[1] // unit
    others = [(x - d + share) % share for d in range(1, share)]
    lane_of = lax.broadcasted_iota(jnp.int32, (1, BLOCK), 1)
    marks = [jnp.zeros((1, BLOCK), jnp.float32) for _ in range(0, units, WORD)]
    for u in range(units):
        marks[u // WORD] = jnp.where(lane_of == u, float(1 << u % WORD), marks[u // WORD])
    words = [[jnp.sum(flags[i:i + 1, :] * mark).astype(jnp.int32) for mark in marks]
             for i in range(queries)]
    acc[...] = acc_in[...]

    def clear(i, _):
        for s in range(share - 1):
            dqt[s, pl.ds(i, 1)] = jnp.zeros((1,) + dqt.shape[2:], jnp.float32)
        return 0

    lax.fori_loop(0, queries, clear, 0)
    total = jnp.int32(0)
    for i in range(queries):
        for u in range(units):
            items[total] = i << SHIFT | u
            total = total + ((words[i][u // WORD] >> (u % WORD)) & 1)
    wide = (share - 1) * heads * BLOCK
    sub = lax.broadcasted_iota(jnp.int32, (unit, wide), 0)
    for n in range(2 * PAIR):
        items[total + n] = 0

    def stacked(n, i):
        at = pl.ds(pl.multiple_of(i * BLOCK, BLOCK), BLOCK)
        return jnp.concatenate(
            [qd[s, n, at, h * D_HEAD:(h + 1) * D_HEAD] for s in others for h in range(heads)],
            axis=0)

    def weigh(n, slot):
        i, u = items[n] >> SHIFT, items[n] & ((1 << SHIFT) - 1)
        at = pl.ds(pl.multiple_of(u * unit, unit), unit)
        k, v = kv[0, at, :], kv[1, at, :]
        q4, do4 = stacked(0, i), stacked(1, i)
        rowed = [stats[s, i] for s in others]
        norm = jnp.concatenate([r[h:h + 1] for r in rowed for h in range(heads)], axis=1)
        delta = jnp.concatenate(
            [r[heads + h:heads + h + 1] for r in rowed for h in range(heads)], axis=1)
        low = jnp.concatenate([lows[u, pl.ds(i, 1), :]] * ((share - 1) * heads), axis=1)
        top = jnp.where(n < total, tops[u, pl.ds(i, 1), :], -1)
        keep = (sub >= low) & (sub <= top)
        st = lax.dot_general(k, q4, NT, preferred_element_type=jnp.float32)
        dpt = lax.dot_general(v, do4, NT, preferred_element_type=jnp.float32)
        w = jnp.where(keep, jnp.exp2(st * (SCALE * LOG2E) - norm), 0.0)
        low_bits[slot, 0] = w.astype(jnp.bfloat16)
        low_bits[slot, 1] = (w * (dpt - delta)).astype(jnp.bfloat16)

    def collect(n, slot):
        i, u = items[n] >> SHIFT, items[n] & ((1 << SHIFT) - 1)
        at = pl.ds(pl.multiple_of(u * unit, unit), unit)
        q4, do4 = stacked(0, i), stacked(1, i)
        ds = low_bits[slot, 1]
        dv = jnp.dot(low_bits[slot, 0], do4, preferred_element_type=jnp.float32)
        dk = jnp.dot(ds, q4, preferred_element_type=jnp.float32)
        dq = lax.dot_general(kv[0, at, :], ds, TN, preferred_element_type=jnp.float32)
        return i, at, dk, dv, dq

    def add(done):
        for i, at, dk, dv, dq in done:
            acc[0, at, :] += dk
            acc[1, at, :] += dv
            for s in range(share - 1):
                dqt[s, i] += dq[:, s * heads * BLOCK:(s + 1) * heads * BLOCK]

    def step(t, _):
        done = [collect((t - 1) * PAIR + n, n) for n in range(PAIR)]
        for n in range(PAIR):
            weigh(t * PAIR + n, n)
        add(done)
        return 0

    steps = jnp.maximum((total + PAIR - 1) // PAIR, 1)
    for n in range(PAIR):
        weigh(jnp.int32(n), n)
    lax.fori_loop(1, steps, step, 0)
    add([collect((steps - 1) * PAIR + n, n) for n in range(PAIR)])


def local_grads(qd, stats, kv, lows, tops, flags, acc, rows, kv_heads, share):
    heads = qd.shape[3] // D_HEAD
    units, queries = tops.shape[:2]
    vmem = pl.BlockSpec(memory_space=pltpu.VMEM)
    return pl.pallas_call(
        functools.partial(grads_kernel, kv_heads, share, rows),
        out_shape=(
            jax.ShapeDtypeStruct((share - 1, queries, D_HEAD, heads * BLOCK), jnp.float32),
            jax.ShapeDtypeStruct(kv.shape, jnp.float32),
        ),
        in_specs=[vmem] * 7,
        out_specs=(vmem, vmem),
        scratch_shapes=[
            pltpu.SMEM((queries * units + 2 * PAIR,), jnp.int32),
            pltpu.VMEM((PAIR, 2, min(rows, BLOCK), (share - 1) * heads * BLOCK),
                       jnp.bfloat16),
        ],
        compiler_params=pltpu.CompilerParams(
            vmem_limit_bytes=24 << 20),
        name="grads",
    )(qd, stats, kv, lows, tops, flags, acc)


def scatter_kernel(
    deep, kv_heads, share, rows, acc, dq_own, dqt, kv_in, dq_sum, dq_in,
    kv_out, joined, own_core, dq_core, dq_out, ready, kv_send, kv_recv, join_recv, core_send, core_recv,
    x_send, x_recv,
):
    z, c, g, x = place(share)
    seq, head = z * CORES + c, g * share + x
    partner = z * CORES + 1 - c
    own = dqt.shape[1] // CORES
    heads = dqt.shape[3] // BLOCK
    mine = z * kv_heads + g
    peers = near(deep, kv_heads, share)
    along = peers[-2:] if deep > 1 else []
    peers += [(to, (g + d) % kv_heads * share + x, there)
              for to, _, there in along for d in range(1, kv_heads)]
    barrier = pltpu.get_barrier_semaphore()
    signal(barrier, peers)
    for p in range(deep * kv_heads):
        part = slice(p * rows, (p + 1) * rows)
        kv_out[p, 0] = (acc[0, part, :] * SCALE).astype(jnp.bfloat16)
        kv_out[p, 1] = acc[1, part, :].astype(jnp.bfloat16)
    kv_in[mine] = kv_out[mine]
    for depth in range(deep):
        def unused(depth=depth):
            at = pl.ds(depth * kv_heads, kv_heads)
            kv_in[at] = jnp.zeros((kv_heads,) + kv_in.shape[1:], kv_in.dtype)

        if depth >= REACH or depth < deep - REACH:
            pl.when((depth - z >= REACH) | (z - depth >= REACH))(unused)
    pl.semaphore_wait(barrier, count(peers))

    sent = []

    def send(make, there=True):
        sent.append((there, make))
        when(there, lambda: make().start())

    def inside(depth):
        return (depth >= 0) & (depth < deep)

    def give(step, turn, there=True):
        depth, group = z + step, (g + turn) % kv_heads
        index = depth * kv_heads + group
        send(functools.partial(remote, kv_out.at[index], kv_in.at[mine], kv_send.at[index],
                               kv_recv.at[mine], depth * CORES + c, group * share + x), there)

    def spare(index):
        return index if deep > REACH + 1 else index % kv_heads

    def join(index):
        where = spare(index)
        landed(joined.at[where], join_recv.at[where])
        at = span(index, rows)
        for n, factor in enumerate((SCALE, 1.0)):
            kv_out[index, n] = (acc[n, at, :] * factor
                                + joined[where, n].astype(jnp.float32)).astype(jnp.bfloat16)

    bulk = 2 - own % 2

    def crossing(core, n):
        at, to = pl.ds(core * own + n * bulk, bulk), pl.ds(n * bulk, bulk)
        return (dqt.at[:, at], dq_core.at[:, to]), (dq_own.at[at], own_core.at[to])

    for far in range(deep - 1, REACH - 1, -1):
        for depth, step in ((far, 1), (deep - 1 - far, -1)):
            away = (depth - z) * step >= REACH
            behind = (z > 0) if step == 1 else (z + 1 < deep)
            for turn in range(kv_heads):
                index = depth * kv_heads + (g + turn) % kv_heads
                if far > REACH:
                    pl.when(away & behind)(functools.partial(join, index))
                where = spare(index)
                send(functools.partial(remote, kv_out.at[index], joined.at[where],
                                       kv_send.at[index], join_recv.at[where],
                                       (z + step) * CORES + c, head), away)
    near_end = {1: z == 0, -1: z == deep - 1}

    def give_all(d):
        for turn in range(kv_heads):
            for step in (1, -1):
                there = inside(z + step * d)
                give(step * d, turn, there & near_end[step] if d == REACH - 1 else there)

    if deep > 1:
        give_all(1)
    for turn in range(1, kv_heads):
        give(0, turn)
    for n in range(own // bulk):
        for m, (src, dst) in enumerate(crossing(1 - c, n)):
            send(functools.partial(remote, src, dst, core_send.at[2 * n + m],
                                   core_recv.at[2 * n + m], partner, head))
    for d in range(1, min(REACH, deep) - 1):
        signal(ready.at[d - 1], along)
        pl.semaphore_wait(ready.at[d - 1], count(along))
        give_all(d + 1)

    def query_block(n):
        for m, (_, dst) in enumerate(crossing(1 - c, n)):
            landed(dst, core_recv.at[2 * n + m])
        for d in range(share - 1, -1, -1):
            for block in range(n * bulk, (n + 1) * bulk):
                at = slice(block * BLOCK, (block + 1) * BLOCK)
                if d:
                    total = (dqt[d - 1, c * own + block] + dq_core[d - 1, block]) * SCALE
                else:
                    total = (dq_own[c * own + block] + own_core[block]) * SCALE
                for h in range(heads):
                    flat = total[:, h * BLOCK:(h + 1) * BLOCK].T
                    if d:
                        dq_out[d - 1, at, h * D_HEAD:(h + 1) * D_HEAD] = flat.astype(jnp.bfloat16)
                    else:
                        dq_sum[at, h * D_HEAD:(h + 1) * D_HEAD] = flat
            if d:
                at, slot = pl.ds(n * bulk * BLOCK, bulk * BLOCK), (d - 1) * (own // bulk) + n
                send(functools.partial(
                    remote, dq_out.at[d - 1, at, :], dq_in.at[d - 1, at, :], x_send.at[slot],
                    x_recv.at[slot], seq, g * share + (x - d + share) % share))

    query_block(0)
    if deep >= REACH:
        for turn in range(kv_heads):
            for step in (1, -1):
                depth = z + step * (REACH - 1)
                there = inside(depth) & ~near_end[step]
                index = depth * kv_heads + (g + turn) % kv_heads
                pl.when(there)(functools.partial(join, index))
                give(step * (REACH - 1), turn, there)
    for n in range(1, own // bulk):
        query_block(n)
    for depth in range(deep):
        for turn in range(kv_heads):
            index = depth * kv_heads + (g + turn) % kv_heads
            close = (depth - z < REACH) & (z - depth < REACH)
            get = functools.partial(
                lambda index: landed(kv_in.at[index], kv_recv.at[index]), index)
            when(close if turn else close & (depth != z), get)
    for d in range(1, share):
        for n in range(own // bulk):
            at = pl.ds(n * bulk * BLOCK, bulk * BLOCK)
            landed(dq_in.at[d - 1, at, :], x_recv.at[(d - 1) * (own // bulk) + n])
    for there, make in sent:
        when(there, functools.partial(lambda make: make().wait_send(), make))


def finish_kernel(deep, kv_heads, share, kv_in, dq_sum, dq_in, dq, dk, dv):
    total = dq_sum[...]
    for d in range(share - 1):
        total += dq_in[d].astype(jnp.float32)
    dq[...] = total
    for j in range(kv_heads):
        for n, ref in enumerate((dk, dv)):
            total = kv_in[j, n].astype(jnp.float32)
            for depth in range(1, deep):
                total += kv_in[depth * kv_heads + j, n].astype(jnp.float32)
            ref[:, j * D_HEAD:(j + 1) * D_HEAD] = total


def scatter(dq_own, dqt, acc, rows, deep, kv_heads, share):
    pieces = deep * kv_heads
    queries, heads = dqt.shape[1], dqt.shape[3] // BLOCK
    own = queries // CORES
    q_rows = own * BLOCK
    vmem = pl.BlockSpec(memory_space=pltpu.VMEM)
    dma = pltpu.SemaphoreType.DMA
    lanes = max(1, share - 1)
    bulks = own // (2 - own % 2)
    spare = pieces if deep > REACH + 1 else kv_heads
    kv_in, dq_sum, dq_in = pl.pallas_call(
        functools.partial(scatter_kernel, deep, kv_heads, share, rows),
        out_shape=(
            jax.ShapeDtypeStruct((pieces, 2, rows, D_HEAD), jnp.bfloat16),
            jax.ShapeDtypeStruct((q_rows, heads * D_HEAD), jnp.float32),
            jax.ShapeDtypeStruct((lanes, q_rows, heads * D_HEAD), jnp.bfloat16),
        ),
        in_specs=[vmem] * 3,
        out_specs=(vmem,) * 3,
        scratch_shapes=[
            pltpu.VMEM((pieces, 2, rows, D_HEAD), jnp.bfloat16),
            pltpu.VMEM((spare, 2, rows, D_HEAD), jnp.bfloat16),
            pltpu.VMEM((own,) + dqt.shape[2:], jnp.float32),
            pltpu.VMEM((dqt.shape[0], own) + dqt.shape[2:], jnp.float32),
            pltpu.VMEM((lanes, q_rows, heads * D_HEAD), jnp.bfloat16),
            pltpu.SemaphoreType.REGULAR((max(1, min(REACH, deep) - 2),)),
            dma((pieces,)),
            dma((pieces,)),
            dma((spare,)),
            dma((2 * bulks,)),
            dma((2 * bulks,)),
            dma((lanes * bulks,)),
            dma((lanes * bulks,)),
        ],
        compiler_params=pltpu.CompilerParams(collective_id=1, has_side_effects=True,
            vmem_limit_bytes=20 << 20),
        name="scatter",
    )(acc, dq_own, dqt)
    grad = jax.ShapeDtypeStruct((rows, kv_heads * D_HEAD), jnp.float32)
    return pl.pallas_call(
        functools.partial(finish_kernel, deep, kv_heads, share),
        out_shape=(jax.ShapeDtypeStruct(dq_sum.shape, jnp.float32), grad, grad),
        in_specs=[vmem] * 3,
        out_specs=(vmem,) * 3,
        compiler_params=pltpu.CompilerParams(vmem_limit_bytes=8 << 20),
        name="finish",
    )(kv_in, dq_sum, dq_in)


def body(
    queries, keys, values, attn_out, out_grad, log_norm, block_layout, document_ids, block_order
):
    share = GROUP // log_norm.shape[0]
    kv_heads = lax.axis_size("head") // share
    deep = lax.axis_size("seq") // CORES
    rows = keys.shape[0]
    kv, qd, stats, lows, tops, flags, acc, dq_own = gather(
        queries, out_grad, attn_out, log_norm, keys, values, block_layout, document_ids,
        block_order, deep, kv_heads, share)
    dqt, acc = local_grads(qd, stats, kv, lows, tops, flags, acc, rows, kv_heads, share)
    return tuple(scatter(dq_own, dqt, acc, rows, deep, kv_heads, share))


def solution(mesh):
    in_specs = (
        P("seq", "head"),
        P(("seq", "head"), None),
        P(("seq", "head"), None),
        P("seq", "head"),
        P("seq", "head"),
        P("head", "seq"),
        P("head", None, None),
        P(),
        P(),
    )
    out_specs = (P("seq", "head"), P(("seq", "head"), None), P(("seq", "head"), None))
    return jax.shard_map(body, mesh=mesh, in_specs=in_specs, out_specs=out_specs, check_vma=False)
```

```python
import functools
import math

import jax
import jax.numpy as jnp
from jax import lax
from jax.experimental import pallas as pl
from jax.experimental.pallas import tpu as pltpu
from jax.sharding import PartitionSpec as P

D_HEAD = 128
GROUP = 4
BLOCK = 128
DOCS = 8
CORES = 2
PAIR = 6
SPAN = 2
REACH = 3
WORD = 16
SHIFT = 10
LOG2E = math.log2(math.e)
SCALE = D_HEAD ** -0.5
NT = (((1,), (1,)), ((), ()))
TN = (((0,), (0,)), ((), ()))


def place(share):
    seq, head = lax.axis_index("seq"), lax.axis_index("head")
    return seq // CORES, seq % CORES, head // share, head % share


def remote(src, dst, send, recv, seq, head):
    return pltpu.make_async_remote_copy(
        src_ref=src, dst_ref=dst, send_sem=send, recv_sem=recv,
        device_id={"seq": seq, "head": head}, device_id_type=pl.DeviceIdType.MESH)


def landed(where, sem):
    pltpu.make_async_copy(where, where, sem).wait()


def when(there, run):
    if there is True:
        run()
    else:
        pl.when(there)(run)


def span(index, rows):
    return pl.ds(pl.multiple_of(index * rows, rows), rows)


def near(deep, kv_heads, share):
    z, c, g, x = place(share)
    seq, head = z * CORES + c, g * share + x
    peers = [(z * CORES + (c + d) % CORES, head, True) for d in range(1, CORES)]
    peers += [(seq, g * share + (x + d) % share, True) for d in range(1, share)]
    peers += [(seq, (g + d) % kv_heads * share + x, True) for d in range(1, kv_heads)]
    if deep > 1:
        peers += [(seq + CORES, head, z + 1 < deep), (seq - CORES, head, z > 0)]
    return peers


def signal(sem, peers):
    for seq, head, there in peers:
        when(there, lambda: pl.semaphore_signal(
            sem, inc=1, device_id={"seq": seq, "head": head},
            device_id_type=pl.DeviceIdType.MESH))


def count(peers):
    total = 0
    for _, _, there in peers:
        total = total + (1 if there is True else there.astype(jnp.int32))
    return total


def unit_row(u, unit, rows, kv_heads, share):
    z, c, g, x = place(share)
    per = rows // unit
    piece, sub = u // per, u % per
    depth, group = piece // kv_heads, piece % kv_heads
    owner = (depth * CORES + c) * kv_heads * share + group * share + x
    return owner * rows + sub * unit


def gather_kernel(
    deep, kv_heads, share, q_in, do_in, o_in, ln_in, k_in, v_in, lay_in, docs_in, order_in,
    kv, qd, stats, lows, tops, flags, acc, dq_own,
    stage, o_buf, ln_buf, docs, order, layout, seen, own_tops, low_bits,
    local, ready, kv_send, kv_recv, x_send, x_recv, core_send, core_recv,
):
    z, c, g, x = place(share)
    seq, head = z * CORES + c, g * share + x
    heads, q_rows = ln_in.shape
    rows = k_in.shape[0]
    own = q_rows // BLOCK
    unit = min(rows, BLOCK)
    mine = z * kv_heads + g

    def cols(index):
        return pl.ds(pl.multiple_of(index * D_HEAD, D_HEAD), D_HEAD)

    here = span(c, q_rows)
    head_rows = pl.ds(c * q_rows, BLOCK)
    tail_rows = pl.ds(c * q_rows + BLOCK, q_rows - BLOCK)
    pulls = [(ref.at[pl.ds(0, BLOCK), :], qd.at[x, n, head_rows, :])
             for n, ref in enumerate((q_in, do_in))]
    pulls += [(k_in.at[:, cols(g)], kv.at[0, span(mine, rows), :]),
              (v_in.at[:, cols(g)], kv.at[1, span(mine, rows), :])]
    for d in range(1, kv_heads):
        other = cols((g + d) % kv_heads)
        pulls += [(k_in.at[:, other], stage.at[d - 1, 0]), (v_in.at[:, other], stage.at[d - 1, 1])]
    urgent = len(pulls)
    if own > 1:
        pulls += [(ref.at[pl.ds(BLOCK, q_rows - BLOCK), :], qd.at[x, n, tail_rows, :])
                  for n, ref in enumerate((q_in, do_in))]
    pulls += [(order_in, order), (lay_in, layout), (o_in, o_buf), (ln_in, ln_buf), (docs_in, docs)]
    pulls = [pltpu.make_async_copy(src, dst, local.at[n]) for n, (src, dst) in enumerate(pulls)]
    for pull in pulls:
        pull.start()
    peers = near(deep, kv_heads, share)
    barrier = pltpu.get_barrier_semaphore()
    signal(barrier, peers)
    for pull in pulls[:urgent]:
        pull.wait()
    pl.semaphore_wait(barrier, count(peers))

    sent = []

    def send(make, there=True):
        sent.append((there, make))
        when(there, lambda: make().start())

    kv_slots = [0]

    def send_kv(src, dst, arrival, to_seq, to_head, there=True):
        slot = kv_slots[0]
        kv_slots[0] += 1
        send(lambda: remote(src, dst, kv_send.at[slot], arrival, to_seq, to_head), there)

    def whole(index):
        return kv.at[:, span(index, rows), :]

    def onward(index, step, there):
        send_kv(whole(index), whole(index), kv_recv.at[index], seq + step * CORES, head, there)

    def reach(index, step):
        there = inside(z + step)
        send_kv(whole(index), whole(index), kv_recv.at[index], seq + step * CORES, head, there)

    def inside(depth):
        return (depth >= 0) & (depth < deep)

    for turn in range(1, kv_heads):
        send_kv(stage.at[turn - 1], whole(mine), kv_recv.at[mine], seq,
                (g + turn) % kv_heads * share + x)
    along = peers[-2:] if deep > 1 else []
    if deep > 1:
        reach(mine, 1)
        reach(mine, -1)
        signal(ready.at[0], along)

    def chunk_of(lane, core, n):
        return qd.at[lane, :, pl.ds(core * q_rows + n * BLOCK, BLOCK), :]

    def send_chunk(n):
        for d in range(1, share):
            part, slot = chunk_of(x, c, n), (d - 1) * own + n
            send(functools.partial(remote, part, part, x_send.at[slot], x_recv.at[slot], seq,
                                   g * share + (x + d) % share))

    stats_at = (share - 1) * own
    seen_at = stats_at + share - 1
    send_chunk(0)
    for pull in pulls[urgent:-3]:
        pull.wait()
    partner = z * CORES + 1 - c
    mine_rows = qd.at[x, :, here, :]
    send(functools.partial(remote, mine_rows, mine_rows, core_send.at[0], core_recv.at[0],
                           partner, head))
    queries, blocks = CORES * own, order.shape[0]
    units = own_tops.shape[0]
    row_of = lax.broadcasted_iota(jnp.int32, (queries, BLOCK), 0)
    at_block = jnp.zeros((queries, BLOCK), jnp.int32)
    for i in range(queries):
        at_block = jnp.where(row_of == i, order[z * queries + i], at_block)
    column = lax.broadcasted_iota(jnp.int32, (queries, blocks), 1)
    picked = jnp.where(column == at_block[:, :blocks], 1.0, 0.0).astype(jnp.bfloat16)
    for h in range(heads):
        seen[0, h] = jnp.dot(picked, layout[h].astype(jnp.float32).astype(jnp.bfloat16),
                             preferred_element_type=jnp.float32)
    for d in range(1, share):
        slot = seen_at + d - 1
        send(functools.partial(remote, seen.at[0], seen.at[d], x_send.at[slot], x_recv.at[slot],
                               seq, g * share + (x + d) % share))
    for d in range(1, min(REACH, deep) - 1):
        pl.semaphore_wait(ready.at[d - 1], count(along))
        if d + 2 < min(REACH, deep):
            signal(ready.at[d], along)
        reach(mine, d + 1)
        reach(mine, -d - 1)
    for pull in pulls[-3:]:
        pull.wait()
    mine_stats = stats.at[x, pl.ds(c * own, own)]
    for n in range(own):
        part = slice(n * BLOCK, (n + 1) * BLOCK)
        at = pl.ds(c * q_rows + n * BLOCK, BLOCK)
        for h in range(heads):
            lanes = slice(h * D_HEAD, (h + 1) * D_HEAD)
            product = (qd[x, 1, at, lanes].astype(jnp.float32)
                       * o_buf[part, lanes].astype(jnp.float32))
            stats[x, c * own + n, h:h + 1, :] = ln_buf[h:h + 1, part] * LOG2E
            stats[x, c * own + n, heads + h:heads + h + 1, :] = jnp.sum(
                product.T, axis=0, keepdims=True)
    for d in range(1, share):
        slot = stats_at + d - 1
        send(functools.partial(remote, mine_stats, mine_stats, x_send.at[slot], x_recv.at[slot],
                               seq, g * share + (x + d) % share))
    send(functools.partial(remote, mine_stats, mine_stats, core_send.at[1], core_recv.at[1],
                           partner, head))
    for n in range(1, own):
        send_chunk(n)

    block_of = lax.broadcasted_iota(jnp.int32, (blocks, BLOCK), 0)
    stored = [unit_row(u, unit, rows, kv_heads, share) for u in range(units)]
    kept = [order[row // BLOCK] for row in stored]
    starts = [block * BLOCK + row % BLOCK for block, row in zip(kept, stored)]
    chosen = jnp.concatenate([jnp.where(block_of == block, 1.0, 0.0) for block in kept],
                             axis=1).astype(jnp.bfloat16)
    at_query = at_block * BLOCK + lax.broadcasted_iota(jnp.int32, (queries, BLOCK), 1)

    def fill_tops(ref, slot, source):
        for h in range(heads):
            on = jnp.dot(seen[source, h].astype(jnp.bfloat16), chosen,
                         preferred_element_type=jnp.float32)
            at = slice((slot * heads + h) * BLOCK, (slot * heads + h + 1) * BLOCK)
            for u in range(units):
                ref[u, :, at] = jnp.where(on[:, u * BLOCK:(u + 1) * BLOCK] > 0.5, at_query - starts[u], -1)

    ids = docs[...]
    low = jnp.zeros_like(ids)
    for d in range(1, DOCS):
        before = jnp.sum(jnp.where(ids < d, 1.0, 0.0), axis=1, keepdims=True)
        before = jnp.sum(before, axis=0, keepdims=True).astype(jnp.int32)
        low = jnp.where(ids >= d, before, low)
    docs[...] = low
    first = jnp.concatenate(
        [docs[pl.ds(order[z * queries + i], 1), :] for i in range(queries)], axis=0)
    lane_of = lax.broadcasted_iota(jnp.int32, (queries, BLOCK), 1)
    start = jnp.zeros((queries, BLOCK), jnp.int32)
    for u in range(units):
        lows[u] = first - starts[u]
        start = jnp.where(lane_of == u, starts[u], start)
    flags[...] = jnp.where(
        (lane_of < units) & (start < (at_block + 1) * BLOCK) & (first[:, :1] < start + unit),
        1.0, 0.0)
    fill_tops(own_tops, 0, 0)
    acc[...] = jnp.zeros_like(acc)
    dq_own[...] = jnp.zeros_like(dq_own)

    sub = lax.broadcasted_iota(jnp.int32, (unit, SPAN * heads * BLOCK), 0)
    both = [(j, h) for j in range(SPAN) for h in range(heads)]

    def stacked(n, t):
        return jnp.concatenate(
            [qd[x, n, pl.ds(pl.multiple_of((t * SPAN + j) * BLOCK, BLOCK), BLOCK),
                 h * D_HEAD:(h + 1) * D_HEAD] for j, h in both], axis=0)

    def joint(n, batch):
        return jnp.concatenate([kv[n, span(index, rows), :] for index in batch], axis=0)

    def weigh(t, batch):
        st = lax.dot_general(joint(0, batch), stacked(0, t), NT,
                             preferred_element_type=jnp.float32)
        dpt = lax.dot_general(joint(1, batch), stacked(1, t), NT,
                              preferred_element_type=jnp.float32)
        rowed = [stats[x, t * SPAN + j] for j in range(SPAN)]
        norm = jnp.concatenate([rowed[j][h:h + 1] for j, h in both], axis=1)
        delta = jnp.concatenate([rowed[j][heads + h:heads + h + 1] for j, h in both], axis=1)
        keeps = []
        for u in [index * (rows // unit) + n for index in batch for n in range(rows // unit)]:
            rowed_low = [lows[u, pl.ds(t * SPAN + j, 1), :] for j in range(SPAN)]
            low = jnp.concatenate([rowed_low[j] for j, _ in both], axis=1)
            top = jnp.concatenate(
                [own_tops[u, pl.ds(t * SPAN + j, 1), :] for j in range(SPAN)], axis=1)
            keeps.append((sub >= low) & (sub <= top))
        keep = jnp.concatenate(keeps, axis=0)
        w = jnp.where(keep, jnp.exp2(st * (SCALE * LOG2E) - norm), 0.0)
        low_bits[0] = w.astype(jnp.bfloat16)
        low_bits[1] = (w * (dpt - delta)).astype(jnp.bfloat16)

    def collect(t, batch):
        ds = low_bits[1]
        dv = jnp.dot(low_bits[0], stacked(1, t), preferred_element_type=jnp.float32)
        dk = jnp.dot(ds, stacked(0, t), preferred_element_type=jnp.float32)
        dq = lax.dot_general(joint(0, batch), ds, TN, preferred_element_type=jnp.float32)
        for n, index in enumerate(batch):
            at, part = span(index, rows), slice(n * rows, (n + 1) * rows)
            acc[0, at, :] += dk[part]
            acc[1, at, :] += dv[part]
        for j in range(SPAN):
            dq_own[t * SPAN + j] += dq[:, j * heads * BLOCK:(j + 1) * heads * BLOCK]

    turns = queries // SPAN

    def nearest(k):
        short = jnp.minimum(z, deep - 1 - z)
        beyond = jnp.where(z < deep - 1 - z, k, deep - 1 - k)
        return jnp.where(k <= 2 * short, z + (k + 1) // 2 * (1 - 2 * (k % 2)), beyond)

    def of(k, turn):
        return nearest(k) * kv_heads + (g + turn) % kv_heads

    order_of = [[(0, turn) for turn in range(kv_heads)]]
    late = 1
    if kv_heads == 2 and deep > 2:
        order_of += [[(1, turn), (2, turn)] for turn in range(kv_heads)]
        late = 3
    order_of += [[(k, turn) for turn in range(kv_heads)] for k in range(late, deep)]
    batches = [[of(*entry) for entry in batch] for batch in order_of]

    def attend(k, midway=None):
        batch, before = batches[k], batches[max(k - 1, 0)]

        def turn(t, _):
            first = t == 0
            collect(jnp.where(first, turns - 1, t - 1),
                    [jnp.where(first, old, new) for old, new in zip(before, batch)])
            weigh(t, batch)
            return 0

        if k == 0:
            weigh(0, batch)
        lax.fori_loop(1 if k == 0 else 0, turns // 2, turn, 0)
        if midway is not None:
            midway()
        lax.fori_loop(turns // 2, turns, turn, 0)

    def relay(part, slot):
        landed(part, x_recv.at[slot])
        send(functools.partial(remote, part, part, core_send.at[2 + slot],
                               core_recv.at[2 + slot], partner, head))

    def relay_chunk(n):
        for d in range(1, share):
            relay(chunk_of((x - d + share) % share, c, n), (d - 1) * own + n)

    for j in range(1, kv_heads):
        index = z * kv_heads + (g + j) % kv_heads
        landed(whole(index), kv_recv.at[index])
        for d in range(1, min(REACH, deep)):
            reach(index, d)
            reach(index, -d)
    there = span(1 - c, q_rows)
    landed(qd.at[x, :, there, :], core_recv.at[0])
    landed(stats.at[x, pl.ds((1 - c) * own, own)], core_recv.at[1])
    attend(0)

    def arrive(d, turns_in):
        for turn in turns_in:
            for depth, step in ((z - d, 1), (z + d, -1)):
                index = depth * kv_heads + (g + turn) % kv_heads
                when(inside(depth), functools.partial(
                    lambda index: landed(whole(index), kv_recv.at[index]), index))
                if REACH - 1 <= d < deep - 1:
                    onward(index, step, inside(depth) & inside(z + step))

    chunks = list(range(own))

    def relay_next():
        if chunks:
            relay_chunk(chunks.pop(0))

    def relay_rest():
        while chunks:
            relay_chunk(chunks.pop(0))

    done = 1
    for turns_in in ([0], list(range(1, kv_heads))):
        for d in range(1, min(REACH, deep)):
            arrive(d, turns_in)
        if turns_in == [0]:
            for e in range(1, share):
                landed(seen.at[e], x_recv.at[seen_at + e - 1])
                fill_tops(tops, e - 1, e)
                relay(stats.at[(x - e + share) % share, pl.ds(c * own, own)], stats_at + e - 1)
        relay_next()
        if late == 3:
            attend(done)
            done += 1
    for d in range(REACH, deep):
        arrive(d, range(kv_heads))
    relay_next()
    for k in range(done, deep):
        attend(k, relay_rest if k == deep - 1 else None)
    relay_rest()
    collect(turns - 1, batches[deep - 1])
    for d in range(1, share):
        lane = (x - d + share) % share
        for n in range(own):
            landed(chunk_of(lane, 1 - c, n), core_recv.at[2 + (d - 1) * own + n])
        landed(stats.at[lane, pl.ds((1 - c) * own, own)], core_recv.at[2 + stats_at + d - 1])
    for there, make in sent:
        when(there, functools.partial(lambda make: make().wait_send(), make))


def gather(queries, out_grad, attn_out, log_norm, keys, values, block_layout, document_ids,
           block_order, deep, kv_heads, share):
    rows = keys.shape[0]
    heads, q_rows = log_norm.shape
    blocks = block_order.shape[0]
    own = q_rows // BLOCK
    unit = min(rows, BLOCK)
    pieces = deep * kv_heads
    kv_rows = pieces * rows
    hbm = pl.BlockSpec(memory_space=pltpu.HBM)
    vmem = pl.BlockSpec(memory_space=pltpu.VMEM)
    lanes = share - 1
    x_copies = max(1, lanes * (own + 2))
    steps = min(REACH, deep) - 1
    kv_copies = max(1, kv_heads - 1 + 2 * kv_heads * (steps + max(0, deep - REACH)))
    dma = pltpu.SemaphoreType.DMA
    return pl.pallas_call(
        functools.partial(gather_kernel, deep, kv_heads, share),
        out_shape=(
            jax.ShapeDtypeStruct((2, kv_rows, D_HEAD), keys.dtype),
            jax.ShapeDtypeStruct((share, 2, CORES * q_rows, heads * D_HEAD), queries.dtype),
            jax.ShapeDtypeStruct((share, CORES * own, 2 * heads, BLOCK), jnp.float32),
            jax.ShapeDtypeStruct((kv_rows // unit, CORES * own, BLOCK), jnp.int32),
            jax.ShapeDtypeStruct(
                (kv_rows // unit, CORES * own, max(1, lanes) * heads * BLOCK), jnp.int32),
            jax.ShapeDtypeStruct((CORES * own, BLOCK), jnp.float32),
            jax.ShapeDtypeStruct((2, kv_rows, D_HEAD), jnp.float32),
            jax.ShapeDtypeStruct((CORES * own, D_HEAD, heads * BLOCK), jnp.float32),
        ),
        in_specs=[hbm] * 9,
        out_specs=(vmem,) * 8,
        scratch_shapes=[
            pltpu.VMEM((max(1, kv_heads - 1), 2, rows, D_HEAD), keys.dtype),
            pltpu.VMEM(attn_out.shape, attn_out.dtype),
            pltpu.VMEM(log_norm.shape, jnp.float32),
            pltpu.VMEM((blocks, BLOCK), jnp.int32),
            pltpu.SMEM((blocks,), jnp.int32),
            pltpu.VMEM(block_layout.shape, jnp.int32),
            pltpu.VMEM((share, heads, CORES * own, blocks), jnp.float32),
            pltpu.VMEM((kv_rows // unit, CORES * own, heads * BLOCK), jnp.int32),
            pltpu.VMEM((2, kv_heads * rows, SPAN * heads * BLOCK), jnp.bfloat16),
            dma((2 * kv_heads + (9 if own > 1 else 7),)),
            pltpu.SemaphoreType.REGULAR((max(1, steps - 1),)),
            dma((kv_copies,)),
            dma((pieces,)),
            dma((x_copies,)),
            dma((x_copies,)),
            dma((2 + x_copies - lanes,)),
            dma((2 + x_copies - lanes,)),
        ],
        compiler_params=pltpu.CompilerParams(collective_id=0, has_side_effects=True,
            vmem_limit_bytes=16 << 20),
        name="gather",
    )(*[pltpu.with_memory_space_constraint(array, pltpu.HBM) for array in (
        queries, out_grad, attn_out, log_norm, keys, values, block_layout,
        document_ids.reshape(blocks, BLOCK), block_order)])


def grads_kernel(
    kv_heads, share, rows, qd, stats, kv, lows, tops, flags, acc_in,
    dqt, acc, items, low_bits,
):
    x = place(share)[3]
    queries = dqt.shape[1]
    heads = qd.shape[3] // D_HEAD
    unit = min(rows, BLOCK)
    units = kv.shape[1] // unit
    others = [(x - d + share) % share for d in range(1, share)]
    lane_of = lax.broadcasted_iota(jnp.int32, (1, BLOCK), 1)
    marks = [jnp.zeros((1, BLOCK), jnp.float32) for _ in range(0, units, WORD)]
    for u in range(units):
        marks[u // WORD] = jnp.where(lane_of == u, float(1 << u % WORD), marks[u // WORD])
    words = [[jnp.sum(flags[i:i + 1, :] * mark).astype(jnp.int32) for mark in marks]
             for i in range(queries)]
    acc[...] = acc_in[...]

    def clear(i, _):
        for s in range(share - 1):
            dqt[s, pl.ds(i, 1)] = jnp.zeros((1,) + dqt.shape[2:], jnp.float32)
        return 0

    lax.fori_loop(0, queries, clear, 0)
    total = jnp.int32(0)
    for i in range(queries):
        for u in range(units):
            items[total] = i << SHIFT | u
            total = total + ((words[i][u // WORD] >> (u % WORD)) & 1)
    wide = (share - 1) * heads * BLOCK
    sub = lax.broadcasted_iota(jnp.int32, (unit, wide), 0)
    for n in range(2 * PAIR):
        items[total + n] = 0

    def stacked(n, i):
        at = pl.ds(pl.multiple_of(i * BLOCK, BLOCK), BLOCK)
        return jnp.concatenate(
            [qd[s, n, at, h * D_HEAD:(h + 1) * D_HEAD] for s in others for h in range(heads)],
            axis=0)

    def weigh(n, slot):
        i, u = items[n] >> SHIFT, items[n] & ((1 << SHIFT) - 1)
        at = pl.ds(pl.multiple_of(u * unit, unit), unit)
        k, v = kv[0, at, :], kv[1, at, :]
        q4, do4 = stacked(0, i), stacked(1, i)
        rowed = [stats[s, i] for s in others]
        norm = jnp.concatenate([r[h:h + 1] for r in rowed for h in range(heads)], axis=1)
        delta = jnp.concatenate(
            [r[heads + h:heads + h + 1] for r in rowed for h in range(heads)], axis=1)
        low = jnp.concatenate([lows[u, pl.ds(i, 1), :]] * ((share - 1) * heads), axis=1)
        top = jnp.where(n < total, tops[u, pl.ds(i, 1), :], -1)
        keep = (sub >= low) & (sub <= top)
        st = lax.dot_general(k, q4, NT, preferred_element_type=jnp.float32)
        dpt = lax.dot_general(v, do4, NT, preferred_element_type=jnp.float32)
        w = jnp.where(keep, jnp.exp2(st * (SCALE * LOG2E) - norm), 0.0)
        low_bits[slot, 0] = w.astype(jnp.bfloat16)
        low_bits[slot, 1] = (w * (dpt - delta)).astype(jnp.bfloat16)

    def collect(n, slot):
        i, u = items[n] >> SHIFT, items[n] & ((1 << SHIFT) - 1)
        at = pl.ds(pl.multiple_of(u * unit, unit), unit)
        q4, do4 = stacked(0, i), stacked(1, i)
        ds = low_bits[slot, 1]
        dv = jnp.dot(low_bits[slot, 0], do4, preferred_element_type=jnp.float32)
        dk = jnp.dot(ds, q4, preferred_element_type=jnp.float32)
        dq = lax.dot_general(kv[0, at, :], ds, TN, preferred_element_type=jnp.float32)
        return i, at, dk, dv, dq

    def add(done):
        for i, at, dk, dv, dq in done:
            acc[0, at, :] += dk
            acc[1, at, :] += dv
            for s in range(share - 1):
                dqt[s, i] += dq[:, s * heads * BLOCK:(s + 1) * heads * BLOCK]

    def step(t, _):
        done = [collect((t - 1) * PAIR + n, n) for n in range(PAIR)]
        for n in range(PAIR):
            weigh(t * PAIR + n, n)
        add(done)
        return 0

    steps = jnp.maximum((total + PAIR - 1) // PAIR, 1)
    for n in range(PAIR):
        weigh(jnp.int32(n), n)
    lax.fori_loop(1, steps, step, 0)
    add([collect((steps - 1) * PAIR + n, n) for n in range(PAIR)])


def local_grads(qd, stats, kv, lows, tops, flags, acc, rows, kv_heads, share):
    heads = qd.shape[3] // D_HEAD
    units, queries = tops.shape[:2]
    vmem = pl.BlockSpec(memory_space=pltpu.VMEM)
    return pl.pallas_call(
        functools.partial(grads_kernel, kv_heads, share, rows),
        out_shape=(
            jax.ShapeDtypeStruct((share - 1, queries, D_HEAD, heads * BLOCK), jnp.float32),
            jax.ShapeDtypeStruct(kv.shape, jnp.float32),
        ),
        in_specs=[vmem] * 7,
        out_specs=(vmem, vmem),
        scratch_shapes=[
            pltpu.SMEM((queries * units + 2 * PAIR,), jnp.int32),
            pltpu.VMEM((PAIR, 2, min(rows, BLOCK), (share - 1) * heads * BLOCK),
                       jnp.bfloat16),
        ],
        compiler_params=pltpu.CompilerParams(
            vmem_limit_bytes=24 << 20),
        name="grads",
    )(qd, stats, kv, lows, tops, flags, acc)


def scatter_kernel(
    deep, kv_heads, share, rows, acc, dq_own, dqt, kv_in, dq_sum, dq_in,
    kv_out, joined, own_core, dq_core, dq_out, ready, kv_send, kv_recv, join_recv, core_send, core_recv,
    x_send, x_recv,
):
    z, c, g, x = place(share)
    seq, head = z * CORES + c, g * share + x
    partner = z * CORES + 1 - c
    own = dqt.shape[1] // CORES
    heads = dqt.shape[3] // BLOCK
    mine = z * kv_heads + g
    peers = near(deep, kv_heads, share)
    along = peers[-2:] if deep > 1 else []
    peers += [(to, (g + d) % kv_heads * share + x, there)
              for to, _, there in along for d in range(1, kv_heads)]
    barrier = pltpu.get_barrier_semaphore()
    signal(barrier, peers)
    for p in range(deep * kv_heads):
        part = slice(p * rows, (p + 1) * rows)
        kv_out[p, 0] = (acc[0, part, :] * SCALE).astype(jnp.bfloat16)
        kv_out[p, 1] = acc[1, part, :].astype(jnp.bfloat16)
    kv_in[mine] = kv_out[mine]
    for depth in range(deep):
        def unused(depth=depth):
            at = pl.ds(depth * kv_heads, kv_heads)
            kv_in[at] = jnp.zeros((kv_heads,) + kv_in.shape[1:], kv_in.dtype)

        if depth >= REACH or depth < deep - REACH:
            pl.when((depth - z >= REACH) | (z - depth >= REACH))(unused)
    pl.semaphore_wait(barrier, count(peers))

    sent = []

    def send(make, there=True):
        sent.append((there, make))
        when(there, lambda: make().start())

    def inside(depth):
        return (depth >= 0) & (depth < deep)

    def give(step, turn, there=True):
        depth, group = z + step, (g + turn) % kv_heads
        index = depth * kv_heads + group
        send(functools.partial(remote, kv_out.at[index], kv_in.at[mine], kv_send.at[index],
                               kv_recv.at[mine], depth * CORES + c, group * share + x), there)

    def spare(index):
        return index if deep > REACH + 1 else index % kv_heads

    def join(index):
        where = spare(index)
        landed(joined.at[where], join_recv.at[where])
        at = span(index, rows)
        for n, factor in enumerate((SCALE, 1.0)):
            kv_out[index, n] = (acc[n, at, :] * factor
                                + joined[where, n].astype(jnp.float32)).astype(jnp.bfloat16)

    bulk = 2 - own % 2

    def crossing(core, n):
        at, to = pl.ds(core * own + n * bulk, bulk), pl.ds(n * bulk, bulk)
        return (dqt.at[:, at], dq_core.at[:, to]), (dq_own.at[at], own_core.at[to])

    for far in range(deep - 1, REACH - 1, -1):
        for depth, step in ((far, 1), (deep - 1 - far, -1)):
            away = (depth - z) * step >= REACH
            behind = (z > 0) if step == 1 else (z + 1 < deep)
            for turn in range(kv_heads):
                index = depth * kv_heads + (g + turn) % kv_heads
                if far > REACH:
                    pl.when(away & behind)(functools.partial(join, index))
                where = spare(index)
                send(functools.partial(remote, kv_out.at[index], joined.at[where],
                                       kv_send.at[index], join_recv.at[where],
                                       (z + step) * CORES + c, head), away)
    near_end = {1: z == 0, -1: z == deep - 1}

    def give_all(d):
        for turn in range(kv_heads):
            for step in (1, -1):
                there = inside(z + step * d)
                give(step * d, turn, there & near_end[step] if d == REACH - 1 else there)

    if deep > 1:
        give_all(1)
    for turn in range(1, kv_heads):
        give(0, turn)
    for n in range(own // bulk):
        for m, (src, dst) in enumerate(crossing(1 - c, n)):
            send(functools.partial(remote, src, dst, core_send.at[2 * n + m],
                                   core_recv.at[2 * n + m], partner, head))
    for d in range(1, min(REACH, deep) - 1):
        signal(ready.at[d - 1], along)
        pl.semaphore_wait(ready.at[d - 1], count(along))
        give_all(d + 1)

    def query_block(n):
        for m, (_, dst) in enumerate(crossing(1 - c, n)):
            landed(dst, core_recv.at[2 * n + m])
        for d in range(share - 1, -1, -1):
            for block in range(n * bulk, (n + 1) * bulk):
                at = slice(block * BLOCK, (block + 1) * BLOCK)
                if d:
                    total = (dqt[d - 1, c * own + block] + dq_core[d - 1, block]) * SCALE
                else:
                    total = (dq_own[c * own + block] + own_core[block]) * SCALE
                for h in range(heads):
                    flat = total[:, h * BLOCK:(h + 1) * BLOCK].T
                    if d:
                        dq_out[d - 1, at, h * D_HEAD:(h + 1) * D_HEAD] = flat.astype(jnp.bfloat16)
                    else:
                        dq_sum[at, h * D_HEAD:(h + 1) * D_HEAD] = flat
            if d:
                at, slot = pl.ds(n * bulk * BLOCK, bulk * BLOCK), (d - 1) * (own // bulk) + n
                send(functools.partial(
                    remote, dq_out.at[d - 1, at, :], dq_in.at[d - 1, at, :], x_send.at[slot],
                    x_recv.at[slot], seq, g * share + (x - d + share) % share))

    query_block(0)
    if deep >= REACH:
        for turn in range(kv_heads):
            for step in (1, -1):
                depth = z + step * (REACH - 1)
                there = inside(depth) & ~near_end[step]
                index = depth * kv_heads + (g + turn) % kv_heads
                pl.when(there)(functools.partial(join, index))
                give(step * (REACH - 1), turn, there)
    for n in range(1, own // bulk):
        query_block(n)
    for depth in range(deep):
        for turn in range(kv_heads):
            index = depth * kv_heads + (g + turn) % kv_heads
            close = (depth - z < REACH) & (z - depth < REACH)
            get = functools.partial(
                lambda index: landed(kv_in.at[index], kv_recv.at[index]), index)
            when(close if turn else close & (depth != z), get)
    for d in range(1, share):
        for n in range(own // bulk):
            at = pl.ds(n * bulk * BLOCK, bulk * BLOCK)
            landed(dq_in.at[d - 1, at, :], x_recv.at[(d - 1) * (own // bulk) + n])
    for there, make in sent:
        when(there, functools.partial(lambda make: make().wait_send(), make))


def finish_kernel(deep, kv_heads, share, kv_in, dq_sum, dq_in, dq, dk, dv):
    total = dq_sum[...]
    for d in range(share - 1):
        total += dq_in[d].astype(jnp.float32)
    dq[...] = total
    for j in range(kv_heads):
        for n, ref in enumerate((dk, dv)):
            total = kv_in[j, n].astype(jnp.float32)
            for depth in range(1, deep):
                total += kv_in[depth * kv_heads + j, n].astype(jnp.float32)
            ref[:, j * D_HEAD:(j + 1) * D_HEAD] = total


def scatter(dq_own, dqt, acc, rows, deep, kv_heads, share):
    pieces = deep * kv_heads
    queries, heads = dqt.shape[1], dqt.shape[3] // BLOCK
    own = queries // CORES
    q_rows = own * BLOCK
    vmem = pl.BlockSpec(memory_space=pltpu.VMEM)
    dma = pltpu.SemaphoreType.DMA
    lanes = max(1, share - 1)
    bulks = own // (2 - own % 2)
    spare = pieces if deep > REACH + 1 else kv_heads
    kv_in, dq_sum, dq_in = pl.pallas_call(
        functools.partial(scatter_kernel, deep, kv_heads, share, rows),
        out_shape=(
            jax.ShapeDtypeStruct((pieces, 2, rows, D_HEAD), jnp.bfloat16),
            jax.ShapeDtypeStruct((q_rows, heads * D_HEAD), jnp.float32),
            jax.ShapeDtypeStruct((lanes, q_rows, heads * D_HEAD), jnp.bfloat16),
        ),
        in_specs=[vmem] * 3,
        out_specs=(vmem,) * 3,
        scratch_shapes=[
            pltpu.VMEM((pieces, 2, rows, D_HEAD), jnp.bfloat16),
            pltpu.VMEM((spare, 2, rows, D_HEAD), jnp.bfloat16),
            pltpu.VMEM((own,) + dqt.shape[2:], jnp.float32),
            pltpu.VMEM((dqt.shape[0], own) + dqt.shape[2:], jnp.float32),
            pltpu.VMEM((lanes, q_rows, heads * D_HEAD), jnp.bfloat16),
            pltpu.SemaphoreType.REGULAR((max(1, min(REACH, deep) - 2),)),
            dma((pieces,)),
            dma((pieces,)),
            dma((spare,)),
            dma((2 * bulks,)),
            dma((2 * bulks,)),
            dma((lanes * bulks,)),
            dma((lanes * bulks,)),
        ],
        compiler_params=pltpu.CompilerParams(collective_id=1, has_side_effects=True,
            vmem_limit_bytes=20 << 20),
        name="scatter",
    )(acc, dq_own, dqt)
    grad = jax.ShapeDtypeStruct((rows, kv_heads * D_HEAD), jnp.float32)
    return pl.pallas_call(
        functools.partial(finish_kernel, deep, kv_heads, share),
        out_shape=(jax.ShapeDtypeStruct(dq_sum.shape, jnp.float32), grad, grad),
        in_specs=[vmem] * 3,
        out_specs=(vmem,) * 3,
        compiler_params=pltpu.CompilerParams(vmem_limit_bytes=8 << 20),
        name="finish",
    )(kv_in, dq_sum, dq_in)


def body(
    queries, keys, values, attn_out, out_grad, log_norm, block_layout, document_ids, block_order
):
    share = GROUP // log_norm.shape[0]
    kv_heads = lax.axis_size("head") // share
    deep = lax.axis_size("seq") // CORES
    rows = keys.shape[0]
    kv, qd, stats, lows, tops, flags, acc, dq_own = gather(
        queries, out_grad, attn_out, log_norm, keys, values, block_layout, document_ids,
        block_order, deep, kv_heads, share)
    dqt, acc = local_grads(qd, stats, kv, lows, tops, flags, acc, rows, kv_heads, share)
    return tuple(scatter(dq_own, dqt, acc, rows, deep, kv_heads, share))


def solution(mesh):
    in_specs = (
        P("seq", "head"),
        P(("seq", "head"), None),
        P(("seq", "head"), None),
        P("seq", "head"),
        P("seq", "head"),
        P("head", "seq"),
        P("head", None, None),
        P(),
        P(),
    )
    out_specs = (P("seq", "head"), P(("seq", "head"), None), P(("seq", "head"), None))
    return jax.shard_map(body, mesh=mesh, in_specs=in_specs, out_specs=out_specs, check_vma=False)
```
